32 devices in a mesh: row: 8 (over z, core), col: 4 (over y, x).
Axes of the slice: x: 2, y: 2, z: 4, core: 2. Of those that a mesh axis runs over, the one named last changes fastest.
Arguments:
- fine_residual: float32 [16, 3, 1572864], P(None, None, ('row', 'col')), may hold values from -6 to 6
- restriction: float32 [3, 3, 1572864], P(None, None, ('row', 'col')), may hold values from -1.25 to 1.25
- restriction_pattern: int32 [1572864], P(('row', 'col')), may hold values 0 or 1
- cell_aggregate: int32 [384, 512], P('row', 'col'), may hold values from 0 to 196607, as said below
- block_inverse: float32 [3, 3, 384, 512], P(None, None, 'row', 'col'), may hold values from -4 to 4, as said below
- off_blocks: float32 [4, 3, 3, 384, 512], P(None, None, None, 'row', 'col'), may hold values from -0.5 to 0.5
- operator_pattern: int32 [4, 384, 512], P(None, 'row', 'col'), may hold values 0 or 1
Outputs:
- coarse_solution: float32 [16, 3, 384, 512], P(None, None, 'row', 'col')
- fine_correction: float32 [16, 3, 1572864], P(None, None, ('row', 'col'))
The draws below stay inside these ranges and needn't reach their ends.
Inputs may be any that keep to these rules, and one draw needn't show every extreme that they name: `cell_aggregate`: every aggregate number 0 to 196607 stands in exactly one coarse cell. Aggregate g = f * 6144 + a lies in the tile numbered a mod 32, where the tile of rows i * 48 to (i + 1) * 48 - 1 and columns j * 128 to (j + 1) * 128 - 1 is numbered i * 4 + j. `block_inverse`: each 3x3 block is the inverse of a cell's diagonal block.
All inputs are finite; a program needn't handle non-finite values. No bound on the sum of `restriction_pattern` or of `operator_pattern` on one device may be relied on, other than what follows from the above.
Results may differ from the reference program's by a relative error of at most 0.00002.
Values sent between devices are 32-bit elements; how exact they have to be, the bound alone decides.
No kernel may reach another device: no remote copies, remote signals or barrier semaphores. Data moves between devices by JAX's collectives and lax.ppermute only.
A program may use at most 128 MiB of HBM per device.

```python
import jax
import jax.numpy as jnp

NRHS = 16
CR = 48
CC = 128
FPA = 8
ITERS = 4
AGG_DEV = 6144
FINE = 1572864
NCR = 384
NCC = 512
N_ROW = 8
N_COL = 4


def draw_cell_aggregate(key, part):
    devices = N_ROW * N_COL

    def tile_cells(tile):
        order = jax.random.permutation(jax.random.fold_in(key, tile), AGG_DEV)
        owner = order % devices
        local = order // devices * devices + tile
        return (owner * AGG_DEV + local).astype(jnp.int32)
    tiles = jax.vmap(tile_cells)(jnp.arange(devices, dtype=jnp.int32))
    grid = tiles.reshape(N_ROW, N_COL, CR, CC).transpose(0, 2, 1, 3)
    return grid.reshape(N_ROW * CR, N_COL * CC)


def draw_block_inverse(key, part):
    scale_key = jax.random.fold_in(key, 11)
    noise_key = jax.random.fold_in(key, 12)
    scale = jnp.exp(jax.random.uniform(scale_key, (NCR, NCC), jnp.float32, jnp.log(0.5), jnp.log(2.0)))
    noise = 0.3 * jnp.clip(jax.random.normal(noise_key, (3, 3, NCR, NCC), jnp.float32), -2.5, 2.5)
    identity = jnp.eye(3, dtype=jnp.float32)[:, :, None, None]
    return (scale[None, None] * (identity + noise)).astype(jnp.float32)


def touch_ends(result, rng, low, high):
    shape = result.shape
    place = [jax.random.randint(jax.random.fold_in(rng, axis), (), 0, shape[axis]) for axis in range(len(shape))]
    result = result.at[tuple(place)].set(low)
    longest = shape.index(max(shape))
    place[longest] = (place[longest] + 1) % shape[longest]
    return result.at[tuple(place)].set(high)


def block_scale(rng, dims, split, smallest, high):
    def one(dim, parts):
        heights = jax.random.uniform(jax.random.fold_in(jax.random.fold_in(rng, 6), dim), (parts,), jnp.float32, smallest / len(split), high / len(split))
        return jnp.repeat(jnp.exp(heights), dims[dim] // parts).reshape((-1,) + (1,) * (len(dims) - dim - 1))

    level = one(*split[0])
    for cut in split[1:]:
        level = level * one(*cut)
    return level


def centred(stream_key, extent, width, bound, pieces=(), kind=jnp.bfloat16):
    drawn = width * jax.random.normal(stream_key, extent, jnp.float32)
    if pieces:
        drawn = drawn * block_scale(stream_key, extent, pieces, -0.22, 0.18)
    return jnp.clip(drawn, -bound, bound).astype(kind)


def setup_inputs(seed: int = 0) -> dict:
    key_list = jax.random.split(jax.random.key(seed), 8)
    return {
        "fine_residual": centred(key_list[0], (NRHS, 3, FINE), 1.0, 6.0, ((2, 32),), jnp.float32),
        "restriction": centred(key_list[1], (3, 3, FINE), (3 * FPA) ** -0.5, 1.25, ((2, 32),), jnp.float32),
        "restriction_pattern": touch_ends((jax.random.randint(key_list[2], (FINE,), 0, 4) < 3).astype(jnp.int32), jax.random.fold_in(key_list[2], 1), 0, 1),
        "cell_aggregate": draw_cell_aggregate(jax.random.fold_in(key_list[7], 71), 0),
        "block_inverse": draw_block_inverse(jax.random.fold_in(key_list[7], 71), 0),
        "off_blocks": centred(key_list[5], (4, 3, 3, NCR, NCC), 0.1, 0.5, ((3, 8), (4, 4)), jnp.float32),
        "operator_pattern": touch_ends((jax.random.randint(key_list[6], (4, NCR, NCC), 0, 4) < 3).astype(jnp.int32), jax.random.fold_in(key_list[6], 1), 0, 1),
    }


def apply_inverse(inverse, vector):
    total = inverse[:, 0][None] * vector[:, 0][:, None]
    for source in range(1, 3):
        total = total + inverse[:, source][None] * vector[:, source][:, None]
    return total


def neighbours(padded):
    height = padded.shape[-2] - 2
    breadth = padded.shape[-1] - 2
    return (padded[..., 0:height, 1:breadth + 1], padded[..., 2:height + 2, 1:breadth + 1],
            padded[..., 1:height + 1, 0:breadth], padded[..., 1:height + 1, 2:breadth + 2])


def sweep_once(padded, target_side, inverse, coupling):
    total = target_side
    for direction, shifted in enumerate(neighbours(padded)):
        for source in range(3):
            total = total - coupling[direction, :, source][None] * shifted[:, source][:, None]
    return apply_inverse(inverse, total)


def restrict_terms(residual, restriction, pattern):
    masked = residual * pattern.astype(jnp.float32)[None, None]
    total = restriction[:, 0][None] * masked[:, 0][:, None]
    for source in range(1, 3):
        total = total + restriction[:, source][None] * masked[:, source][:, None]
    loads = total.shape[0]
    return total.reshape(loads, 3, -1, FPA, AGG_DEV).sum(axis=3).reshape(loads, 3, -1)


def prolong_terms(values, restriction, pattern):
    loads = values.shape[0]
    slabs = values.shape[2] // AGG_DEV
    expanded = jnp.broadcast_to(values.reshape(loads, 3, slabs, 1, AGG_DEV), (loads, 3, slabs, FPA, AGG_DEV)).reshape(loads, 3, -1)
    total = restriction[0][None] * expanded[:, 0][:, None]
    for source in range(1, 3):
        total = total + restriction[source][None] * expanded[:, source][:, None]
    return total * pattern.astype(jnp.float32)[None, None]


def reference(fine_residual, restriction, restriction_pattern, cell_aggregate, block_inverse, off_blocks, operator_pattern):
    loads = fine_residual.shape[0]
    aggregate_rhs = restrict_terms(fine_residual, restriction, restriction_pattern)
    flat_cells = cell_aggregate.reshape(-1)
    coarse_rhs = jnp.take(aggregate_rhs, flat_cells, axis=2).reshape(loads, 3, NCR, NCC)
    coupling = off_blocks * operator_pattern.astype(jnp.float32)[:, None, None]
    iterate = apply_inverse(block_inverse, coarse_rhs)
    for sweep_index in range(ITERS - 1):
        padded = jnp.pad(iterate, ((0, 0), (0, 0), (1, 1), (1, 1)))
        iterate = sweep_once(padded, coarse_rhs, block_inverse, coupling)
    aggregate_solution = jnp.zeros_like(aggregate_rhs).at[:, :, flat_cells].set(iterate.reshape(loads, 3, -1))
    fine_correction = prolong_terms(aggregate_solution, restriction, restriction_pattern)
    return iterate, fine_correction
```

```python
import functools

import jax
import jax.numpy as jnp
from jax import lax
from jax.experimental import pallas as pl
from jax.experimental.pallas import tpu as pltpu
from jax.sharding import PartitionSpec as P

FPA = 8
ITERS = 4
LANES = 128
CHUNKS = 2
AXES = ("row", "col")


def vmem_spec():
    return pl.BlockSpec(memory_space=pltpu.VMEM)


class Sizes:
    def __init__(self, fine, loads, rows, cols, rows_n, cols_n):
        self.devices = rows_n * cols_n
        self.rows_n, self.cols_n = rows_n, cols_n
        self.fine = fine
        self.agg = fine // FPA
        self.blocks = self.agg // LANES
        self.loads = loads
        self.rows, self.cols = rows, cols
        self.q = loads // CHUNKS
        self.comps = 3 * self.q
        self.group = LANES // self.q
        self.groups = self.blocks // self.group
        self.low = LANES // self.devices
        self.per_peer = 3 * self.groups * self.low
        self.depth = ITERS - 1
        self.wide = rows + 2 * self.depth


def for_tiles(s, visit):
    for comp in range(3):
        for grp in range(s.groups):
            starts = []
            for low in range(s.low):
                slot = (comp * s.groups + grp) * s.low + low
                for first in range(0, s.devices, 8):
                    starts.append(first * s.per_peer + slot)
            visit(comp, grp, starts)


def store_tiles(s, out_ref, tile_of):
    def visit(comp, grp, starts):
        turned = tile_of(comp, grp).T
        for at, start in enumerate(starts):
            out_ref[pl.ds(start, 8, stride=s.per_peer), :] = turned[at * 8 : at * 8 + 8]

    for_tiles(s, visit)


def load_tiles(s, in_ref, take):
    def visit(comp, grp, starts):
        parts = [in_ref[pl.ds(start, 8, stride=s.per_peer), :] for start in starts]
        take(comp, grp, jnp.concatenate(parts, axis=0).T)

    for_tiles(s, visit)


def restrict_kernel(s, x_ref, rest_ref, pat_ref, out_ref, acc):
    step = pl.program_id(0)

    @pl.when(step == 0)
    def _():
        acc[...] = jnp.zeros_like(acc)

    def column(block, carry):
        at = pl.ds(pl.multiple_of(block * LANES, LANES), LANES)
        mask = pat_ref[0:1, at].astype(jnp.float32)
        value = [x_ref[comp, :, at] for comp in range(3)]
        for comp in range(3):
            total = acc[comp, :, at]
            for source in range(3):
                total = total + (rest_ref[comp, source : source + 1, at] * mask) * value[source]
            acc[comp, :, at] = total
        return carry

    lax.fori_loop(0, s.blocks, column, 0)

    @pl.when(step == FPA - 1)
    def _():
        def tile_of(comp, grp):
            parts = []
            for member in range(s.group):
                low = (grp * s.group + member) * LANES
                parts.append(acc[comp, :, low : low + LANES])
            return jnp.concatenate(parts, axis=0)

        store_tiles(s, out_ref, tile_of)


def restrict(s, residual, restriction, pattern, chunk):
    return pl.pallas_call(
        functools.partial(restrict_kernel, s),
        grid=(FPA,),
        in_specs=[
            pl.BlockSpec((3, s.q, s.agg), lambda p: (0, chunk, p)),
            pl.BlockSpec((3, 3, s.agg), lambda p: (0, 0, p)),
            pl.BlockSpec((1, s.agg), lambda p: (0, p)),
        ],
        out_specs=pl.BlockSpec((s.devices * s.per_peer, LANES), lambda p: (0, 0)),
        out_shape=jax.ShapeDtypeStruct((s.devices * s.per_peer, LANES), jnp.float32),
        scratch_shapes=[pltpu.VMEM((3, s.q, s.agg), jnp.float32)],
        name="restrict",
    )(residual, restriction, pattern)


def prolong_kernel(s, in_ref, rest_ref, pat_ref, out_ref, agg):
    step = pl.program_id(0)

    @pl.when(step == 0)
    def _():
        def take(comp, grp, turned):
            for member in range(s.group):
                low = (grp * s.group + member) * LANES
                agg[comp, :, low : low + LANES] = turned[member * s.q : (member + 1) * s.q]

        load_tiles(s, in_ref, take)

    def column(block, carry):
        at = pl.ds(pl.multiple_of(block * LANES, LANES), LANES)
        mask = pat_ref[0:1, at].astype(jnp.float32)
        value = [agg[comp, :, at] for comp in range(3)]
        for comp in range(3):
            total = (rest_ref[0, comp : comp + 1, at] * mask) * value[0]
            for source in range(1, 3):
                total = total + (rest_ref[source, comp : comp + 1, at] * mask) * value[source]
            out_ref[comp, :, at] = total
        return carry

    lax.fori_loop(0, s.blocks, column, 0)


def prolong(s, arrived, restriction, pattern, chunk, whole):
    kernel = functools.partial(prolong_kernel, s)
    specs = [
        vmem_spec(),
        pl.BlockSpec((3, 3, s.agg), lambda p: (0, 0, p)),
        pl.BlockSpec((1, s.agg), lambda p: (0, p)),
    ]
    args = [arrived, restriction, pattern]
    alias = {}
    body = kernel
    if whole is not None:
        specs.append(pl.BlockSpec(memory_space=pl.ANY))
        args.append(whole)
        alias = {3: 0}

        def body(in_ref, rest_ref, pat_ref, whole_ref, out_ref, agg):
            del whole_ref
            kernel(in_ref, rest_ref, pat_ref, out_ref, agg)

    return pl.pallas_call(
        body,
        grid=(FPA,),
        in_specs=specs,
        out_specs=pl.BlockSpec((3, s.q, s.agg), lambda p: (0, chunk, p)),
        out_shape=jax.ShapeDtypeStruct((3, s.loads, s.fine), jnp.float32),
        scratch_shapes=[pltpu.VMEM((3, s.q, s.agg), jnp.float32)],
        input_output_aliases=alias,
        name="prolong",
    )(*args)


def gather_rows(s, table_ref, row_ref, lane_ref, out_ref, count):
    def one(k, carry):
        rows = jnp.broadcast_to(row_ref[pl.ds(k, 1), :], (8, LANES))
        lanes = jnp.broadcast_to(lane_ref[pl.ds(k, 1), :], (8, LANES))
        parts = s.comps // 8
        total = [jnp.zeros((8, LANES), jnp.float32) for _ in range(parts)]
        for source in range(count):
            hit = rows == source
            for part in range(parts):
                moved = jnp.take_along_axis(
                    table_ref[source, part * 8 : part * 8 + 8, :],
                    lanes,
                    axis=1,
                    mode="promise_in_bounds",
                )
                total[part] = jnp.where(hit, moved, total[part])
        for part in range(parts):
            out_ref[k, part * 8 : part * 8 + 8, :] = total[part]
        return carry

    lax.fori_loop(0, count, one, 0)


def collect_kernel(s, in_ref, row_ref, lane_ref, out_ref, table):
    def take(comp, grp, turned):
        for member in range(s.group):
            block = grp * s.group + member
            table[block, comp * s.q : (comp + 1) * s.q, :] = turned[member * s.q : (member + 1) * s.q]

    load_tiles(s, in_ref, take)
    gather_rows(s, table, row_ref, lane_ref, out_ref, s.rows)


def collect(s, received, row, lane):
    return pl.pallas_call(
        functools.partial(collect_kernel, s),
        in_specs=[vmem_spec()] * 3,
        out_specs=vmem_spec(),
        out_shape=jax.ShapeDtypeStruct((s.rows, s.comps, LANES), jnp.float32),
        scratch_shapes=[pltpu.VMEM((s.blocks, s.comps, LANES), jnp.float32)],
        name="collect",
    )(received, row, lane)


PACK = 32
EDGE = LANES // PACK


def pack_kernel(s, body_ref, before_ref, after_ref, left_ref, right_ref):
    where = lax.broadcasted_iota(jnp.int32, (s.comps, LANES), 1) // EDGE
    packs = left_ref.shape[0]
    for pack in range(packs):
        left = jnp.zeros((s.comps, LANES), jnp.float32)
        right = jnp.zeros((s.comps, LANES), jnp.float32)
        for member in range(PACK):
            at = pack * PACK + member
            if at >= s.wide:
                break
            if at < s.depth:
                line = before_ref[at]
            elif at < s.depth + s.rows:
                line = body_ref[at - s.depth]
            else:
                line = after_ref[at - s.depth - s.rows]
            here = where == member
            left = jnp.where(here, pltpu.roll(line, member * EDGE, 1) if member else line, left)
            turn = (member + 1) * EDGE
            right = jnp.where(here, pltpu.roll(line, turn, 1) if turn < LANES else line, right)
        left_ref[pack] = left
        right_ref[pack] = right


def pack_edges(s, body, before, after):
    packs = -(-s.wide // PACK)
    shape = jax.ShapeDtypeStruct((packs, s.comps, LANES), jnp.float32)
    return pl.pallas_call(
        functools.partial(pack_kernel, s),
        in_specs=[vmem_spec()] * 3,
        out_specs=[vmem_spec()] * 2,
        out_shape=[shape, shape],
        name="pack_edges",
    )(body, before, after)


def sweeps_kernel(
    s, rhs_ref, before_ref, after_ref, left_ref, right_ref, coef_ref, row_ref, lane_ref,
    sol_ref, out_ref, wide, even, odd, final, back,
):
    lane = lax.broadcasted_iota(jnp.int32, (s.comps, LANES), 1)
    for at in range(s.wide):
        if at < s.depth:
            line = before_ref[at]
        elif at < s.depth + s.rows:
            line = rhs_ref[at - s.depth]
        else:
            line = after_ref[at - s.depth - s.rows]
        pack, member = divmod(at, PACK)
        past = right_ref[pack]
        if member:
            past = pltpu.roll(past, LANES - member * EDGE, 1)
        ahead = left_ref[pack]
        turn = (member + 1) * EDGE
        if turn < LANES:
            ahead = pltpu.roll(ahead, LANES - turn, 1)
        wide[at, :, 0:LANES] = line
        wide[at, :, LANES : 2 * LANES] = jnp.where(
            lane < s.depth, past, jnp.where(lane >= LANES - s.depth, ahead, 0.0)
        )

    q = s.q

    def coefficient(at, index, width):
        return coef_ref[at, index : index + 1, 0:width]

    def invert(at, total, width):
        fresh = []
        for comp in range(3):
            value = coefficient(at, comp * 3, width) * total[0]
            for source in range(1, 3):
                value = value + coefficient(at, comp * 3 + source, width) * total[source]
            fresh.append(value)
        return fresh

    def first(at, carry):
        total = [wide[at, comp * q : (comp + 1) * q, :] for comp in range(3)]
        fresh = invert(at, total, 2 * LANES)
        for comp in range(3):
            even[at, comp * q : (comp + 1) * q, :] = fresh[comp]
        return carry

    lax.fori_loop(0, s.wide, first, 0)

    def sweep(old, at, width):
        pieces = [[] for _ in range(4)]
        for source in range(3):
            part = slice(source * q, (source + 1) * q)
            pieces[0].append(old[at - 1, part, 0:width])
            pieces[1].append(old[at + 1, part, 0:width])
            here = old[at, part, :]
            pieces[2].append(pltpu.roll(here, 1, 1)[:, 0:width])
            pieces[3].append(pltpu.roll(here, 2 * LANES - 1, 1)[:, 0:width])
        total = []
        for comp in range(3):
            value = wide[at, comp * q : (comp + 1) * q, 0:width]
            for direction in range(4):
                for source in range(3):
                    index = 9 + (direction * 3 + comp) * 3 + source
                    value = value - coefficient(at, index, width) * pieces[direction][source]
            total.append(value)
        return invert(at, total, width)

    old, new = even, odd
    for inner in range(1, s.depth):
        def middle(at, carry, old=old, new=new):
            fresh = sweep(old, at, 2 * LANES)
            for comp in range(3):
                new[at, comp * q : (comp + 1) * q, :] = fresh[comp]
            return carry

        lax.fori_loop(inner, s.wide - inner, middle, 0)
        old, new = new, old

    def last(k, carry):
        fresh = sweep(old, k + s.depth, LANES)
        for comp in range(3):
            final[k, comp * q : (comp + 1) * q, :] = fresh[comp]
            for low in range(0, q, 8):
                start = (low * 3 + comp) * s.rows + k
                sol_ref[pl.ds(start, 8, stride=3 * s.rows), :] = fresh[comp][low : low + 8]
        return carry

    lax.fori_loop(0, s.rows, last, 0)

    gather_rows(s, final, row_ref, lane_ref, back, s.blocks)

    def tile_of(comp, grp):
        parts = []
        for member in range(s.group):
            parts.append(back[grp * s.group + member, comp * q : (comp + 1) * q, :])
        return jnp.concatenate(parts, axis=0)

    store_tiles(s, out_ref, tile_of)


def sweeps(s, rhs, before, after, left, right, coefs, row, lane):
    state = pltpu.VMEM((s.wide, s.comps, 2 * LANES), jnp.float32)
    tile = pltpu.VMEM((s.rows, s.comps, LANES), jnp.float32)
    return pl.pallas_call(
        functools.partial(sweeps_kernel, s),
        in_specs=[vmem_spec()] * 8,
        out_specs=[vmem_spec()] * 2,
        out_shape=[
            jax.ShapeDtypeStruct((s.q * 3 * s.rows, LANES), jnp.float32),
            jax.ShapeDtypeStruct((s.devices * s.per_peer, LANES), jnp.float32),
        ],
        scratch_shapes=[state, state, state, tile, tile],
        name="sweeps",
    )(rhs, before, after, left, right, coefs, row, lane)


def invert_kernel(count, slot_ref, out_ref):
    def some(at, carry):
        for step in range(8):
            k = at * 8 + step
            out_ref[slot_ref[k]] = k
        return carry

    lax.fori_loop(0, count // 8, some, 0)


def invert_permutation(slots):
    count = slots.shape[0]
    return pl.pallas_call(
        functools.partial(invert_kernel, count),
        in_specs=[pl.BlockSpec(memory_space=pltpu.SMEM)],
        out_specs=pl.BlockSpec(memory_space=pltpu.SMEM),
        out_shape=jax.ShapeDtypeStruct((count,), jnp.int32),
        name="invert_permutation",
    )(slots)


def ring(axis):
    count = lax.axis_size(axis)
    up = [(i, i + 1) for i in range(count - 1)]
    return up, [(j, i) for i, j in up]


def wide_coefficients(s, inverse, blocks, pattern):
    coupling = blocks * pattern.astype(jnp.float32)[:, None, None]
    coefs = jnp.concatenate([inverse.reshape(9, s.rows, s.cols), coupling.reshape(36, s.rows, s.cols)])
    coefs = coefs.transpose(1, 0, 2)
    up, down = ring("row")
    before = lax.ppermute(coefs[-s.depth :], "row", up)
    after = lax.ppermute(coefs[: s.depth], "row", down)
    coefs = jnp.concatenate([before, coefs, after])
    up, down = ring("col")
    ahead = lax.ppermute(coefs[..., -s.depth :].transpose(2, 1, 0), "col", up).transpose(2, 1, 0)
    past = lax.ppermute(coefs[..., : s.depth].transpose(2, 1, 0), "col", down).transpose(2, 1, 0)
    gap = jnp.zeros(coefs.shape[:2] + (LANES - 2 * s.depth,), jnp.float32)
    return jnp.concatenate([coefs, past, gap, ahead], axis=2)


def exchange(s, outgoing):
    blocks = outgoing.reshape(s.devices, s.per_peer, LANES)
    moved = lax.all_to_all(blocks, AXES, split_axis=0, concat_axis=0, tiled=True)
    return moved.reshape(s.devices * s.per_peer, LANES)


def body(
    fine_residual,
    restriction,
    restriction_pattern,
    cell_aggregate,
    block_inverse,
    off_blocks,
    operator_pattern,
):
    s = Sizes(
        fine_residual.shape[2],
        fine_residual.shape[0],
        cell_aggregate.shape[0],
        cell_aggregate.shape[1],
        lax.axis_size("row"),
        lax.axis_size("col"),
    )
    residual = fine_residual.transpose(1, 0, 2)
    pattern = restriction_pattern.reshape(1, -1)

    received = []
    for chunk in range(CHUNKS):
        received.append(exchange(s, restrict(s, residual, restriction, pattern, chunk)))

    owner = cell_aggregate // s.agg
    local = cell_aggregate % s.agg
    row = local // LANES
    lane = local % LANES // s.devices * s.devices + owner
    back = invert_permutation((row * LANES + lane).reshape(-1)).reshape(s.blocks, LANES)
    coefs = wide_coefficients(s, block_inverse, off_blocks, operator_pattern)

    row_up, row_down = ring("row")
    col_up, col_down = ring("col")
    solutions = []
    arrived = []
    for chunk in range(CHUNKS):
        rhs = collect(s, received[chunk], row, lane)
        before = lax.ppermute(rhs[-s.depth :], "row", row_up)
        after = lax.ppermute(rhs[: s.depth], "row", row_down)
        left, right = pack_edges(s, rhs, before, after)
        ahead = lax.ppermute(right, "col", col_up)
        past = lax.ppermute(left, "col", col_down)
        sol, outgoing = sweeps(s, rhs, before, after, ahead, past, coefs, back // LANES, back % LANES)
        solutions.append(sol.reshape(s.q, 3, s.rows, LANES))
        arrived.append(exchange(s, outgoing))
    correction = None
    for chunk in range(CHUNKS):
        correction = prolong(s, arrived[chunk], restriction, pattern, chunk, correction)
    return jnp.concatenate(solutions), correction.transpose(1, 0, 2)


def solution(mesh):
    in_specs = (
        P(None, None, AXES),
        P(None, None, AXES),
        P(AXES),
        P("row", "col"),
        P(None, None, "row", "col"),
        P(None, None, None, "row", "col"),
        P(None, "row", "col"),
    )
    out_specs = (P(None, None, "row", "col"), P(None, None, AXES))
    return jax.shard_map(body, mesh=mesh, in_specs=in_specs, out_specs=out_specs, check_vma=False)
```

```python
import functools

import jax
import jax.numpy as jnp
from jax import lax
from jax.experimental import pallas as pl
from jax.experimental.pallas import tpu as pltpu
from jax.sharding import PartitionSpec as P

FPA = 8
ITERS = 4
LANES = 128
CHUNKS = 1
UNROLL = 4
AXES = ("row", "col")


def vmem_spec():
    return pl.BlockSpec(memory_space=pltpu.VMEM)


class Sizes:
    def __init__(self, fine, loads, rows, cols, rows_n, cols_n):
        self.devices = rows_n * cols_n
        self.rows_n, self.cols_n = rows_n, cols_n
        self.fine = fine
        self.agg = fine // FPA
        self.blocks = self.agg // LANES
        self.loads = loads
        self.rows, self.cols = rows, cols
        self.q = loads // CHUNKS
        self.comps = 3 * self.q
        self.group = LANES // self.q
        self.groups = self.blocks // self.group
        self.low = LANES // self.devices
        self.per_peer = 3 * self.groups * self.low
        self.depth = ITERS - 1
        self.wide = rows + 2 * self.depth


def for_tiles(s, visit):
    for comp in range(3):
        for grp in range(s.groups):
            starts = []
            for low in range(s.low):
                slot = (comp * s.groups + grp) * s.low + low
                for first in range(0, s.devices, 8):
                    starts.append(first * s.per_peer + slot)
            visit(comp, grp, starts)


def store_tiles(s, out_ref, tile_of):
    def visit(comp, grp, starts):
        turned = tile_of(comp, grp).T
        for at, start in enumerate(starts):
            out_ref[pl.ds(start, 8, stride=s.per_peer), :] = turned[at * 8 : at * 8 + 8]

    for_tiles(s, visit)


def load_tiles(s, in_ref, take):
    def visit(comp, grp, starts):
        parts = [in_ref[pl.ds(start, 8, stride=s.per_peer), :] for start in starts]
        take(comp, grp, jnp.concatenate(parts, axis=0).T)

    for_tiles(s, visit)


def each_column(s, visit):
    def some(block, carry):
        for step in range(UNROLL):
            visit(pl.ds(pl.multiple_of((block * UNROLL + step) * LANES, LANES), LANES))
        return carry

    lax.fori_loop(0, s.blocks // UNROLL, some, 0)


def restrict_kernel(s, x_ref, rest_ref, pat_ref, out_ref, acc):
    step = pl.program_id(0)

    @pl.when(step == 0)
    def _():
        acc[...] = jnp.zeros_like(acc)

    def column(at):
        mask = pat_ref[0:1, at].astype(jnp.float32)
        value = [x_ref[comp, :, at] for comp in range(3)]
        for comp in range(3):
            total = acc[comp, :, at]
            for source in range(3):
                total = total + (rest_ref[comp, source : source + 1, at] * mask) * value[source]
            acc[comp, :, at] = total

    each_column(s, column)

    @pl.when(step == FPA - 1)
    def _():
        def tile_of(comp, grp):
            parts = []
            for member in range(s.group):
                low = (grp * s.group + member) * LANES
                parts.append(acc[comp, :, low : low + LANES])
            return jnp.concatenate(parts, axis=0)

        store_tiles(s, out_ref, tile_of)


def restrict(s, residual, restriction, pattern, chunk):
    return pl.pallas_call(
        functools.partial(restrict_kernel, s),
        grid=(FPA,),
        in_specs=[
            pl.BlockSpec((3, s.q, s.agg), lambda p: (0, chunk, p)),
            pl.BlockSpec((3, 3, s.agg), lambda p: (0, 0, p)),
            pl.BlockSpec((1, s.agg), lambda p: (0, p)),
        ],
        out_specs=pl.BlockSpec((s.devices * s.per_peer, LANES), lambda p: (0, 0)),
        out_shape=jax.ShapeDtypeStruct((s.devices * s.per_peer, LANES), jnp.float32),
        scratch_shapes=[pltpu.VMEM((3, s.q, s.agg), jnp.float32)],
        name="restrict",
    )(residual, restriction, pattern)


def prolong_kernel(s, in_ref, rest_ref, pat_ref, out_ref, agg):
    step = pl.program_id(0)

    @pl.when(step == 0)
    def _():
        def take(comp, grp, turned):
            for member in range(s.group):
                low = (grp * s.group + member) * LANES
                agg[comp, :, low : low + LANES] = turned[member * s.q : (member + 1) * s.q]

        load_tiles(s, in_ref, take)

    def column(at):
        mask = pat_ref[0:1, at].astype(jnp.float32)
        value = [agg[comp, :, at] for comp in range(3)]
        for comp in range(3):
            total = (rest_ref[0, comp : comp + 1, at] * mask) * value[0]
            for source in range(1, 3):
                total = total + (rest_ref[source, comp : comp + 1, at] * mask) * value[source]
            out_ref[comp, :, at] = total

    each_column(s, column)


def prolong(s, arrived, restriction, pattern, chunk, whole):
    kernel = functools.partial(prolong_kernel, s)
    specs = [
        vmem_spec(),
        pl.BlockSpec((3, 3, s.agg), lambda p: (0, 0, p)),
        pl.BlockSpec((1, s.agg), lambda p: (0, p)),
    ]
    args = [arrived, restriction, pattern]
    alias = {}
    body = kernel
    if whole is not None:
        specs.append(pl.BlockSpec(memory_space=pl.ANY))
        args.append(whole)
        alias = {3: 0}

        def body(in_ref, rest_ref, pat_ref, whole_ref, out_ref, agg):
            del whole_ref
            kernel(in_ref, rest_ref, pat_ref, out_ref, agg)

    return pl.pallas_call(
        body,
        grid=(FPA,),
        in_specs=specs,
        out_specs=pl.BlockSpec((3, s.q, s.agg), lambda p: (0, chunk, p)),
        out_shape=jax.ShapeDtypeStruct((3, s.loads, s.fine), jnp.float32),
        scratch_shapes=[pltpu.VMEM((3, s.q, s.agg), jnp.float32)],
        input_output_aliases=alias,
        name="prolong",
    )(*args)


def collect_kernel(s, slot_ref, in_ref, out_ref, table, lines, even, odd):
    def take(comp, grp, turned):
        for member in range(s.group):
            block = grp * s.group + member
            table[block, comp * s.q : (comp + 1) * s.q, :] = turned[member * s.q : (member + 1) * s.q]

    load_tiles(s, in_ref, take)
    for block in range(s.blocks):
        lines[block * LANES : (block + 1) * LANES, 0 : s.comps] = table[block].T

    def fetch(row, held):
        for lane in range(LANES):
            slot = slot_ref[row * LANES + lane]
            held[lane : lane + 1, :] = lines[pl.ds(slot, 1), :]

    def place(row, held):
        out_ref[row] = held[...].T[0 : s.comps]

    fetch(0, even)

    def two(k, carry):
        row = 2 * k
        fetch(row + 1, odd)
        place(row, even)
        fetch(jnp.minimum(row + 2, s.rows - 1), even)
        place(row + 1, odd)
        return carry

    lax.fori_loop(0, s.rows // 2, two, 0)


def line_scratch(s):
    return [
        pltpu.VMEM((s.blocks, s.comps, LANES), jnp.float32),
        pltpu.VMEM((s.agg, LANES), jnp.float32),
        pltpu.VMEM((LANES, LANES), jnp.float32),
        pltpu.VMEM((LANES, LANES), jnp.float32),
    ]


def collect(s, received, slots):
    return pl.pallas_call(
        functools.partial(collect_kernel, s),
        in_specs=[pl.BlockSpec(memory_space=pltpu.SMEM), vmem_spec()],
        out_specs=vmem_spec(),
        out_shape=jax.ShapeDtypeStruct((s.rows, s.comps, LANES), jnp.float32),
        scratch_shapes=line_scratch(s),
        name="collect",
    )(slots, received)


PACK = 32
EDGE = LANES // PACK


def pack_kernel(s, body_ref, before_ref, after_ref, left_ref, right_ref):
    where = lax.broadcasted_iota(jnp.int32, (s.comps, LANES), 1) // EDGE
    packs = left_ref.shape[0]
    for pack in range(packs):
        left = jnp.zeros((s.comps, LANES), jnp.float32)
        right = jnp.zeros((s.comps, LANES), jnp.float32)
        for member in range(PACK):
            at = pack * PACK + member
            if at >= s.wide:
                break
            if at < s.depth:
                line = before_ref[at]
            elif at < s.depth + s.rows:
                line = body_ref[at - s.depth]
            else:
                line = after_ref[at - s.depth - s.rows]
            here = where == member
            left = jnp.where(here, pltpu.roll(line, member * EDGE, 1) if member else line, left)
            turn = (member + 1) * EDGE
            right = jnp.where(here, pltpu.roll(line, turn, 1) if turn < LANES else line, right)
        left_ref[pack] = left
        right_ref[pack] = right


def pack_edges(s, body, before, after):
    packs = -(-s.wide // PACK)
    shape = jax.ShapeDtypeStruct((packs, s.comps, LANES), jnp.float32)
    return pl.pallas_call(
        functools.partial(pack_kernel, s),
        in_specs=[vmem_spec()] * 3,
        out_specs=[vmem_spec()] * 2,
        out_shape=[shape, shape],
        name="pack_edges",
    )(body, before, after)


def sweeps_kernel(
    s, slot_ref, rhs_ref, before_ref, after_ref, left_ref, right_ref, coef_ref,
    sol_ref, out_ref, wide, even, odd, final, table, lines, ahead_lines, behind_lines,
):
    lane = lax.broadcasted_iota(jnp.int32, (s.comps, LANES), 1)
    for at in range(s.wide):
        if at < s.depth:
            line = before_ref[at]
        elif at < s.depth + s.rows:
            line = rhs_ref[at - s.depth]
        else:
            line = after_ref[at - s.depth - s.rows]
        pack, member = divmod(at, PACK)
        past = right_ref[pack]
        if member:
            past = pltpu.roll(past, LANES - member * EDGE, 1)
        ahead = left_ref[pack]
        turn = (member + 1) * EDGE
        if turn < LANES:
            ahead = pltpu.roll(ahead, LANES - turn, 1)
        wide[at, :, 0:LANES] = line
        wide[at, :, LANES : 2 * LANES] = jnp.where(
            lane < s.depth, past, jnp.where(lane >= LANES - s.depth, ahead, 0.0)
        )

    q = s.q

    def coefficient(at, index, width):
        return coef_ref[at, index : index + 1, 0:width]

    def invert(at, total, width):
        fresh = []
        for comp in range(3):
            value = coefficient(at, comp * 3, width) * total[0]
            for source in range(1, 3):
                value = value + coefficient(at, comp * 3 + source, width) * total[source]
            fresh.append(value)
        return fresh

    def span(comp, low):
        return slice(comp * q + low, comp * q + low + 8)

    def first(at, carry):
        for low in range(0, q, 8):
            total = [wide[at, span(comp, low), :] for comp in range(3)]
            fresh = invert(at, total, 2 * LANES)
            for comp in range(3):
                even[at, span(comp, low), :] = fresh[comp]
        return carry

    lax.fori_loop(0, s.wide, first, 0)

    def sweep(old, at, low, width):
        pieces = [[] for _ in range(4)]
        for source in range(3):
            part = span(source, low)
            pieces[0].append(old[at - 1, part, 0:width])
            pieces[1].append(old[at + 1, part, 0:width])
            here = old[at, part, :]
            pieces[2].append(pltpu.roll(here, 1, 1)[:, 0:width])
            pieces[3].append(pltpu.roll(here, 2 * LANES - 1, 1)[:, 0:width])
        total = []
        for comp in range(3):
            value = wide[at, span(comp, low), 0:width]
            for direction in range(4):
                for source in range(3):
                    index = 9 + (direction * 3 + comp) * 3 + source
                    value = value - coefficient(at, index, width) * pieces[direction][source]
            total.append(value)
        return invert(at, total, width)

    old, new = even, odd
    for inner in range(1, s.depth):
        def middle(at, carry, old=old, new=new):
            for low in range(0, q, 8):
                fresh = sweep(old, at, low, 2 * LANES)
                for comp in range(3):
                    new[at, span(comp, low), :] = fresh[comp]
            return carry

        lax.fori_loop(inner, s.wide - inner, middle, 0)
        old, new = new, old

    def last(k, carry):
        for low in range(0, q, 8):
            fresh = sweep(old, k + s.depth, low, LANES)
            for comp in range(3):
                final[k, span(comp, low), :] = fresh[comp]
                start = (low * 3 + comp) * s.rows + k
                sol_ref[pl.ds(start, 8, stride=3 * s.rows), :] = fresh[comp]
        return carry

    lax.fori_loop(0, s.rows, last, 0)

    def turn_line(row, held):
        held[:, 0 : s.comps] = final[row].T

    def send(row, held):
        for lane in range(LANES):
            slot = slot_ref[row * LANES + lane]
            lines[pl.ds(slot, 1), :] = held[lane : lane + 1, :]

    turn_line(0, ahead_lines)

    def two(k, carry):
        row = 2 * k
        turn_line(row + 1, behind_lines)
        send(row, ahead_lines)
        turn_line(jnp.minimum(row + 2, s.rows - 1), ahead_lines)
        send(row + 1, behind_lines)
        return carry

    lax.fori_loop(0, s.rows // 2, two, 0)
    for block in range(s.blocks):
        table[block] = lines[block * LANES : (block + 1) * LANES, :].T[0 : s.comps]

    def tile_of(comp, grp):
        parts = []
        for member in range(s.group):
            parts.append(table[grp * s.group + member, comp * q : (comp + 1) * q, :])
        return jnp.concatenate(parts, axis=0)

    store_tiles(s, out_ref, tile_of)


def sweeps(s, slots, rhs, before, after, left, right, coefs):
    state = pltpu.VMEM((s.wide, s.comps, 2 * LANES), jnp.float32)
    tile = pltpu.VMEM((s.rows, s.comps, LANES), jnp.float32)
    return pl.pallas_call(
        functools.partial(sweeps_kernel, s),
        in_specs=[pl.BlockSpec(memory_space=pltpu.SMEM)] + [vmem_spec()] * 6,
        out_specs=[vmem_spec()] * 2,
        out_shape=[
            jax.ShapeDtypeStruct((s.q * 3 * s.rows, LANES), jnp.float32),
            jax.ShapeDtypeStruct((s.devices * s.per_peer, LANES), jnp.float32),
        ],
        scratch_shapes=[state, state, state, tile] + line_scratch(s),
        name="sweeps",
    )(slots, rhs, before, after, left, right, coefs)


def ring(axis):
    count = lax.axis_size(axis)
    up = [(i, i + 1) for i in range(count - 1)]
    return up, [(j, i) for i, j in up]


def wide_coefficients(s, inverse, blocks, pattern):
    coupling = blocks * pattern.astype(jnp.float32)[:, None, None]
    coefs = jnp.concatenate([inverse.reshape(9, s.rows, s.cols), coupling.reshape(36, s.rows, s.cols)])
    coefs = coefs.transpose(1, 0, 2)
    up, down = ring("row")
    before = lax.ppermute(coefs[-s.depth :], "row", up)
    after = lax.ppermute(coefs[: s.depth], "row", down)
    coefs = jnp.concatenate([before, coefs, after])
    up, down = ring("col")
    ahead = lax.ppermute(coefs[..., -s.depth :].transpose(2, 1, 0), "col", up).transpose(2, 1, 0)
    past = lax.ppermute(coefs[..., : s.depth].transpose(2, 1, 0), "col", down).transpose(2, 1, 0)
    gap = jnp.zeros(coefs.shape[:2] + (LANES - 2 * s.depth,), jnp.float32)
    return jnp.concatenate([coefs, past, gap, ahead], axis=2)


def exchange(s, outgoing):
    blocks = outgoing.reshape(s.devices, s.per_peer, LANES)
    moved = lax.all_to_all(blocks, AXES, split_axis=0, concat_axis=0, tiled=True)
    return moved.reshape(s.devices * s.per_peer, LANES)


def body(
    fine_residual,
    restriction,
    restriction_pattern,
    cell_aggregate,
    block_inverse,
    off_blocks,
    operator_pattern,
):
    s = Sizes(
        fine_residual.shape[2],
        fine_residual.shape[0],
        cell_aggregate.shape[0],
        cell_aggregate.shape[1],
        lax.axis_size("row"),
        lax.axis_size("col"),
    )
    residual = fine_residual.transpose(1, 0, 2)
    pattern = restriction_pattern.reshape(1, -1)

    received = []
    for chunk in range(CHUNKS):
        received.append(exchange(s, restrict(s, residual, restriction, pattern, chunk)))

    owner = cell_aggregate // s.agg
    local = cell_aggregate % s.agg
    row = local // LANES
    lane = local % LANES // s.devices * s.devices + owner
    slots = (row * LANES + lane).reshape(-1)
    coefs = wide_coefficients(s, block_inverse, off_blocks, operator_pattern)

    row_up, row_down = ring("row")
    col_up, col_down = ring("col")
    solutions = []
    arrived = []
    for chunk in range(CHUNKS):
        rhs = collect(s, received[chunk], slots)
        before = lax.ppermute(rhs[-s.depth :], "row", row_up)
        after = lax.ppermute(rhs[: s.depth], "row", row_down)
        left, right = pack_edges(s, rhs, before, after)
        ahead = lax.ppermute(right, "col", col_up)
        past = lax.ppermute(left, "col", col_down)
        sol, outgoing = sweeps(s, slots, rhs, before, after, ahead, past, coefs)
        solutions.append(sol.reshape(s.q, 3, s.rows, LANES))
        arrived.append(exchange(s, outgoing))
    correction = None
    for chunk in range(CHUNKS):
        correction = prolong(s, arrived[chunk], restriction, pattern, chunk, correction)
    return solutions[0] if CHUNKS == 1 else jnp.concatenate(solutions), correction.transpose(1, 0, 2)


def solution(mesh):
    in_specs = (
        P(None, None, AXES),
        P(None, None, AXES),
        P(AXES),
        P("row", "col"),
        P(None, None, "row", "col"),
        P(None, None, None, "row", "col"),
        P(None, "row", "col"),
    )
    out_specs = (P(None, None, "row", "col"), P(None, None, AXES))
    return jax.shard_map(body, mesh=mesh, in_specs=in_specs, out_specs=out_specs, check_vma=False)
```

```python
import functools

import jax
import jax.numpy as jnp
from jax import lax
from jax.experimental import pallas as pl
from jax.experimental.pallas import tpu as pltpu
from jax.sharding import PartitionSpec as P

FPA = 8
ITERS = 4
LANES = 128
CHUNKS = 1
UNROLL = 4
AXES = ("row", "col")


def vmem_spec():
    return pl.BlockSpec(memory_space=pltpu.VMEM)


KERNEL = pltpu.CompilerParams(vmem_limit_bytes=30 * 1024 * 1024)


def in_vmem(x):
    return pltpu.with_memory_space_constraint(x, pltpu.VMEM)


def vmem_result(*shape):
    return pltpu.VMEM(shape, jnp.float32)


class Sizes:
    def __init__(self, fine, loads, rows, cols, rows_n, cols_n):
        self.devices = rows_n * cols_n
        self.rows_n, self.cols_n = rows_n, cols_n
        self.fine = fine
        self.agg = fine // FPA
        self.blocks = self.agg // LANES
        self.loads = loads
        self.rows, self.cols = rows, cols
        self.q = loads // CHUNKS
        self.comps = 3 * self.q
        self.group = LANES // self.q
        self.groups = self.blocks // self.group
        self.low = LANES // self.devices
        self.per_peer = 3 * self.groups * self.low
        self.depth = ITERS - 1
        self.wide = rows + 2 * self.depth


def for_tiles(s, visit):
    for comp in range(3):
        for grp in range(s.groups):
            starts = []
            for low in range(s.low):
                slot = (comp * s.groups + grp) * s.low + low
                for first in range(0, s.devices, 8):
                    starts.append(first * s.per_peer + slot)
            visit(comp, grp, starts)


def store_tiles(s, out_ref, tile_of):
    def visit(comp, grp, starts):
        turned = tile_of(comp, grp).T
        for at, start in enumerate(starts):
            out_ref[pl.ds(start, 8, stride=s.per_peer), :] = turned[at * 8 : at * 8 + 8]

    for_tiles(s, visit)


def load_tiles(s, in_ref, take):
    def visit(comp, grp, starts):
        parts = [in_ref[pl.ds(start, 8, stride=s.per_peer), :] for start in starts]
        take(comp, grp, jnp.concatenate(parts, axis=0).T)

    for_tiles(s, visit)


def each_column(s, visit):
    def some(block, carry):
        for step in range(UNROLL):
            visit(pl.ds(pl.multiple_of((block * UNROLL + step) * LANES, LANES), LANES))
        return carry

    lax.fori_loop(0, s.blocks // UNROLL, some, 0)


def restrict_kernel(s, chunk, x_hbm, rest_hbm, pat_hbm, out_ref, x_ref, rest_ref, pat_ref, acc, sems):
    loads = pl.ds(chunk * s.q, s.q)
    copies = []
    for part in range(FPA):
        at = pl.ds(part * s.agg, s.agg)
        group = (
            pltpu.make_async_copy(rest_hbm.at[:, :, at], rest_ref.at[part], sems.at[part, 0]),
            pltpu.make_async_copy(pat_hbm.at[:, at], pat_ref.at[part], sems.at[part, 1]),
            pltpu.make_async_copy(x_hbm.at[:, loads, at], x_ref.at[part], sems.at[part, 2]),
        )
        for copy in group:
            copy.start()
        copies.append(group)

    for part in range(FPA):
        for copy in copies[part]:
            copy.wait()

        def column(at, part=part):
            mask = pat_ref[part, 0:1, at].astype(jnp.float32)
            value = [x_ref[part, comp, :, at] for comp in range(3)]
            for comp in range(3):
                total = (rest_ref[part, comp, 0:1, at] * mask) * value[0]
                for source in range(1, 3):
                    total = total + (rest_ref[part, comp, source : source + 1, at] * mask) * value[source]
                acc[comp, :, at] = total if part == 0 else acc[comp, :, at] + total

        each_column(s, column)

    def tile_of(comp, grp):
        parts = []
        for member in range(s.group):
            low = (grp * s.group + member) * LANES
            parts.append(acc[comp, :, low : low + LANES])
        return jnp.concatenate(parts, axis=0)

    store_tiles(s, out_ref, tile_of)


def restrict(s, residual, restriction, pattern, chunk):
    return pl.pallas_call(
        functools.partial(restrict_kernel, s, chunk),
        in_specs=[pl.BlockSpec(memory_space=pltpu.HBM)] * 3,
        out_specs=vmem_spec(),
        out_shape=vmem_result(s.devices * s.per_peer, LANES),
        scratch_shapes=[
            pltpu.VMEM((FPA, 3, s.q, s.agg), jnp.float32),
            pltpu.VMEM((FPA, 3, 3, s.agg), jnp.float32),
            pltpu.VMEM((FPA, 1, s.agg), jnp.int32),
            pltpu.VMEM((3, s.q, s.agg), jnp.float32),
            pltpu.SemaphoreType.DMA((FPA, 3)),
        ],
        name="restrict",
        compiler_params=KERNEL,
    )(*(pltpu.with_memory_space_constraint(x, pltpu.HBM) for x in (residual, restriction, pattern)))


def prolong_kernel(s, in_ref, rest_ref, pat_ref, out_hbm, agg, out_ref, sems):
    def take(comp, grp, turned):
        for member in range(s.group):
            low = (grp * s.group + member) * LANES
            agg[comp, :, low : low + LANES] = turned[member * s.q : (member + 1) * s.q]

    load_tiles(s, in_ref, take)
    copies = []
    for part in range(FPA):
        def column(at, part=part):
            there = pl.ds(pl.multiple_of(at.start + part * s.agg, LANES), LANES)
            mask = pat_ref[0:1, there].astype(jnp.float32)
            value = [agg[comp, :, at] for comp in range(3)]
            for comp in range(3):
                total = (rest_ref[0, comp : comp + 1, there] * mask) * value[0]
                for source in range(1, 3):
                    total = total + (rest_ref[source, comp : comp + 1, there] * mask) * value[source]
                out_ref[part, comp, :, at] = total

        each_column(s, column)
        copy = pltpu.make_async_copy(
            out_ref.at[part], out_hbm.at[:, :, pl.ds(part * s.agg, s.agg)], sems.at[part]
        )
        copy.start()
        copies.append(copy)
    for copy in copies:
        copy.wait()


def prolong(s, arrived, restriction, pattern):
    return pl.pallas_call(
        functools.partial(prolong_kernel, s),
        in_specs=[vmem_spec()] * 3,
        out_specs=pl.BlockSpec(memory_space=pltpu.HBM),
        out_shape=jax.ShapeDtypeStruct((3, s.loads, s.fine), jnp.float32),
        scratch_shapes=[
            pltpu.VMEM((3, s.q, s.agg), jnp.float32),
            pltpu.VMEM((FPA, 3, s.q, s.agg), jnp.float32),
            pltpu.SemaphoreType.DMA((FPA,)),
        ],
        name="prolong",
        compiler_params=KERNEL,
    )(in_vmem(arrived), in_vmem(restriction), in_vmem(pattern))


def collect_kernel(s, slot_ref, in_ref, out_ref, table, lines, even, odd):
    def take(comp, grp, turned):
        for member in range(s.group):
            block = grp * s.group + member
            table[block, comp * s.q : (comp + 1) * s.q, :] = turned[member * s.q : (member + 1) * s.q]

    load_tiles(s, in_ref, take)
    for block in range(s.blocks):
        lines[block * LANES : (block + 1) * LANES, 0 : s.comps] = table[block].T

    def fetch(row, held):
        for lane in range(LANES):
            slot = slot_ref[row * LANES + lane]
            held[lane : lane + 1, :] = lines[pl.ds(slot, 1), :]

    def place(row, held):
        out_ref[row] = held[...].T[0 : s.comps]

    fetch(0, even)

    def two(k, carry):
        row = 2 * k
        fetch(row + 1, odd)
        place(row, even)
        fetch(jnp.minimum(row + 2, s.rows - 1), even)
        place(row + 1, odd)
        return carry

    lax.fori_loop(0, s.rows // 2, two, 0)


def line_scratch(s):
    return [
        pltpu.VMEM((s.blocks, s.comps, LANES), jnp.float32),
        pltpu.VMEM((s.agg, LANES), jnp.float32),
        pltpu.VMEM((LANES, LANES), jnp.float32),
        pltpu.VMEM((LANES, LANES), jnp.float32),
    ]


def collect(s, received, slots):
    return pl.pallas_call(
        functools.partial(collect_kernel, s),
        in_specs=[pl.BlockSpec(memory_space=pltpu.SMEM), vmem_spec()],
        out_specs=vmem_spec(),
        out_shape=vmem_result(s.rows, s.comps, LANES),
        scratch_shapes=line_scratch(s),
        name="collect",
        compiler_params=KERNEL,
    )(slots, in_vmem(received))


PACK = 32
EDGE = LANES // PACK


def pack_kernel(s, body_ref, before_ref, after_ref, left_ref, right_ref):
    where = lax.broadcasted_iota(jnp.int32, (s.comps, LANES), 1) // EDGE
    packs = left_ref.shape[0]
    for pack in range(packs):
        left = jnp.zeros((s.comps, LANES), jnp.float32)
        right = jnp.zeros((s.comps, LANES), jnp.float32)
        for member in range(PACK):
            at = pack * PACK + member
            if at >= s.wide:
                break
            if at < s.depth:
                line = before_ref[at]
            elif at < s.depth + s.rows:
                line = body_ref[at - s.depth]
            else:
                line = after_ref[at - s.depth - s.rows]
            here = where == member
            left = jnp.where(here, pltpu.roll(line, member * EDGE, 1) if member else line, left)
            turn = (member + 1) * EDGE
            right = jnp.where(here, pltpu.roll(line, turn, 1) if turn < LANES else line, right)
        left_ref[pack] = left
        right_ref[pack] = right


def pack_edges(s, body, before, after):
    packs = -(-s.wide // PACK)
    shape = vmem_result(packs, s.comps, LANES)
    return pl.pallas_call(
        functools.partial(pack_kernel, s),
        in_specs=[vmem_spec()] * 3,
        out_specs=[vmem_spec()] * 2,
        out_shape=[shape, shape],
        name="pack_edges",
        compiler_params=KERNEL,
    )(body, in_vmem(before), in_vmem(after))


def sweeps_kernel(
    s, slot_ref, rhs_ref, before_ref, after_ref, left_ref, right_ref, coef_ref,
    sol_ref, out_ref, wide, even, odd, final, table, lines, ahead_lines, behind_lines,
):
    lane = lax.broadcasted_iota(jnp.int32, (s.comps, LANES), 1)
    for at in range(s.wide):
        if at < s.depth:
            line = before_ref[at]
        elif at < s.depth + s.rows:
            line = rhs_ref[at - s.depth]
        else:
            line = after_ref[at - s.depth - s.rows]
        pack, member = divmod(at, PACK)
        past = right_ref[pack]
        if member:
            past = pltpu.roll(past, LANES - member * EDGE, 1)
        ahead = left_ref[pack]
        turn = (member + 1) * EDGE
        if turn < LANES:
            ahead = pltpu.roll(ahead, LANES - turn, 1)
        wide[at, :, 0:LANES] = line
        wide[at, :, LANES : 2 * LANES] = jnp.where(
            lane < s.depth, past, jnp.where(lane >= LANES - s.depth, ahead, 0.0)
        )

    q = s.q

    def coefficient(at, index, width):
        return coef_ref[at, index : index + 1, 0:width]

    def invert(at, total, width):
        fresh = []
        for comp in range(3):
            value = coefficient(at, comp * 3, width) * total[0]
            for source in range(1, 3):
                value = value + coefficient(at, comp * 3 + source, width) * total[source]
            fresh.append(value)
        return fresh

    def span(comp, low):
        return slice(comp * q + low, comp * q + low + 8)

    def first(at, carry):
        for low in range(0, q, 8):
            total = [wide[at, span(comp, low), :] for comp in range(3)]
            fresh = invert(at, total, 2 * LANES)
            for comp in range(3):
                even[at, span(comp, low), :] = fresh[comp]
        return carry

    lax.fori_loop(0, s.wide, first, 0)

    def sweep(old, at, low, width):
        pieces = [[] for _ in range(4)]
        for source in range(3):
            part = span(source, low)
            pieces[0].append(old[at - 1, part, 0:width])
            pieces[1].append(old[at + 1, part, 0:width])
            here = old[at, part, :]
            pieces[2].append(pltpu.roll(here, 1, 1)[:, 0:width])
            pieces[3].append(pltpu.roll(here, 2 * LANES - 1, 1)[:, 0:width])
        total = []
        for comp in range(3):
            value = wide[at, span(comp, low), 0:width]
            for direction in range(4):
                for source in range(3):
                    index = 9 + (direction * 3 + comp) * 3 + source
                    value = value - coefficient(at, index, width) * pieces[direction][source]
            total.append(value)
        return invert(at, total, width)

    old, new = even, odd
    for inner in range(1, s.depth):
        def middle(at, carry, old=old, new=new):
            for low in range(0, q, 8):
                fresh = sweep(old, at, low, 2 * LANES)
                for comp in range(3):
                    new[at, span(comp, low), :] = fresh[comp]
            return carry

        lax.fori_loop(inner, s.wide - inner, middle, 0)
        old, new = new, old

    def last(k, carry):
        for low in range(0, q, 8):
            fresh = sweep(old, k + s.depth, low, LANES)
            for comp in range(3):
                final[k, span(comp, low), :] = fresh[comp]
                start = (low * 3 + comp) * s.rows + k
                sol_ref[pl.ds(start, 8, stride=3 * s.rows), :] = fresh[comp]
        return carry

    lax.fori_loop(0, s.rows, last, 0)

    def turn_line(row, held):
        held[:, 0 : s.comps] = final[row].T

    def send(row, held):
        for lane in range(LANES):
            slot = slot_ref[row * LANES + lane]
            lines[pl.ds(slot, 1), :] = held[lane : lane + 1, :]

    turn_line(0, ahead_lines)

    def two(k, carry):
        row = 2 * k
        turn_line(row + 1, behind_lines)
        send(row, ahead_lines)
        turn_line(jnp.minimum(row + 2, s.rows - 1), ahead_lines)
        send(row + 1, behind_lines)
        return carry

    lax.fori_loop(0, s.rows // 2, two, 0)
    for block in range(s.blocks):
        table[block] = lines[block * LANES : (block + 1) * LANES, :].T[0 : s.comps]

    def tile_of(comp, grp):
        parts = []
        for member in range(s.group):
            parts.append(table[grp * s.group + member, comp * q : (comp + 1) * q, :])
        return jnp.concatenate(parts, axis=0)

    store_tiles(s, out_ref, tile_of)


def sweeps(s, slots, rhs, before, after, left, right, coefs):
    state = pltpu.VMEM((s.wide, s.comps, 2 * LANES), jnp.float32)
    tile = pltpu.VMEM((s.rows, s.comps, LANES), jnp.float32)
    return pl.pallas_call(
        functools.partial(sweeps_kernel, s),
        in_specs=[pl.BlockSpec(memory_space=pltpu.SMEM)] + [vmem_spec()] * 6,
        out_specs=[vmem_spec()] * 2,
        out_shape=[
            jax.ShapeDtypeStruct((s.q * 3 * s.rows, LANES), jnp.float32),
            vmem_result(s.devices * s.per_peer, LANES),
        ],
        scratch_shapes=[state, state, state, tile] + line_scratch(s),
        name="sweeps",
        compiler_params=KERNEL,
    )(slots, rhs, *map(in_vmem, (before, after, left, right, coefs)))


def ring(axis):
    count = lax.axis_size(axis)
    up = [(i, i + 1) for i in range(count - 1)]
    return up, [(j, i) for i, j in up]


def wide_coefficients(s, inverse, blocks, pattern):
    coupling = blocks * pattern.astype(jnp.float32)[:, None, None]
    coefs = jnp.concatenate([inverse.reshape(9, s.rows, s.cols), coupling.reshape(36, s.rows, s.cols)])
    coefs = coefs.transpose(1, 0, 2)
    up, down = ring("row")
    before = lax.ppermute(coefs[-s.depth :], "row", up)
    after = lax.ppermute(coefs[: s.depth], "row", down)
    coefs = jnp.concatenate([before, coefs, after])
    up, down = ring("col")
    ahead = lax.ppermute(coefs[..., -s.depth :].transpose(2, 1, 0), "col", up).transpose(2, 1, 0)
    past = lax.ppermute(coefs[..., : s.depth].transpose(2, 1, 0), "col", down).transpose(2, 1, 0)
    gap = jnp.zeros(coefs.shape[:2] + (LANES - 2 * s.depth,), jnp.float32)
    return jnp.concatenate([coefs, past, gap, ahead], axis=2)


def exchange(s, outgoing):
    blocks = outgoing.reshape(s.devices, s.per_peer, LANES)
    moved = lax.all_to_all(blocks, AXES, split_axis=0, concat_axis=0, tiled=True)
    return moved.reshape(s.devices * s.per_peer, LANES)


def body(
    fine_residual,
    restriction,
    restriction_pattern,
    cell_aggregate,
    block_inverse,
    off_blocks,
    operator_pattern,
):
    s = Sizes(
        fine_residual.shape[2],
        fine_residual.shape[0],
        cell_aggregate.shape[0],
        cell_aggregate.shape[1],
        lax.axis_size("row"),
        lax.axis_size("col"),
    )
    residual = fine_residual.transpose(1, 0, 2)
    pattern = restriction_pattern.reshape(1, -1)

    received = []
    for chunk in range(CHUNKS):
        received.append(exchange(s, restrict(s, residual, restriction, pattern, chunk)))

    owner = cell_aggregate // s.agg
    local = cell_aggregate % s.agg
    row = local // LANES
    lane = local % LANES // s.devices * s.devices + owner
    slots = (row * LANES + lane).reshape(-1)
    coefs = wide_coefficients(s, block_inverse, off_blocks, operator_pattern)

    row_up, row_down = ring("row")
    col_up, col_down = ring("col")
    solutions = []
    arrived = []
    for chunk in range(CHUNKS):
        received[chunk], coefs = lax.optimization_barrier((received[chunk], coefs))
        rhs = collect(s, received[chunk], slots)
        before = lax.ppermute(rhs[-s.depth :], "row", row_up)
        after = lax.ppermute(rhs[: s.depth], "row", row_down)
        left, right = pack_edges(s, rhs, before, after)
        ahead = lax.ppermute(right, "col", col_up)
        past = lax.ppermute(left, "col", col_down)
        sol, outgoing = sweeps(s, slots, rhs, before, after, ahead, past, coefs)
        solutions.append(sol.reshape(s.q, 3, s.rows, LANES))
        arrived.append(exchange(s, outgoing))
    correction = prolong(s, arrived[0], restriction, pattern)
    return solutions[0] if CHUNKS == 1 else jnp.concatenate(solutions), correction.transpose(1, 0, 2)


def solution(mesh):
    in_specs = (
        P(None, None, AXES),
        P(None, None, AXES),
        P(AXES),
        P("row", "col"),
        P(None, None, "row", "col"),
        P(None, None, None, "row", "col"),
        P(None, "row", "col"),
    )
    out_specs = (P(None, None, "row", "col"), P(None, None, AXES))
    return jax.shard_map(body, mesh=mesh, in_specs=in_specs, out_specs=out_specs, check_vma=False)
```

```python
import functools

import jax
import jax.numpy as jnp
from jax import lax
from jax.experimental import pallas as pl
from jax.experimental.pallas import tpu as pltpu
from jax.sharding import PartitionSpec as P

FPA = 8
ITERS = 4
LANES = 128
CHUNKS = 1
UNROLL = 4
AXES = ("row", "col")


def vmem_spec():
    return pl.BlockSpec(memory_space=pltpu.VMEM)


KERNEL = pltpu.CompilerParams(vmem_limit_bytes=30 * 1024 * 1024)


def in_vmem(x):
    return pltpu.with_memory_space_constraint(x, pltpu.VMEM)


def vmem_result(*shape):
    return pltpu.VMEM(shape, jnp.float32)


class Sizes:
    def __init__(self, fine, loads, rows, cols, rows_n, cols_n):
        self.devices = rows_n * cols_n
        self.rows_n, self.cols_n = rows_n, cols_n
        self.fine = fine
        self.agg = fine // FPA
        self.blocks = self.agg // LANES
        self.loads = loads
        self.rows, self.cols = rows, cols
        self.q = loads // CHUNKS
        self.comps = 3 * self.q
        self.group = LANES // self.q
        self.groups = self.blocks // self.group
        self.low = LANES // self.devices
        self.per_peer = 3 * self.groups * self.low
        self.depth = ITERS - 1
        self.wide = rows + 2 * self.depth


def for_tiles(s, visit):
    for comp in range(3):
        for grp in range(s.groups):
            starts = []
            for low in range(s.low):
                slot = (comp * s.groups + grp) * s.low + low
                for first in range(0, s.devices, 8):
                    starts.append(first * s.per_peer + slot)
            visit(comp, grp, starts)


def store_tiles(s, out_ref, tile_of):
    def visit(comp, grp, starts):
        turned = tile_of(comp, grp).T
        for at, start in enumerate(starts):
            out_ref[pl.ds(start, 8, stride=s.per_peer), :] = turned[at * 8 : at * 8 + 8]

    for_tiles(s, visit)


def load_tiles(s, in_ref, take):
    def visit(comp, grp, starts):
        parts = [in_ref[pl.ds(start, 8, stride=s.per_peer), :] for start in starts]
        take(comp, grp, jnp.concatenate(parts, axis=0).T)

    for_tiles(s, visit)


def each_column(s, visit):
    def some(block, carry):
        for step in range(UNROLL):
            visit(pl.ds(pl.multiple_of((block * UNROLL + step) * LANES, LANES), LANES))
        return carry

    lax.fori_loop(0, s.blocks // UNROLL, some, 0)


def restrict_kernel(s, chunk, x_hbm, rest_hbm, pat_hbm, out_ref, x_ref, rest_ref, pat_ref, acc, sems):
    loads = pl.ds(chunk * s.q, s.q)
    copies = []
    for part in range(FPA):
        at = pl.ds(part * s.agg, s.agg)
        group = (
            pltpu.make_async_copy(rest_hbm.at[:, :, at], rest_ref.at[part], sems.at[part, 0]),
            pltpu.make_async_copy(pat_hbm.at[:, at], pat_ref.at[part], sems.at[part, 1]),
            pltpu.make_async_copy(x_hbm.at[:, loads, at], x_ref.at[part], sems.at[part, 2]),
        )
        for copy in group:
            copy.start()
        copies.append(group)

    for part in range(FPA):
        for copy in copies[part]:
            copy.wait()

        def column(at, part=part):
            mask = pat_ref[part, 0:1, at].astype(jnp.float32)
            value = [x_ref[part, comp, :, at] for comp in range(3)]
            for comp in range(3):
                total = (rest_ref[part, comp, 0:1, at] * mask) * value[0]
                for source in range(1, 3):
                    total = total + (rest_ref[part, comp, source : source + 1, at] * mask) * value[source]
                acc[comp, :, at] = total if part == 0 else acc[comp, :, at] + total

        each_column(s, column)

    def tile_of(comp, grp):
        parts = []
        for member in range(s.group):
            low = (grp * s.group + member) * LANES
            parts.append(acc[comp, :, low : low + LANES])
        return jnp.concatenate(parts, axis=0)

    store_tiles(s, out_ref, tile_of)


def restrict(s, residual, restriction, pattern, chunk):
    return pl.pallas_call(
        functools.partial(restrict_kernel, s, chunk),
        in_specs=[pl.BlockSpec(memory_space=pltpu.HBM)] * 3,
        out_specs=vmem_spec(),
        out_shape=vmem_result(s.devices * s.per_peer, LANES),
        scratch_shapes=[
            pltpu.VMEM((FPA, 3, s.q, s.agg), jnp.float32),
            pltpu.VMEM((FPA, 3, 3, s.agg), jnp.float32),
            pltpu.VMEM((FPA, 1, s.agg), jnp.int32),
            pltpu.VMEM((3, s.q, s.agg), jnp.float32),
            pltpu.SemaphoreType.DMA((FPA, 3)),
        ],
        name="restrict",
        compiler_params=KERNEL,
    )(*(pltpu.with_memory_space_constraint(x, pltpu.HBM) for x in (residual, restriction, pattern)))


def prolong_kernel(s, in_ref, rest_ref, pat_ref, out_hbm, agg, out_ref, sems):
    def take(comp, grp, turned):
        for member in range(s.group):
            low = (grp * s.group + member) * LANES
            agg[comp, :, low : low + LANES] = turned[member * s.q : (member + 1) * s.q]

    load_tiles(s, in_ref, take)
    copies = []
    for part in range(FPA):
        def column(at, part=part):
            there = pl.ds(pl.multiple_of(at.start + part * s.agg, LANES), LANES)
            mask = pat_ref[0:1, there].astype(jnp.float32)
            value = [agg[comp, :, at] for comp in range(3)]
            for comp in range(3):
                total = (rest_ref[0, comp : comp + 1, there] * mask) * value[0]
                for source in range(1, 3):
                    total = total + (rest_ref[source, comp : comp + 1, there] * mask) * value[source]
                out_ref[part, comp, :, at] = total

        each_column(s, column)
        copy = pltpu.make_async_copy(
            out_ref.at[part], out_hbm.at[:, :, pl.ds(part * s.agg, s.agg)], sems.at[part]
        )
        copy.start()
        copies.append(copy)
    for copy in copies:
        copy.wait()


def prolong(s, arrived, restriction, pattern):
    return pl.pallas_call(
        functools.partial(prolong_kernel, s),
        in_specs=[vmem_spec()] * 3,
        out_specs=pl.BlockSpec(memory_space=pltpu.HBM),
        out_shape=jax.ShapeDtypeStruct((3, s.loads, s.fine), jnp.float32),
        scratch_shapes=[
            pltpu.VMEM((3, s.q, s.agg), jnp.float32),
            pltpu.VMEM((FPA, 3, s.q, s.agg), jnp.float32),
            pltpu.SemaphoreType.DMA((FPA,)),
        ],
        name="prolong",
        compiler_params=KERNEL,
    )(in_vmem(arrived), in_vmem(restriction), in_vmem(pattern))


def collect_kernel(s, slot_ref, in_ref, out_ref, table, lines, even, odd):
    def take(comp, grp, turned):
        for member in range(s.group):
            block = grp * s.group + member
            table[block, comp * s.q : (comp + 1) * s.q, :] = turned[member * s.q : (member + 1) * s.q]

    load_tiles(s, in_ref, take)
    for block in range(s.blocks):
        lines[block * LANES : (block + 1) * LANES, 0 : s.comps] = table[block].T

    def fetch(row, held):
        for lane in range(LANES):
            slot = slot_ref[row * LANES + lane]
            held[lane : lane + 1, :] = lines[pl.ds(slot, 1), :]

    def place(row, held):
        out_ref[row] = held[...].T[0 : s.comps]

    fetch(0, even)

    def two(k, carry):
        row = 2 * k
        fetch(row + 1, odd)
        place(row, even)
        fetch(jnp.minimum(row + 2, s.rows - 1), even)
        place(row + 1, odd)
        return carry

    lax.fori_loop(0, s.rows // 2, two, 0)


def line_scratch(s):
    return [
        pltpu.VMEM((s.blocks, s.comps, LANES), jnp.float32),
        pltpu.VMEM((s.agg, LANES), jnp.float32),
        pltpu.VMEM((LANES, LANES), jnp.float32),
        pltpu.VMEM((LANES, LANES), jnp.float32),
    ]


def collect(s, received, slots):
    return pl.pallas_call(
        functools.partial(collect_kernel, s),
        in_specs=[pl.BlockSpec(memory_space=pltpu.SMEM), vmem_spec()],
        out_specs=vmem_spec(),
        out_shape=vmem_result(s.rows, s.comps, LANES),
        scratch_shapes=line_scratch(s),
        name="collect",
        compiler_params=KERNEL,
    )(slots, in_vmem(received))


PACK = 32
EDGE = LANES // PACK


def pack_lines(line_of, count, left_ref, right_ref):
    for pack in range(left_ref.shape[0]):
        left = right = None
        for member in range(min(PACK, count - pack * PACK)):
            line = line_of(pack * PACK + member)
            head = pltpu.roll(line, member * EDGE, 1) if member else line
            turn = (member + 1) * EDGE
            tail = pltpu.roll(line, turn, 1) if turn < LANES else line
            if left is None:
                here = lax.broadcasted_iota(jnp.int32, line.shape, 1) // EDGE
                left, right = head, tail
            else:
                left = jnp.where(here == member, head, left)
                right = jnp.where(here == member, tail, right)
        left_ref[pack] = left
        right_ref[pack] = right


def beyond(past, ahead, member, depth):
    if member:
        past = pltpu.roll(past, LANES - member * EDGE, 1)
    turn = (member + 1) * EDGE
    if turn < LANES:
        ahead = pltpu.roll(ahead, LANES - turn, 1)
    lane = lax.broadcasted_iota(jnp.int32, past.shape, 1)
    return jnp.where(lane < depth, past, jnp.where(lane >= LANES - depth, ahead, 0.0))


def pack_kernel(s, body_ref, before_ref, after_ref, left_ref, right_ref):
    def line_of(at):
        if at < s.depth:
            return before_ref[at]
        if at < s.depth + s.rows:
            return body_ref[at - s.depth]
        return after_ref[at - s.depth - s.rows]

    pack_lines(line_of, s.wide, left_ref, right_ref)


def pack_edges(s, body, before, after):
    packs = -(-s.wide // PACK)
    shape = vmem_result(packs, s.comps, LANES)
    return pl.pallas_call(
        functools.partial(pack_kernel, s),
        in_specs=[vmem_spec()] * 3,
        out_specs=[vmem_spec()] * 2,
        out_shape=[shape, shape],
        name="pack_edges",
        compiler_params=KERNEL,
    )(body, in_vmem(before), in_vmem(after))


COEFS = 48


def prepare_kernel(s, inv_ref, off_ref, pat_ref, body_ref, top_ref, bottom_ref, left_ref, right_ref, flat):
    rows = s.rows
    flat[0 : 9 * rows, :] = inv_ref[...]
    for direction in range(4):
        mask = pat_ref[direction * rows : (direction + 1) * rows, :].astype(jnp.float32)
        for entry in range(9):
            at = direction * 9 + entry
            flat[(9 + at) * rows : (10 + at) * rows, :] = off_ref[at * rows : (at + 1) * rows, :] * mask
    flat[45 * rows : COEFS * rows, :] = jnp.zeros(((COEFS - 45) * rows, LANES), jnp.float32)

    def one(row, carry):
        for low in range(0, COEFS, 8):
            body_ref[row, low : low + 8, :] = flat[pl.ds(low * rows + row, 8, stride=rows), :]
        return carry

    lax.fori_loop(0, rows, one, 0)
    top_ref[...] = body_ref[0 : s.depth]
    bottom_ref[...] = body_ref[rows - s.depth : rows]
    pack_lines(lambda at: body_ref[at], rows, left_ref, right_ref)


def prepare(s, inverse, blocks, pattern):
    packs = vmem_result(-(-s.rows // PACK), COEFS, LANES)
    edge = vmem_result(s.depth, COEFS, LANES)
    return pl.pallas_call(
        functools.partial(prepare_kernel, s),
        in_specs=[vmem_spec()] * 3,
        out_specs=[vmem_spec()] * 5,
        out_shape=[vmem_result(s.rows, COEFS, LANES), edge, edge, packs, packs],
        scratch_shapes=[pltpu.VMEM((COEFS * s.rows, LANES), jnp.float32)],
        name="prepare",
        compiler_params=KERNEL,
    )(inverse.reshape(-1, LANES), blocks.reshape(-1, LANES), pattern.reshape(-1, LANES))


def widen_kernel(
    s, body_ref, before_ref, after_ref, past_ref, ahead_ref,
    before_past_ref, before_ahead_ref, after_past_ref, after_ahead_ref, out_ref,
):
    last = (s.rows - s.depth) % PACK
    for at in range(s.wide):
        row = at - s.depth
        if row < 0:
            line = before_ref[at]
            side = beyond(before_past_ref[0], before_ahead_ref[0], last + at, s.depth)
        elif row < s.rows:
            line = body_ref[row]
            side = beyond(past_ref[row // PACK], ahead_ref[row // PACK], row % PACK, s.depth)
        else:
            line = after_ref[row - s.rows]
            side = beyond(after_past_ref[0], after_ahead_ref[0], row - s.rows, s.depth)
        out_ref[at, :, 0:LANES] = line
        out_ref[at, :, LANES : 2 * LANES] = side


def widen(s, *parts):
    return pl.pallas_call(
        functools.partial(widen_kernel, s),
        in_specs=[vmem_spec()] * 9,
        out_specs=vmem_spec(),
        out_shape=vmem_result(s.wide, COEFS, 2 * LANES),
        name="widen",
        compiler_params=KERNEL,
    )(*map(in_vmem, parts))


def sweeps_kernel(
    s, slot_ref, rhs_ref, before_ref, after_ref, past_ref, ahead_ref, coef_ref,
    sol_ref, out_ref, wide, even, odd, table, lines, ahead_lines, behind_lines,
):
    q = s.q
    halves = range(0, q, 8)
    for at in range(s.wide):
        if at < s.depth:
            line = before_ref[at]
        elif at < s.depth + s.rows:
            line = rhs_ref[at - s.depth]
        else:
            line = after_ref[at - s.depth - s.rows]
        pack, member = divmod(at, PACK)
        wide[at, :, 0:LANES] = line
        wide[at, :, LANES : 2 * LANES] = beyond(past_ref[pack], ahead_ref[pack], member, s.depth)

    lane = lax.broadcasted_iota(jnp.int32, (8, LANES), 1)
    is_first = lane == 0
    is_last = lane == LANES - 1
    columns = (slice(0, LANES), slice(LANES, 2 * LANES))

    def span(comp, low):
        return slice(comp * q + low, comp * q + low + 8)

    def invert(at, total, column):
        fresh = []
        for comp in range(3):
            value = [None] * len(halves)
            for source in range(3):
                index = comp * 3 + source
                factor = coef_ref[at, index : index + 1, column]
                for half in range(len(halves)):
                    term = factor * total[source][half]
                    value[half] = term if source == 0 else value[half] + term
            fresh.append(value)
        return fresh

    def put(target, at, fresh, column):
        for comp in range(3):
            for half, low in enumerate(halves):
                target[at, span(comp, low), column] = fresh[comp][half]

    def first(at, carry):
        for column in columns:
            total = [[wide[at, span(comp, low), column] for low in halves] for comp in range(3)]
            put(even, at, invert(at, total, column), column)
        return carry

    lax.fori_loop(0, s.wide, first, 0)

    def turned(old, at):
        west = ([], [])
        east = ([], [])
        for comp in range(3):
            for side in west + east:
                side.append([])
            for low in halves:
                here = [old[at, span(comp, low), column] for column in columns]
                up = [pltpu.roll(x, 1, 1) for x in here]
                down = [pltpu.roll(x, LANES - 1, 1) for x in here]
                for v in range(2):
                    west[v][-1].append(jnp.where(is_first, up[1 - v], up[v]))
                    east[v][-1].append(jnp.where(is_last, down[1 - v], down[v]))
        return west, east

    def sweep(old, at, count):
        west, east = turned(old, at)
        result = []
        for v in range(count):
            column = columns[v]
            pieces = []
            for where in (at - 1, at + 1):
                pieces.append([[old[where, span(comp, low), column] for low in halves] for comp in range(3)])
            pieces += [west[v], east[v]]
            total = []
            for comp in range(3):
                value = [wide[at, span(comp, low), column] for low in halves]
                for direction in range(4):
                    for source in range(3):
                        index = 9 + (direction * 3 + comp) * 3 + source
                        factor = coef_ref[at, index : index + 1, column]
                        for half in range(len(halves)):
                            value[half] = value[half] - factor * pieces[direction][source][half]
                total.append(value)
            result.append(invert(at, total, column))
        return result

    old, new = even, odd
    for inner in range(1, s.depth):
        def middle(k, carry, old=old, new=new, inner=inner):
            for step in range(2):
                at = inner + 2 * k + step
                for column, fresh in zip(columns, sweep(old, at, 2)):
                    put(new, at, fresh, column)
            return carry

        lax.fori_loop(0, (s.wide - 2 * inner) // 2, middle, 0)
        old, new = new, old

    def finish(row, held):
        (fresh,) = sweep(old, row + s.depth, 1)
        put(sol_ref, row, fresh, columns[0])
        parts = [fresh[comp][half] for comp in range(3) for half in range(len(halves))]
        held[:, 0 : s.comps] = jnp.concatenate(parts, axis=0).T

    def send(row, held):
        for column in range(LANES):
            slot = slot_ref[row * LANES + column]
            lines[pl.ds(slot, 1), :] = held[column : column + 1, :]

    finish(0, ahead_lines)
    finish(1, behind_lines)

    def two(k, carry):
        row = 2 * k
        send(row, ahead_lines)
        send(row + 1, behind_lines)
        finish(row + 2, ahead_lines)
        finish(row + 3, behind_lines)
        return carry

    lax.fori_loop(0, s.rows // 2 - 1, two, 0)
    send(s.rows - 2, ahead_lines)
    send(s.rows - 1, behind_lines)
    for block in range(s.blocks):
        table[block] = lines[block * LANES : (block + 1) * LANES, :].T[0 : s.comps]

    def tile_of(comp, grp):
        parts = []
        for member in range(s.group):
            parts.append(table[grp * s.group + member, comp * q : (comp + 1) * q, :])
        return jnp.concatenate(parts, axis=0)

    store_tiles(s, out_ref, tile_of)


def sweeps(s, slots, rhs, before, after, past, ahead, coefs):
    state = pltpu.VMEM((s.wide, s.comps, 2 * LANES), jnp.float32)
    return pl.pallas_call(
        functools.partial(sweeps_kernel, s),
        in_specs=[pl.BlockSpec(memory_space=pltpu.SMEM)] + [vmem_spec()] * 6,
        out_specs=[vmem_spec()] * 2,
        out_shape=[
            vmem_result(s.rows, s.comps, LANES),
            vmem_result(s.devices * s.per_peer, LANES),
        ],
        scratch_shapes=[state, state, state] + line_scratch(s),
        name="sweeps",
        compiler_params=KERNEL,
    )(slots, rhs, *map(in_vmem, (before, after, past, ahead)), coefs)


def ring(axis):
    count = lax.axis_size(axis)
    up = [(i, i + 1) for i in range(count - 1)]
    return up, [(j, i) for i, j in up]


def shifted(x, down, right):
    rows, cols = lax.axis_size("row"), lax.axis_size("col")
    pairs = []
    for i in range(rows):
        for j in range(cols):
            if 0 <= i + down < rows and 0 <= j + right < cols:
                pairs.append((i * cols + j, (i + down) * cols + j + right))
    return lax.ppermute(x, AXES, pairs)


def wide_coefficients(s, inverse, blocks, pattern):
    body, top, bottom, left, right = prepare(s, inverse, blocks, pattern)
    head, tail = slice(0, 1), slice(-1, None)
    return widen(
        s,
        body,
        shifted(bottom, 1, 0),
        shifted(top, -1, 0),
        shifted(left, 0, -1),
        shifted(right, 0, 1),
        shifted(left[tail], 1, -1),
        shifted(right[tail], 1, 1),
        shifted(left[head], -1, -1),
        shifted(right[head], -1, 1),
    )


def exchange(s, outgoing):
    blocks = outgoing.reshape(s.devices, s.per_peer, LANES)
    moved = lax.all_to_all(blocks, AXES, split_axis=0, concat_axis=0, tiled=True)
    return moved.reshape(s.devices * s.per_peer, LANES)


def body(
    fine_residual,
    restriction,
    restriction_pattern,
    cell_aggregate,
    block_inverse,
    off_blocks,
    operator_pattern,
):
    s = Sizes(
        fine_residual.shape[2],
        fine_residual.shape[0],
        cell_aggregate.shape[0],
        cell_aggregate.shape[1],
        lax.axis_size("row"),
        lax.axis_size("col"),
    )
    residual = fine_residual.transpose(1, 0, 2)
    pattern = restriction_pattern.reshape(1, -1)

    received = []
    for chunk in range(CHUNKS):
        received.append(exchange(s, restrict(s, residual, restriction, pattern, chunk)))

    owner = cell_aggregate // s.agg
    local = cell_aggregate % s.agg
    row = local // LANES
    lane = local % LANES // s.devices * s.devices + owner
    slots = (row * LANES + lane).reshape(-1)
    coefs = wide_coefficients(s, block_inverse, off_blocks, operator_pattern)

    row_up, row_down = ring("row")
    col_up, col_down = ring("col")
    solutions = []
    arrived = []
    for chunk in range(CHUNKS):
        received[chunk], coefs = lax.optimization_barrier((received[chunk], coefs))
        rhs = collect(s, received[chunk], slots)
        before = lax.ppermute(rhs[-s.depth :], "row", row_up)
        after = lax.ppermute(rhs[: s.depth], "row", row_down)
        left, right = pack_edges(s, rhs, before, after)
        ahead = lax.ppermute(right, "col", col_up)
        past = lax.ppermute(left, "col", col_down)
        sol, outgoing = sweeps(s, slots, rhs, before, after, past, ahead, coefs)
        solutions.append(sol.reshape(s.rows, 3, s.q, LANES).transpose(2, 1, 0, 3))
        arrived.append(exchange(s, outgoing))
    correction = prolong(s, arrived[0], restriction, pattern)
    return solutions[0] if CHUNKS == 1 else jnp.concatenate(solutions), correction.transpose(1, 0, 2)


def solution(mesh):
    in_specs = (
        P(None, None, AXES),
        P(None, None, AXES),
        P(AXES),
        P("row", "col"),
        P(None, None, "row", "col"),
        P(None, None, None, "row", "col"),
        P(None, "row", "col"),
    )
    out_specs = (P(None, None, "row", "col"), P(None, None, AXES))
    return jax.shard_map(body, mesh=mesh, in_specs=in_specs, out_specs=out_specs, check_vma=False)
```

```python
import functools
import math

import jax
import jax.numpy as jnp
from jax import lax
from jax.experimental import pallas as pl
from jax.experimental.pallas import tpu as pltpu
from jax.sharding import PartitionSpec as P

FPA = 8
ITERS = 4
LANES = 128
UNROLL = 4
AXES = ("row", "col")


def vmem_spec():
    return pl.BlockSpec(memory_space=pltpu.VMEM)


KERNEL = pltpu.CompilerParams(vmem_limit_bytes=30 * 1024 * 1024)


def in_vmem(x):
    return pltpu.with_memory_space_constraint(x, pltpu.VMEM)


def in_hbm(x):
    return pltpu.with_memory_space_constraint(x, pltpu.HBM)


def vmem_result(*shape):
    return pltpu.VMEM(shape, jnp.float32)


class Sizes:
    def __init__(self, fine, loads, rows, cols, rows_n, cols_n):
        self.devices = rows_n * cols_n
        self.rows_n, self.cols_n = rows_n, cols_n
        self.fine = fine
        self.agg = fine // FPA
        self.blocks = self.agg // LANES
        self.loads = loads
        self.rows, self.cols = rows, cols
        self.q = loads
        self.comps = 3 * self.q
        self.group = LANES // math.gcd(self.comps, LANES)
        self.groups = self.blocks // self.group
        self.tiles = self.group * self.comps // LANES
        self.low = LANES // self.devices
        self.per_peer = self.tiles * self.groups * self.low
        self.depth = ITERS - 1
        self.wide = rows + 2 * self.depth


def starts(s, grp, tile):
    for low in range(s.low):
        slot = (grp * s.tiles + tile) * s.low + low
        for first in range(0, s.devices, 8):
            yield low * s.devices + first, first * s.per_peer + slot


def pieces(s, grp):
    for member in range(s.group):
        done = 0
        while done < s.comps:
            at = member * s.comps + done
            size = min(s.comps - done, LANES - at % LANES)
            yield at // LANES, at % LANES, member, done, size
            done += size


def store_tiles(s, out_ref, rows_of):
    for grp in range(s.groups):
        rows = jnp.concatenate([rows_of(grp * s.group + member) for member in range(s.group)], axis=0)
        for tile in range(s.tiles):
            turned = rows[tile * LANES : (tile + 1) * LANES].T
            for lane, start in starts(s, grp, tile):
                out_ref[pl.ds(start, 8, stride=s.per_peer), :] = turned[lane : lane + 8]


def load_tiles(s, in_ref, take):
    for grp in range(s.groups):
        turned = []
        for tile in range(s.tiles):
            parts = [in_ref[pl.ds(start, 8, stride=s.per_peer), :] for _, start in starts(s, grp, tile)]
            turned.append(jnp.concatenate(parts, axis=0).T)
        rows = jnp.concatenate(turned, axis=0)
        for member in range(s.group):
            take(grp * s.group + member, rows[member * s.comps : (member + 1) * s.comps])


def turn(x, by):
    return pltpu.roll(x, by % LANES, 1) if by % LANES else x


def lines_from_tiles(s, in_ref, lines):
    where = lax.broadcasted_iota(jnp.int32, (8, LANES), 1)
    for grp in range(s.groups):
        runs = [dict(starts(s, grp, tile)) for tile in range(s.tiles)]
        for lane in runs[0]:
            held = [in_ref[pl.ds(run[lane], 8, stride=s.per_peer), :] for run in runs]
            made = {}
            for tile, low, member, done, size in pieces(s, grp):
                part = turn(held[tile], done - low)
                made[member] = jnp.where(where >= done, part, made[member]) if member in made else part
            for member, line in made.items():
                row = (grp * s.group + member) * LANES + lane
                lines[row : row + 8, :] = line


def tiles_from_lines(s, lines, out_ref):
    where = lax.broadcasted_iota(jnp.int32, (8, LANES), 1)
    for grp in range(s.groups):
        runs = [dict(starts(s, grp, tile)) for tile in range(s.tiles)]
        for lane in runs[0]:
            held = []
            for member in range(s.group):
                row = (grp * s.group + member) * LANES + lane
                held.append(lines[row : row + 8, :])
            made = {}
            for tile, low, member, done, size in pieces(s, grp):
                part = turn(held[member], low - done)
                made[tile] = jnp.where(where >= low, part, made[tile]) if tile in made else part
            for tile, value in made.items():
                out_ref[pl.ds(runs[tile][lane], 8, stride=s.per_peer), :] = value


def each_column(s, visit):
    def some(block, carry):
        for step in range(UNROLL):
            visit(pl.ds(pl.multiple_of((block * UNROLL + step) * LANES, LANES), LANES))
        return carry

    lax.fori_loop(0, s.blocks // UNROLL, some, 0)


def restrict_kernel(s, x_hbm, rest_hbm, pat_hbm, out_ref, x_ref, rest_ref, pat_ref, acc, sems):
    copies = []
    for part in range(FPA):
        at = pl.ds(part * s.agg, s.agg)
        group = (
            pltpu.make_async_copy(rest_hbm.at[:, :, at], rest_ref.at[part], sems.at[part, 0]),
            pltpu.make_async_copy(pat_hbm.at[:, at], pat_ref.at[part], sems.at[part, 1]),
            pltpu.make_async_copy(x_hbm.at[:, :, at], x_ref.at[part], sems.at[part, 2]),
        )
        for copy in group:
            copy.start()
        copies.append(group)

    for part in range(FPA):
        for copy in copies[part]:
            copy.wait()

        def column(at, part=part):
            mask = pat_ref[part, 0:1, at].astype(jnp.float32)
            value = [x_ref[part, comp, :, at] for comp in range(3)]
            for comp in range(3):
                total = (rest_ref[part, comp, 0:1, at] * mask) * value[0]
                for source in range(1, 3):
                    total = total + (rest_ref[part, comp, source : source + 1, at] * mask) * value[source]
                acc[comp, :, at] = total if part == 0 else acc[comp, :, at] + total

        each_column(s, column)

    def rows_of(block):
        return jnp.concatenate([acc[comp, :, block * LANES : (block + 1) * LANES] for comp in range(3)], axis=0)

    store_tiles(s, out_ref, rows_of)


def restrict(s, residual, restriction, pattern):
    return pl.pallas_call(
        functools.partial(restrict_kernel, s),
        in_specs=[pl.BlockSpec(memory_space=pltpu.HBM)] * 3,
        out_specs=vmem_spec(),
        out_shape=vmem_result(s.devices * s.per_peer, LANES),
        scratch_shapes=[
            pltpu.VMEM((FPA, 3, s.q, s.agg), jnp.float32),
            pltpu.VMEM((FPA, 3, 3, s.agg), jnp.float32),
            pltpu.VMEM((FPA, 1, s.agg), jnp.int32),
            pltpu.VMEM((3, s.q, s.agg), jnp.float32),
            pltpu.SemaphoreType.DMA((FPA, 3)),
        ],
        name="restrict",
        compiler_params=KERNEL,
    )(*map(in_hbm, (residual, restriction, pattern)))


def prolong_kernel(s, in_ref, rest_ref, pat_hbm, out_hbm, agg, out_ref, pat_ref, sems):
    fetch = pltpu.make_async_copy(pat_hbm, pat_ref, sems.at[FPA])
    fetch.start()

    def take(block, rows):
        for comp in range(3):
            agg[comp, :, block * LANES : (block + 1) * LANES] = rows[comp * s.q : (comp + 1) * s.q]

    load_tiles(s, in_ref, take)
    fetch.wait()
    copies = []
    for part in range(FPA):
        def column(at, part=part):
            there = pl.ds(pl.multiple_of(at.start + part * s.agg, LANES), LANES)
            mask = pat_ref[0:1, there].astype(jnp.float32)
            value = [agg[comp, :, at] for comp in range(3)]
            for comp in range(3):
                total = (rest_ref[0, comp : comp + 1, there] * mask) * value[0]
                for source in range(1, 3):
                    total = total + (rest_ref[source, comp : comp + 1, there] * mask) * value[source]
                out_ref[part, comp, :, at] = total

        each_column(s, column)
        copy = pltpu.make_async_copy(
            out_ref.at[part], out_hbm.at[:, :, pl.ds(part * s.agg, s.agg)], sems.at[part]
        )
        copy.start()
        copies.append(copy)
    for copy in copies:
        copy.wait()


def prolong(s, arrived, restriction, pattern):
    return pl.pallas_call(
        functools.partial(prolong_kernel, s),
        in_specs=[vmem_spec()] * 2 + [pl.BlockSpec(memory_space=pltpu.HBM)],
        out_specs=pl.BlockSpec(memory_space=pltpu.HBM),
        out_shape=jax.ShapeDtypeStruct((3, s.loads, s.fine), jnp.float32),
        scratch_shapes=[
            pltpu.VMEM((3, s.q, s.agg), jnp.float32),
            pltpu.VMEM((FPA, 3, s.q, s.agg), jnp.float32),
            pltpu.VMEM((1, s.fine), jnp.int32),
            pltpu.SemaphoreType.DMA((FPA + 1,)),
        ],
        name="prolong",
        compiler_params=KERNEL,
    )(in_vmem(arrived), in_vmem(restriction), in_hbm(pattern))


def fetch_row(slot_ref, lines, row, held):
    for lane in range(LANES):
        slot = slot_ref[row * LANES + lane]
        held[lane : lane + 1, :] = lines[pl.ds(slot, 1), :]


def edges_kernel(s, slot_ref, in_ref, coef_ref, lines, top_ref, bottom_ref, *held):
    lines_from_tiles(s, in_ref, lines)
    places = []
    for at in range(s.depth):
        places += [(at, top_ref, at), (s.rows - s.depth + at, bottom_ref, at)]
    for (row, _, _), buffer in zip(places, held):
        fetch_row(slot_ref, lines, row, buffer)
    for (row, target, at), buffer in zip(places, held):
        target[at, 0 : s.comps, :] = buffer[...].T[0 : s.comps]
        target[at, s.comps :, :] = coef_ref[row]


def edges(s, received, slots, coefs):
    edge = vmem_result(s.depth, s.comps + COEFS, LANES)
    return pl.pallas_call(
        functools.partial(edges_kernel, s),
        in_specs=[pl.BlockSpec(memory_space=pltpu.SMEM)] + [vmem_spec()] * 2,
        out_specs=[vmem_spec()] * 3,
        out_shape=[vmem_result(s.agg, LANES), edge, edge],
        scratch_shapes=[pltpu.VMEM((LANES, LANES), jnp.float32)] * (2 * s.depth),
        name="edges",
        compiler_params=KERNEL,
    )(slots, in_vmem(received), coefs)


def collect_kernel(s, slot_ref, lines, top_ref, bottom_ref, out_ref, even, odd):
    for at in range(s.depth):
        out_ref[at] = top_ref[at, 0 : s.comps]
        out_ref[s.rows - s.depth + at] = bottom_ref[at, 0 : s.comps]

    def place(row, held):
        out_ref[row] = held[...].T[0 : s.comps]

    fetch_row(slot_ref, lines, s.depth, even)
    last = s.rows - s.depth - 1

    def two(k, carry):
        row = s.depth + 2 * k
        fetch_row(slot_ref, lines, row + 1, odd)
        place(row, even)
        fetch_row(slot_ref, lines, jnp.minimum(row + 2, last), even)
        place(row + 1, odd)
        return carry

    lax.fori_loop(0, (s.rows - 2 * s.depth) // 2, two, 0)


def collect(s, slots, lines, top, bottom):
    return pl.pallas_call(
        functools.partial(collect_kernel, s),
        in_specs=[pl.BlockSpec(memory_space=pltpu.SMEM)] + [vmem_spec()] * 3,
        out_specs=vmem_spec(),
        out_shape=vmem_result(s.rows, s.comps, LANES),
        scratch_shapes=[pltpu.VMEM((LANES, LANES), jnp.float32)] * 2,
        name="collect",
        compiler_params=KERNEL,
    )(slots, lines, top, bottom)


PACK = 32
EDGE = LANES // PACK


def pack_lines(line_of, count, left_ref, right_ref, span):
    for pack in range(left_ref.shape[0]):
        left = right = None
        for member in range(min(PACK, count - pack * PACK)):
            line = line_of(pack * PACK + member)
            head = pltpu.roll(line, member * EDGE, 1) if member else line
            turn = (member + 1) * EDGE
            tail = pltpu.roll(line, turn, 1) if turn < LANES else line
            if left is None:
                here = lax.broadcasted_iota(jnp.int32, line.shape, 1) // EDGE
                left, right = head, tail
            else:
                left = jnp.where(here == member, head, left)
                right = jnp.where(here == member, tail, right)
        left_ref[pack, span, :] = left
        right_ref[pack, span, :] = right


def beyond(past, ahead, member, depth):
    if member:
        past = pltpu.roll(past, LANES - member * EDGE, 1)
    turn = (member + 1) * EDGE
    if turn < LANES:
        ahead = pltpu.roll(ahead, LANES - turn, 1)
    lane = lax.broadcasted_iota(jnp.int32, past.shape, 1)
    return jnp.where(lane < depth, past, jnp.where(lane >= LANES - depth, ahead, 0.0))


def pack_kernel(s, body_ref, coef_ref, before_ref, after_ref, left_ref, right_ref):
    for own_ref, span in ((body_ref, slice(0, s.comps)), (coef_ref, slice(s.comps, s.comps + COEFS))):
        def line_of(at, own_ref=own_ref, span=span):
            if at < s.depth:
                return before_ref[at, span, :]
            if at < s.depth + s.rows:
                return own_ref[at - s.depth]
            return after_ref[at - s.depth - s.rows, span, :]

        pack_lines(line_of, s.wide, left_ref, right_ref, span)


def pack_edges(s, body, coefs, before, after):
    packs = -(-s.wide // PACK)
    shape = vmem_result(packs, s.comps + COEFS, LANES)
    return pl.pallas_call(
        functools.partial(pack_kernel, s),
        in_specs=[vmem_spec()] * 4,
        out_specs=[vmem_spec()] * 2,
        out_shape=[shape, shape],
        name="pack_edges",
        compiler_params=KERNEL,
    )(body, coefs, in_vmem(before), in_vmem(after))


COEFS = 48


def prepare_kernel(s, inv_ref, off_ref, pat_ref, body_ref, flat):
    rows = s.rows
    flat[0 : 9 * rows, :] = inv_ref[...]
    for direction in range(4):
        mask = pat_ref[direction * rows : (direction + 1) * rows, :].astype(jnp.float32)
        for entry in range(9):
            at = direction * 9 + entry
            flat[(9 + at) * rows : (10 + at) * rows, :] = off_ref[at * rows : (at + 1) * rows, :] * mask
    flat[45 * rows : COEFS * rows, :] = jnp.zeros(((COEFS - 45) * rows, LANES), jnp.float32)

    def one(row, carry):
        for low in range(0, COEFS, 8):
            body_ref[row, low : low + 8, :] = flat[pl.ds(low * rows + row, 8, stride=rows), :]
        return carry

    lax.fori_loop(0, rows, one, 0)


def prepare(s, inverse, blocks, pattern):
    return pl.pallas_call(
        functools.partial(prepare_kernel, s),
        in_specs=[vmem_spec()] * 3,
        out_specs=vmem_spec(),
        out_shape=vmem_result(s.rows, COEFS, LANES),
        scratch_shapes=[pltpu.VMEM((COEFS * s.rows, LANES), jnp.float32)],
        name="prepare",
        compiler_params=KERNEL,
    )(inverse.reshape(-1, LANES), blocks.reshape(-1, LANES), pattern.reshape(-1, LANES))


def sweeps_kernel(
    s, slot_ref, rhs_ref, own_ref, before_ref, after_ref, past_ref, ahead_ref,
    sol_hbm, out_ref, wide, coef_ref, even, odd, sol_ref, lines, ahead_lines, behind_lines, sem,
):
    q = s.q
    halves = range(0, q, 8)
    for held, inner_ref, part in (
        (wide, rhs_ref, slice(0, s.comps)),
        (coef_ref, own_ref, slice(s.comps, s.comps + COEFS)),
    ):
        for at in range(s.wide):
            if at < s.depth:
                line = before_ref[at, part, :]
            elif at < s.depth + s.rows:
                line = inner_ref[at - s.depth]
            else:
                line = after_ref[at - s.depth - s.rows, part, :]
            pack, member = divmod(at, PACK)
            held[at, :, 0:LANES] = line
            held[at, :, LANES : 2 * LANES] = beyond(
                past_ref[pack, part, :], ahead_ref[pack, part, :], member, s.depth
            )

    lane = lax.broadcasted_iota(jnp.int32, (8, LANES), 1)
    is_first = lane == 0
    is_last = lane == LANES - 1
    columns = (slice(0, LANES), slice(LANES, 2 * LANES))

    def span(comp, low):
        return slice(comp * q + low, comp * q + low + 8)

    def invert(at, total, column):
        fresh = []
        for comp in range(3):
            value = [None] * len(halves)
            for source in range(3):
                index = comp * 3 + source
                factor = coef_ref[at, index : index + 1, column]
                for half in range(len(halves)):
                    term = factor * total[source][half]
                    value[half] = term if source == 0 else value[half] + term
            fresh.append(value)
        return fresh

    def put(target, at, fresh, column):
        for comp in range(3):
            for half, low in enumerate(halves):
                target[at, span(comp, low), column] = fresh[comp][half]

    def first(at, carry):
        for column in columns:
            total = [[wide[at, span(comp, low), column] for low in halves] for comp in range(3)]
            put(even, at, invert(at, total, column), column)
        return carry

    lax.fori_loop(0, s.wide, first, 0)

    def turned(old, at):
        west = ([], [])
        east = ([], [])
        for comp in range(3):
            for side in west + east:
                side.append([])
            for low in halves:
                here = [old[at, span(comp, low), column] for column in columns]
                up = [pltpu.roll(x, 1, 1) for x in here]
                down = [pltpu.roll(x, LANES - 1, 1) for x in here]
                for v in range(2):
                    west[v][-1].append(jnp.where(is_first, up[1 - v], up[v]))
                    east[v][-1].append(jnp.where(is_last, down[1 - v], down[v]))
        return west, east

    def sweep(old, at, count):
        west, east = turned(old, at)
        result = []
        for v in range(count):
            column = columns[v]
            pieces = []
            for where in (at - 1, at + 1):
                pieces.append([[old[where, span(comp, low), column] for low in halves] for comp in range(3)])
            pieces += [west[v], east[v]]
            total = []
            for comp in range(3):
                value = [wide[at, span(comp, low), column] for low in halves]
                for direction in range(4):
                    for source in range(3):
                        index = 9 + (direction * 3 + comp) * 3 + source
                        factor = coef_ref[at, index : index + 1, column]
                        for half in range(len(halves)):
                            value[half] = value[half] - factor * pieces[direction][source][half]
                total.append(value)
            result.append(invert(at, total, column))
        return result

    old, new = even, odd
    for inner in range(1, s.depth):
        def middle(k, carry, old=old, new=new, inner=inner):
            for step in range(2):
                at = inner + 2 * k + step
                for column, fresh in zip(columns, sweep(old, at, 2)):
                    put(new, at, fresh, column)
            return carry

        lax.fori_loop(0, (s.wide - 2 * inner) // 2, middle, 0)
        old, new = new, old

    def finish(row, held):
        (fresh,) = sweep(old, row + s.depth, 1)
        put(sol_ref, row, fresh, columns[0])
        parts = [fresh[comp][half] for comp in range(3) for half in range(len(halves))]
        held[:, 0 : s.comps] = jnp.concatenate(parts, axis=0).T

    def send(row, held):
        for column in range(LANES):
            slot = slot_ref[row * LANES + column]
            lines[pl.ds(slot, 1), :] = held[column : column + 1, :]

    finish(0, ahead_lines)
    finish(1, behind_lines)

    def two(k, carry):
        row = 2 * k
        send(row, ahead_lines)
        send(row + 1, behind_lines)
        finish(row + 2, ahead_lines)
        finish(row + 3, behind_lines)
        return carry

    lax.fori_loop(0, s.rows // 2 - 1, two, 0)
    copy = pltpu.make_async_copy(sol_ref, sol_hbm, sem)
    copy.start()
    send(s.rows - 2, ahead_lines)
    send(s.rows - 1, behind_lines)
    tiles_from_lines(s, lines, out_ref)
    copy.wait()


def sweeps(s, slots, rhs, coefs, before, after, past, ahead):
    state = pltpu.VMEM((s.wide, s.comps, 2 * LANES), jnp.float32)
    return pl.pallas_call(
        functools.partial(sweeps_kernel, s),
        in_specs=[pl.BlockSpec(memory_space=pltpu.SMEM)] + [vmem_spec()] * 6,
        out_specs=[pl.BlockSpec(memory_space=pltpu.HBM), vmem_spec()],
        out_shape=[
            jax.ShapeDtypeStruct((s.rows, s.comps, LANES), jnp.float32),
            jax.ShapeDtypeStruct((s.devices * s.per_peer, LANES), jnp.float32),
        ],
        scratch_shapes=[
            state,
            pltpu.VMEM((s.wide, COEFS, 2 * LANES), jnp.float32),
            state,
            state,
            pltpu.VMEM((s.rows, s.comps, LANES), jnp.float32),
            pltpu.VMEM((s.agg, LANES), jnp.float32),
            pltpu.VMEM((LANES, LANES), jnp.float32),
            pltpu.VMEM((LANES, LANES), jnp.float32),
            pltpu.SemaphoreType.DMA,
        ],
        name="sweeps",
        compiler_params=KERNEL,
    )(slots, rhs, coefs, *map(in_vmem, (before, after, past, ahead)))


def ring(axis):
    count = lax.axis_size(axis)
    up = [(i, i + 1) for i in range(count - 1)]
    return up, [(j, i) for i, j in up]


def exchange(s, outgoing):
    blocks = outgoing.reshape(s.devices, s.per_peer, LANES)
    moved = lax.all_to_all(blocks, AXES, split_axis=0, concat_axis=0, tiled=True)
    return moved.reshape(s.devices * s.per_peer, LANES)


def body(
    fine_residual,
    restriction,
    restriction_pattern,
    cell_aggregate,
    block_inverse,
    off_blocks,
    operator_pattern,
):
    s = Sizes(
        fine_residual.shape[2],
        fine_residual.shape[0],
        cell_aggregate.shape[0],
        cell_aggregate.shape[1],
        lax.axis_size("row"),
        lax.axis_size("col"),
    )
    residual = fine_residual.transpose(1, 0, 2)
    pattern = restriction_pattern.reshape(1, -1)

    outgoing = restrict(s, residual, restriction, pattern)
    received = exchange(s, outgoing)
    owner = cell_aggregate // s.agg
    local = cell_aggregate % s.agg
    slots = (local // s.devices * s.devices + owner).reshape(-1)
    coefs = prepare(s, block_inverse, off_blocks, operator_pattern)

    up, down = ring("row")
    lines, top, bottom = edges(s, received, slots, coefs)
    before = lax.ppermute(bottom, "row", up)
    after = lax.ppermute(top, "row", down)
    rhs = collect(s, slots, lines, top, bottom)
    left, right = pack_edges(s, rhs, coefs, before, after)
    up, down = ring("col")
    ahead = lax.ppermute(right, "col", up)
    past = lax.ppermute(left, "col", down)
    solved, outgoing = sweeps(s, slots, rhs, coefs, before, after, past, ahead)
    correction = prolong(s, exchange(s, outgoing), restriction, pattern)
    coarse = solved.reshape(s.rows, 3, s.loads, LANES).transpose(2, 1, 0, 3)
    return coarse, correction.transpose(1, 0, 2)


def solution(mesh):
    in_specs = (
        P(None, None, AXES),
        P(None, None, AXES),
        P(AXES),
        P("row", "col"),
        P(None, None, "row", "col"),
        P(None, None, None, "row", "col"),
        P(None, "row", "col"),
    )
    out_specs = (P(None, None, "row", "col"), P(None, None, AXES))
    return jax.shard_map(body, mesh=mesh, in_specs=in_specs, out_specs=out_specs, check_vma=False)
```

```python
import functools
import math

import jax
import jax.numpy as jnp
from jax import lax
from jax.experimental import pallas as pl
from jax.experimental.pallas import tpu as pltpu
from jax.sharding import PartitionSpec as P

FPA = 8
ITERS = 4
LANES = 128
UNROLL = 4
AXES = ("row", "col")


def vmem_spec():
    return pl.BlockSpec(memory_space=pltpu.VMEM)


KERNEL = pltpu.CompilerParams(vmem_limit_bytes=30 * 1024 * 1024)


def in_vmem(x):
    return pltpu.with_memory_space_constraint(x, pltpu.VMEM)


def in_hbm(x):
    return pltpu.with_memory_space_constraint(x, pltpu.HBM)


def vmem_result(*shape):
    return pltpu.VMEM(shape, jnp.float32)


class Sizes:
    def __init__(self, fine, loads, rows, cols, rows_n, cols_n):
        self.devices = rows_n * cols_n
        self.rows_n, self.cols_n = rows_n, cols_n
        self.fine = fine
        self.agg = fine // FPA
        self.blocks = self.agg // LANES
        self.loads = loads
        self.rows, self.cols = rows, cols
        self.q = loads
        self.comps = 3 * self.q
        self.group = LANES // math.gcd(self.comps, LANES)
        self.groups = self.blocks // self.group
        self.tiles = self.group * self.comps // LANES
        self.low = LANES // self.devices
        self.per_peer = self.tiles * self.groups * self.low
        self.depth = ITERS - 1
        self.wide = rows + 2 * self.depth


def starts(s, grp, tile):
    for low in range(s.low):
        slot = (grp * s.tiles + tile) * s.low + low
        for first in range(0, s.devices, 8):
            yield low * s.devices + first, first * s.per_peer + slot


def pieces(s, grp):
    for member in range(s.group):
        done = 0
        while done < s.comps:
            at = member * s.comps + done
            size = min(s.comps - done, LANES - at % LANES)
            yield at // LANES, at % LANES, member, done, size
            done += size


def store_tiles(s, out_ref, rows_of):
    for grp in range(s.groups):
        rows = jnp.concatenate([rows_of(grp * s.group + member) for member in range(s.group)], axis=0)
        for tile in range(s.tiles):
            turned = rows[tile * LANES : (tile + 1) * LANES].T
            for lane, start in starts(s, grp, tile):
                out_ref[pl.ds(start, 8, stride=s.per_peer), :] = turned[lane : lane + 8]


def load_tiles(s, in_ref, take):
    for grp in range(s.groups):
        turned = []
        for tile in range(s.tiles):
            parts = [in_ref[pl.ds(start, 8, stride=s.per_peer), :] for _, start in starts(s, grp, tile)]
            turned.append(jnp.concatenate(parts, axis=0).T)
        rows = jnp.concatenate(turned, axis=0)
        for member in range(s.group):
            take(grp * s.group + member, rows[member * s.comps : (member + 1) * s.comps])


def turn(x, by):
    return pltpu.roll(x, by % LANES, 1) if by % LANES else x


def lines_from_tiles(s, in_ref, lines):
    where = lax.broadcasted_iota(jnp.int32, (8, LANES), 1)
    for grp in range(s.groups):
        runs = [dict(starts(s, grp, tile)) for tile in range(s.tiles)]
        for lane in runs[0]:
            held = [in_ref[pl.ds(run[lane], 8, stride=s.per_peer), :] for run in runs]
            made = {}
            for tile, low, member, done, size in pieces(s, grp):
                part = turn(held[tile], done - low)
                made[member] = jnp.where(where >= done, part, made[member]) if member in made else part
            for member, line in made.items():
                row = (grp * s.group + member) * LANES + lane
                lines[row : row + 8, :] = line


def tiles_from_lines(s, lines, out_ref):
    where = lax.broadcasted_iota(jnp.int32, (8, LANES), 1)
    for grp in range(s.groups):
        runs = [dict(starts(s, grp, tile)) for tile in range(s.tiles)]
        for lane in runs[0]:
            held = []
            for member in range(s.group):
                row = (grp * s.group + member) * LANES + lane
                held.append(lines[row : row + 8, :])
            made = {}
            for tile, low, member, done, size in pieces(s, grp):
                part = turn(held[member], low - done)
                made[tile] = jnp.where(where >= low, part, made[tile]) if tile in made else part
            for tile, value in made.items():
                out_ref[pl.ds(runs[tile][lane], 8, stride=s.per_peer), :] = value


def spread(row):
    return jnp.broadcast_to(row, (8, LANES))


def each_column(s, visit):
    def some(block, carry):
        for step in range(UNROLL):
            visit(pl.ds(pl.multiple_of((block * UNROLL + step) * LANES, LANES), LANES))
        return carry

    lax.fori_loop(0, s.blocks // UNROLL, some, 0)


def restrict_kernel(s, x_hbm, rest_hbm, pat_hbm, out_ref, x_ref, rest_ref, pat_ref, acc, sems):
    copies = []
    for part in range(FPA):
        at = pl.ds(part * s.agg, s.agg)
        group = (
            pltpu.make_async_copy(rest_hbm.at[:, :, at], rest_ref.at[part], sems.at[part, 0]),
            pltpu.make_async_copy(pat_hbm.at[:, at], pat_ref.at[part], sems.at[part, 1]),
            pltpu.make_async_copy(x_hbm.at[:, :, at], x_ref.at[part], sems.at[part, 2]),
        )
        for copy in group:
            copy.start()
        copies.append(group)

    for part in range(FPA):
        for copy in copies[part]:
            copy.wait()

        def column(at, part=part):
            mask = spread(pat_ref[part, 0:1, at]).astype(jnp.float32)
            for comp in range(3):
                factor = [spread(rest_ref[part, comp, k : k + 1, at]) * mask for k in range(3)]
                for low in range(0, s.q, 8):
                    loads = slice(low, low + 8)
                    total = factor[0] * x_ref[part, 0, loads, at]
                    for source in range(1, 3):
                        total = total + factor[source] * x_ref[part, source, loads, at]
                    acc[comp, loads, at] = total if part == 0 else acc[comp, loads, at] + total

        each_column(s, column)

    def rows_of(block):
        return jnp.concatenate([acc[comp, :, block * LANES : (block + 1) * LANES] for comp in range(3)], axis=0)

    store_tiles(s, out_ref, rows_of)


def restrict(s, residual, restriction, pattern):
    return pl.pallas_call(
        functools.partial(restrict_kernel, s),
        in_specs=[pl.BlockSpec(memory_space=pltpu.HBM)] * 3,
        out_specs=vmem_spec(),
        out_shape=vmem_result(s.devices * s.per_peer, LANES),
        scratch_shapes=[
            pltpu.VMEM((FPA, 3, s.q, s.agg), jnp.float32),
            pltpu.VMEM((FPA, 3, 3, s.agg), jnp.float32),
            pltpu.VMEM((FPA, 1, s.agg), jnp.int32),
            pltpu.VMEM((3, s.q, s.agg), jnp.float32),
            pltpu.SemaphoreType.DMA((FPA, 3)),
        ],
        name="restrict",
        compiler_params=KERNEL,
    )(*map(in_hbm, (residual, restriction, pattern)))


def prolong_kernel(s, in_ref, rest_ref, pat_hbm, out_hbm, agg, out_ref, pat_ref, sems):
    fetch = pltpu.make_async_copy(pat_hbm, pat_ref, sems.at[FPA])
    fetch.start()

    def take(block, rows):
        for comp in range(3):
            agg[comp, :, block * LANES : (block + 1) * LANES] = rows[comp * s.q : (comp + 1) * s.q]

    load_tiles(s, in_ref, take)
    fetch.wait()
    copies = []
    for part in range(FPA):
        def column(at, part=part):
            there = pl.ds(pl.multiple_of(at.start + part * s.agg, LANES), LANES)
            mask = spread(pat_ref[0:1, there]).astype(jnp.float32)
            for comp in range(3):
                factor = [spread(rest_ref[k, comp : comp + 1, there]) * mask for k in range(3)]
                for low in range(0, s.q, 8):
                    loads = slice(low, low + 8)
                    total = factor[0] * agg[0, loads, at]
                    for source in range(1, 3):
                        total = total + factor[source] * agg[source, loads, at]
                    out_ref[part, comp, loads, at] = total

        each_column(s, column)
        copy = pltpu.make_async_copy(
            out_ref.at[part], out_hbm.at[:, :, pl.ds(part * s.agg, s.agg)], sems.at[part]
        )
        copy.start()
        copies.append(copy)
    for copy in copies:
        copy.wait()


def prolong(s, arrived, restriction, pattern):
    return pl.pallas_call(
        functools.partial(prolong_kernel, s),
        in_specs=[vmem_spec()] * 2 + [pl.BlockSpec(memory_space=pltpu.HBM)],
        out_specs=pl.BlockSpec(memory_space=pltpu.HBM),
        out_shape=jax.ShapeDtypeStruct((3, s.loads, s.fine), jnp.float32),
        scratch_shapes=[
            pltpu.VMEM((3, s.q, s.agg), jnp.float32),
            pltpu.VMEM((FPA, 3, s.q, s.agg), jnp.float32),
            pltpu.VMEM((1, s.fine), jnp.int32),
            pltpu.SemaphoreType.DMA((FPA + 1,)),
        ],
        name="prolong",
        compiler_params=KERNEL,
    )(in_vmem(arrived), in_vmem(restriction), in_hbm(pattern))


def fetch_row(slot_ref, lines, row, held):
    for lane in range(LANES):
        slot = slot_ref[row, lane]
        held[lane : lane + 1, :] = lines[pl.ds(slot, 1), :]


def edges_kernel(s, slot_ref, in_ref, coef_ref, lines, top_ref, bottom_ref, *held):
    lines_from_tiles(s, in_ref, lines)
    places = []
    for at in range(s.depth):
        places += [(at, top_ref, at), (s.rows - s.depth + at, bottom_ref, at)]
    for (row, _, _), buffer in zip(places, held):
        fetch_row(slot_ref, lines, row, buffer)
    for (row, target, at), buffer in zip(places, held):
        target[at, 0 : s.comps, :] = buffer[...].T[0 : s.comps]
        target[at, s.comps :, :] = coef_ref[row]


def edges(s, received, slots, coefs):
    edge = vmem_result(s.depth, s.comps + COEFS, LANES)
    return pl.pallas_call(
        functools.partial(edges_kernel, s),
        in_specs=[pl.BlockSpec(memory_space=pltpu.SMEM)] + [vmem_spec()] * 2,
        out_specs=[vmem_spec()] * 3,
        out_shape=[vmem_result(s.agg, LANES), edge, edge],
        scratch_shapes=[pltpu.VMEM((LANES, LANES), jnp.float32)] * (2 * s.depth),
        name="edges",
        compiler_params=KERNEL,
    )(slots, in_vmem(received), coefs)


def collect_kernel(s, slot_ref, lines, top_ref, bottom_ref, out_ref, even, odd):
    for at in range(s.depth):
        out_ref[at] = top_ref[at, 0 : s.comps]
        out_ref[s.rows - s.depth + at] = bottom_ref[at, 0 : s.comps]

    def place(row, held):
        out_ref[row] = held[...].T[0 : s.comps]

    fetch_row(slot_ref, lines, s.depth, even)
    last = s.rows - s.depth - 1

    def two(k, carry):
        row = s.depth + 2 * k
        fetch_row(slot_ref, lines, row + 1, odd)
        place(row, even)
        fetch_row(slot_ref, lines, jnp.minimum(row + 2, last), even)
        place(row + 1, odd)
        return carry

    lax.fori_loop(0, (s.rows - 2 * s.depth) // 2, two, 0)


def collect(s, slots, lines, top, bottom):
    return pl.pallas_call(
        functools.partial(collect_kernel, s),
        in_specs=[pl.BlockSpec(memory_space=pltpu.SMEM)] + [vmem_spec()] * 3,
        out_specs=vmem_spec(),
        out_shape=vmem_result(s.rows, s.comps, LANES),
        scratch_shapes=[pltpu.VMEM((LANES, LANES), jnp.float32)] * 2,
        name="collect",
        compiler_params=KERNEL,
    )(slots, lines, top, bottom)


PACK = 32
EDGE = LANES // PACK


def pack_lines(line_of, count, left_ref, right_ref, span, start=None):
    for pack in range(left_ref.shape[0]):
        left, right = (None, None) if start is None else (start[0][pack], start[1][pack])
        for member in range(min(PACK, count - pack * PACK)):
            line = line_of(pack * PACK + member)
            if line is None:
                continue
            by = (member + 1) * EDGE
            head, tail = turn(line, by - EDGE), turn(line, by)
            if left is None:
                left, right = head, tail
            else:
                here = lax.broadcasted_iota(jnp.int32, line.shape, 1) // EDGE == member
                left = jnp.where(here, head, left)
                right = jnp.where(here, tail, right)
        left_ref[pack, span, :] = left
        right_ref[pack, span, :] = right


def beyond(past, ahead, member, depth):
    if member:
        past = pltpu.roll(past, LANES - member * EDGE, 1)
    turn = (member + 1) * EDGE
    if turn < LANES:
        ahead = pltpu.roll(ahead, LANES - turn, 1)
    lane = lax.broadcasted_iota(jnp.int32, past.shape, 1)
    return jnp.where(lane < depth, past, jnp.where(lane >= LANES - depth, ahead, 0.0))


def pack_kernel(s, body_ref, left_coef_ref, right_coef_ref, before_ref, after_ref, left_ref, right_ref):
    def line_of(at, own_ref, span):
        if at < s.depth:
            return before_ref[at, span, :]
        if at < s.depth + s.rows:
            return None if own_ref is None else own_ref[at - s.depth]
        return after_ref[at - s.depth - s.rows, span, :]

    loads, coefs = slice(0, s.comps), slice(s.comps, s.comps + COEFS)
    pack_lines(lambda at: line_of(at, body_ref, loads), s.wide, left_ref, right_ref, loads)
    start = (left_coef_ref, right_coef_ref)
    pack_lines(lambda at: line_of(at, None, coefs), s.wide, left_ref, right_ref, coefs, start)


def pack_edges(s, body, packs, before, after):
    shape = vmem_result(-(-s.wide // PACK), s.comps + COEFS, LANES)
    return pl.pallas_call(
        functools.partial(pack_kernel, s),
        in_specs=[vmem_spec()] * 5,
        out_specs=[vmem_spec()] * 2,
        out_shape=[shape, shape],
        name="pack_edges",
        compiler_params=KERNEL,
    )(body, *packs, in_vmem(before), in_vmem(after))


COEFS = 48


def prepare_kernel(s, inv_ref, off_ref, pat_ref, body_ref, left_ref, right_ref, flat):
    rows = s.rows
    flat[0 : 9 * rows, :] = inv_ref[...]
    for direction in range(4):
        mask = pat_ref[direction * rows : (direction + 1) * rows, :].astype(jnp.float32)
        for entry in range(9):
            at = direction * 9 + entry
            flat[(9 + at) * rows : (10 + at) * rows, :] = off_ref[at * rows : (at + 1) * rows, :] * mask
    flat[45 * rows : COEFS * rows, :] = jnp.zeros(((COEFS - 45) * rows, LANES), jnp.float32)

    def one(row, carry):
        for low in range(0, COEFS, 8):
            body_ref[row, low : low + 8, :] = flat[pl.ds(low * rows + row, 8, stride=rows), :]
        return carry

    lax.fori_loop(0, rows, one, 0)

    def line_of(at):
        return body_ref[at - s.depth] if s.depth <= at < s.depth + rows else None

    pack_lines(line_of, s.wide, left_ref, right_ref, slice(0, COEFS))


def prepare(s, inverse, blocks, pattern):
    return pl.pallas_call(
        functools.partial(prepare_kernel, s),
        in_specs=[vmem_spec()] * 3,
        out_specs=[vmem_spec()] * 3,
        out_shape=[vmem_result(s.rows, COEFS, LANES)] + [vmem_result(-(-s.wide // PACK), COEFS, LANES)] * 2,
        scratch_shapes=[pltpu.VMEM((COEFS * s.rows, LANES), jnp.float32)],
        name="prepare",
        compiler_params=KERNEL,
    )(inverse.reshape(-1, LANES), blocks.reshape(-1, LANES), pattern.reshape(-1, LANES))


def sweeps_kernel(
    s, slot_ref, inside_ref, rhs_ref, own_ref, before_ref, after_ref, past_ref, ahead_ref,
    sol_hbm, out_ref, wide, coef_ref, even, odd, sol_ref, lines, ahead_lines, behind_lines, sem,
):
    q = s.q
    halves = range(0, q, 8)
    lane = lax.broadcasted_iota(jnp.int32, (COEFS, LANES), 1)
    side = jnp.where(lane < LANES // 2, inside_ref[3], inside_ref[2])
    for held, inner_ref, part in (
        (wide, rhs_ref, slice(0, s.comps)),
        (coef_ref, own_ref, slice(s.comps, s.comps + COEFS)),
    ):
        for at in range(s.wide):
            if at < s.depth:
                line, inside = before_ref[at, part, :], inside_ref[0]
            elif at < s.depth + s.rows:
                line, inside = inner_ref[at - s.depth], None
            else:
                line, inside = after_ref[at - s.depth - s.rows, part, :], inside_ref[1]
            pack, member = divmod(at, PACK)
            other = beyond(past_ref[pack, part, :], ahead_ref[pack, part, :], member, s.depth)
            if held is coef_ref:
                other = other * side
                if inside is not None:
                    line, other = line * inside, other * inside
            held[at, :, 0:LANES] = line
            held[at, :, LANES : 2 * LANES] = other

    lane = lax.broadcasted_iota(jnp.int32, (8, LANES), 1)
    is_first = lane == 0
    is_last = lane == LANES - 1
    columns = (slice(0, LANES), slice(LANES, 2 * LANES))

    def span(comp, low):
        return slice(comp * q + low, comp * q + low + 8)

    def invert(at, total, column):
        fresh = []
        for comp in range(3):
            value = [None] * len(halves)
            for source in range(3):
                index = comp * 3 + source
                factor = coef_ref[at, index : index + 1, column]
                for half in range(len(halves)):
                    term = factor * total[source][half]
                    value[half] = term if source == 0 else value[half] + term
            fresh.append(value)
        return fresh

    def put(target, at, fresh, column):
        for comp in range(3):
            for half, low in enumerate(halves):
                target[at, span(comp, low), column] = fresh[comp][half]

    def first(at, carry):
        for column in columns:
            total = [[wide[at, span(comp, low), column] for low in halves] for comp in range(3)]
            put(even, at, invert(at, total, column), column)
        return carry

    lax.fori_loop(0, s.wide, first, 0)

    def turned(old, at):
        west = ([], [])
        east = ([], [])
        for comp in range(3):
            for side in west + east:
                side.append([])
            for low in halves:
                here = [old[at, span(comp, low), column] for column in columns]
                up = [pltpu.roll(x, 1, 1) for x in here]
                down = [pltpu.roll(x, LANES - 1, 1) for x in here]
                for v in range(2):
                    west[v][-1].append(jnp.where(is_first, up[1 - v], up[v]))
                    east[v][-1].append(jnp.where(is_last, down[1 - v], down[v]))
        return west, east

    def sweep(old, at, count):
        west, east = turned(old, at)
        result = []
        for v in range(count):
            column = columns[v]
            pieces = []
            for where in (at - 1, at + 1):
                pieces.append([[old[where, span(comp, low), column] for low in halves] for comp in range(3)])
            pieces += [west[v], east[v]]
            total = []
            for comp in range(3):
                value = [wide[at, span(comp, low), column] for low in halves]
                for direction in range(4):
                    for source in range(3):
                        index = 9 + (direction * 3 + comp) * 3 + source
                        factor = coef_ref[at, index : index + 1, column]
                        for half in range(len(halves)):
                            value[half] = value[half] - factor * pieces[direction][source][half]
                total.append(value)
            result.append(invert(at, total, column))
        return result

    old, new = even, odd
    for inner in range(1, s.depth):
        def middle(k, carry, old=old, new=new, inner=inner):
            for step in range(2):
                at = inner + 2 * k + step
                for column, fresh in zip(columns, sweep(old, at, 2)):
                    put(new, at, fresh, column)
            return carry

        lax.fori_loop(0, (s.wide - 2 * inner) // 2, middle, 0)
        old, new = new, old

    def finish(row, held):
        (fresh,) = sweep(old, row + s.depth, 1)
        put(sol_ref, row, fresh, columns[0])
        parts = [fresh[comp][half] for comp in range(3) for half in range(len(halves))]
        held[:, 0 : s.comps] = jnp.concatenate(parts, axis=0).T

    def send(row, held):
        for column in range(LANES):
            slot = slot_ref[row, column]
            lines[pl.ds(slot, 1), :] = held[column : column + 1, :]

    finish(0, ahead_lines)
    finish(1, behind_lines)

    def two(k, carry):
        row = 2 * k
        send(row, ahead_lines)
        send(row + 1, behind_lines)
        finish(row + 2, ahead_lines)
        finish(row + 3, behind_lines)
        return carry

    lax.fori_loop(0, s.rows // 2 - 1, two, 0)
    copy = pltpu.make_async_copy(sol_ref, sol_hbm, sem)
    copy.start()
    send(s.rows - 2, ahead_lines)
    send(s.rows - 1, behind_lines)
    tiles_from_lines(s, lines, out_ref)
    copy.wait()


def sweeps(s, slots, inside, rhs, coefs, before, after, past, ahead):
    state = pltpu.VMEM((s.wide, s.comps, 2 * LANES), jnp.float32)
    return pl.pallas_call(
        functools.partial(sweeps_kernel, s),
        in_specs=[pl.BlockSpec(memory_space=pltpu.SMEM)] * 2 + [vmem_spec()] * 6,
        out_specs=[pl.BlockSpec(memory_space=pltpu.HBM), vmem_spec()],
        out_shape=[
            pltpu.HBM((s.rows, s.comps, LANES), jnp.float32),
            jax.ShapeDtypeStruct((s.devices * s.per_peer, LANES), jnp.float32),
        ],
        scratch_shapes=[
            state,
            pltpu.VMEM((s.wide, COEFS, 2 * LANES), jnp.float32),
            state,
            state,
            pltpu.VMEM((s.rows, s.comps, LANES), jnp.float32),
            pltpu.VMEM((s.agg, LANES), jnp.float32),
            pltpu.VMEM((LANES, LANES), jnp.float32),
            pltpu.VMEM((LANES, LANES), jnp.float32),
            pltpu.SemaphoreType.DMA,
        ],
        name="sweeps",
        compiler_params=KERNEL,
    )(slots, inside, rhs, coefs, *map(in_vmem, (before, after, past, ahead)))


def ring(axis):
    count = lax.axis_size(axis)
    up = [(i, (i + 1) % count) for i in range(count)]
    return up, [(j, i) for i, j in up]


def exchange(s, outgoing):
    blocks = outgoing.reshape(s.devices, s.per_peer, LANES)
    moved = lax.all_to_all(blocks, AXES, split_axis=0, concat_axis=0, tiled=True)
    return moved.reshape(s.devices * s.per_peer, LANES)


def body(
    fine_residual,
    restriction,
    restriction_pattern,
    cell_aggregate,
    block_inverse,
    off_blocks,
    operator_pattern,
):
    s = Sizes(
        fine_residual.shape[2],
        fine_residual.shape[0],
        cell_aggregate.shape[0],
        cell_aggregate.shape[1],
        lax.axis_size("row"),
        lax.axis_size("col"),
    )
    residual = fine_residual.transpose(1, 0, 2)
    pattern = restriction_pattern.reshape(1, -1)

    outgoing = restrict(s, residual, restriction, pattern)
    received = exchange(s, outgoing)
    owner = cell_aggregate // s.agg
    local = cell_aggregate % s.agg
    slots = local // s.devices * s.devices + owner
    coefs, *packs = prepare(s, block_inverse, off_blocks, operator_pattern)

    ends = []
    for axis in AXES:
        here = lax.axis_index(axis)
        ends += [here > 0, here < lax.axis_size(axis) - 1]
    inside = jnp.stack(ends).astype(jnp.float32)

    up, down = ring("row")
    lines, top, bottom = edges(s, received, slots, coefs)
    before = lax.ppermute(bottom, "row", up)
    after = lax.ppermute(top, "row", down)
    rhs = collect(s, slots, lines, top, bottom)
    left, right = pack_edges(s, rhs, packs, before, after)
    up, down = ring("col")
    ahead = lax.ppermute(right, "col", up)
    past = lax.ppermute(left, "col", down)
    solved, outgoing = sweeps(s, slots, inside, rhs, coefs, before, after, past, ahead)
    correction = prolong(s, exchange(s, outgoing), restriction, pattern)
    coarse = solved.reshape(s.rows, 3, s.loads, LANES).transpose(2, 1, 0, 3)
    return coarse, correction.transpose(1, 0, 2)


def solution(mesh):
    in_specs = (
        P(None, None, AXES),
        P(None, None, AXES),
        P(AXES),
        P("row", "col"),
        P(None, None, "row", "col"),
        P(None, None, None, "row", "col"),
        P(None, "row", "col"),
    )
    out_specs = (P(None, None, "row", "col"), P(None, None, AXES))
    return jax.shard_map(body, mesh=mesh, in_specs=in_specs, out_specs=out_specs, check_vma=False)
```

```python
import functools
import math

import jax
import jax.numpy as jnp
from jax import lax
from jax.experimental import pallas as pl
from jax.experimental.pallas import tpu as pltpu
from jax.sharding import PartitionSpec as P

FPA = 8
ITERS = 4
LANES = 128
UNROLL = 4
AXES = ("row", "col")


def vmem_spec():
    return pl.BlockSpec(memory_space=pltpu.VMEM)


KERNEL = pltpu.CompilerParams(vmem_limit_bytes=30 * 1024 * 1024)


def in_vmem(x):
    return pltpu.with_memory_space_constraint(x, pltpu.VMEM)


def in_hbm(x):
    return pltpu.with_memory_space_constraint(x, pltpu.HBM)


def vmem_result(*shape):
    return pltpu.VMEM(shape, jnp.float32)


class Sizes:
    def __init__(self, fine, loads, rows, cols, rows_n, cols_n):
        self.devices = rows_n * cols_n
        self.rows_n, self.cols_n = rows_n, cols_n
        self.fine = fine
        self.agg = fine // FPA
        self.blocks = self.agg // LANES
        self.loads = loads
        self.rows, self.cols = rows, cols
        self.q = loads
        self.comps = 3 * self.q
        self.group = LANES // math.gcd(self.comps, LANES)
        self.groups = self.blocks // self.group
        self.tiles = self.group * self.comps // LANES
        self.low = LANES // self.devices
        self.per_peer = self.tiles * self.groups * self.low
        self.depth = ITERS - 1
        self.wide = rows + 2 * self.depth


def starts(s, grp, tile):
    for low in range(s.low):
        slot = (grp * s.tiles + tile) * s.low + low
        for first in range(0, s.devices, 8):
            yield low * s.devices + first, first * s.per_peer + slot


def pieces(s, grp):
    for member in range(s.group):
        done = 0
        while done < s.comps:
            at = member * s.comps + done
            size = min(s.comps - done, LANES - at % LANES)
            yield at // LANES, at % LANES, member, done, size
            done += size


def store_tiles(s, out_ref, rows_of):
    for grp in range(s.groups):
        rows = jnp.concatenate([rows_of(grp * s.group + member) for member in range(s.group)], axis=0)
        for tile in range(s.tiles):
            turned = rows[tile * LANES : (tile + 1) * LANES].T
            for lane, start in starts(s, grp, tile):
                out_ref[pl.ds(start, 8, stride=s.per_peer), :] = turned[lane : lane + 8]


def load_tiles(s, in_ref, take):
    for grp in range(s.groups):
        turned = []
        for tile in range(s.tiles):
            parts = [in_ref[pl.ds(start, 8, stride=s.per_peer), :] for _, start in starts(s, grp, tile)]
            turned.append(jnp.concatenate(parts, axis=0).T)
        rows = jnp.concatenate(turned, axis=0)
        for member in range(s.group):
            take(grp * s.group + member, rows[member * s.comps : (member + 1) * s.comps])


def turn(x, by):
    return pltpu.roll(x, by % LANES, 1) if by % LANES else x


def lines_from_tiles(s, in_ref, lines):
    where = lax.broadcasted_iota(jnp.int32, (8, LANES), 1)
    for grp in range(s.groups):
        runs = [dict(starts(s, grp, tile)) for tile in range(s.tiles)]
        for lane in runs[0]:
            held = [in_ref[pl.ds(run[lane], 8, stride=s.per_peer), :] for run in runs]
            made = {}
            for tile, low, member, done, size in pieces(s, grp):
                part = turn(held[tile], done - low)
                made[member] = jnp.where(where >= done, part, made[member]) if member in made else part
            for member, line in made.items():
                row = (grp * s.group + member) * LANES + lane
                lines[row : row + 8, :] = line


def tiles_from_lines(s, lines, out_ref):
    where = lax.broadcasted_iota(jnp.int32, (8, LANES), 1)
    for grp in range(s.groups):
        runs = [dict(starts(s, grp, tile)) for tile in range(s.tiles)]
        for lane in runs[0]:
            held = []
            for member in range(s.group):
                row = (grp * s.group + member) * LANES + lane
                held.append(lines[row : row + 8, :])
            made = {}
            for tile, low, member, done, size in pieces(s, grp):
                part = turn(held[member], low - done)
                made[tile] = jnp.where(where >= low, part, made[tile]) if tile in made else part
            for tile, value in made.items():
                out_ref[pl.ds(runs[tile][lane], 8, stride=s.per_peer), :] = value


def spread(row):
    return jnp.broadcast_to(row, (8, LANES))


def each_column(s, visit):
    def some(block, carry):
        for step in range(UNROLL):
            visit(pl.ds(pl.multiple_of((block * UNROLL + step) * LANES, LANES), LANES))
        return carry

    lax.fori_loop(0, s.blocks // UNROLL, some, 0)


def restrict_kernel(s, x_hbm, rest_hbm, pat_hbm, out_ref, x_ref, rest_ref, pat_ref, acc, sems):
    copies = []
    for part in range(FPA):
        at = pl.ds(part * s.agg, s.agg)
        group = (
            pltpu.make_async_copy(rest_hbm.at[:, :, at], rest_ref.at[part], sems.at[part, 0]),
            pltpu.make_async_copy(pat_hbm.at[:, at], pat_ref.at[part], sems.at[part, 1]),
            pltpu.make_async_copy(x_hbm.at[:, :, at], x_ref.at[part], sems.at[part, 2]),
        )
        for copy in group:
            copy.start()
        copies.append(group)

    for part in range(FPA):
        for copy in copies[part]:
            copy.wait()

        def column(at, part=part):
            mask = spread(pat_ref[part, 0:1, at]).astype(jnp.float32)
            for comp in range(3):
                factor = [spread(rest_ref[part, comp, k : k + 1, at]) * mask for k in range(3)]
                for low in range(0, s.q, 8):
                    loads = slice(low, low + 8)
                    total = factor[0] * x_ref[part, 0, loads, at]
                    for source in range(1, 3):
                        total = total + factor[source] * x_ref[part, source, loads, at]
                    acc[comp, loads, at] = total if part == 0 else acc[comp, loads, at] + total

        each_column(s, column)

    def rows_of(block):
        return jnp.concatenate([acc[comp, :, block * LANES : (block + 1) * LANES] for comp in range(3)], axis=0)

    store_tiles(s, out_ref, rows_of)


def restrict(s, residual, restriction, pattern):
    return pl.pallas_call(
        functools.partial(restrict_kernel, s),
        in_specs=[pl.BlockSpec(memory_space=pltpu.HBM)] * 3,
        out_specs=vmem_spec(),
        out_shape=vmem_result(s.devices * s.per_peer, LANES),
        scratch_shapes=[
            pltpu.VMEM((FPA, 3, s.q, s.agg), jnp.float32),
            pltpu.VMEM((FPA, 3, 3, s.agg), jnp.float32),
            pltpu.VMEM((FPA, 1, s.agg), jnp.int32),
            pltpu.VMEM((3, s.q, s.agg), jnp.float32),
            pltpu.SemaphoreType.DMA((FPA, 3)),
        ],
        name="restrict",
        compiler_params=KERNEL,
    )(*map(in_hbm, (residual, restriction, pattern)))


def prolong_kernel(s, in_ref, rest_ref, pat_hbm, out_hbm, agg, out_ref, pat_ref, sems):
    fetch = pltpu.make_async_copy(pat_hbm, pat_ref, sems.at[FPA])
    fetch.start()

    def take(block, rows):
        for comp in range(3):
            agg[comp, :, block * LANES : (block + 1) * LANES] = rows[comp * s.q : (comp + 1) * s.q]

    load_tiles(s, in_ref, take)
    fetch.wait()
    copies = []
    for part in range(FPA):
        def column(at, part=part):
            there = pl.ds(pl.multiple_of(at.start + part * s.agg, LANES), LANES)
            mask = spread(pat_ref[0:1, there]).astype(jnp.float32)
            for comp in range(3):
                factor = [spread(rest_ref[k, comp : comp + 1, there]) * mask for k in range(3)]
                for low in range(0, s.q, 8):
                    loads = slice(low, low + 8)
                    total = factor[0] * agg[0, loads, at]
                    for source in range(1, 3):
                        total = total + factor[source] * agg[source, loads, at]
                    out_ref[part, comp, loads, at] = total

        each_column(s, column)
        copy = pltpu.make_async_copy(
            out_ref.at[part], out_hbm.at[:, :, pl.ds(part * s.agg, s.agg)], sems.at[part]
        )
        copy.start()
        copies.append(copy)
    for copy in copies:
        copy.wait()


def prolong(s, arrived, restriction, pattern):
    return pl.pallas_call(
        functools.partial(prolong_kernel, s),
        in_specs=[vmem_spec()] * 2 + [pl.BlockSpec(memory_space=pltpu.HBM)],
        out_specs=pl.BlockSpec(memory_space=pltpu.HBM),
        out_shape=jax.ShapeDtypeStruct((3, s.loads, s.fine), jnp.float32),
        scratch_shapes=[
            pltpu.VMEM((3, s.q, s.agg), jnp.float32),
            pltpu.VMEM((FPA, 3, s.q, s.agg), jnp.float32),
            pltpu.VMEM((1, s.fine), jnp.int32),
            pltpu.SemaphoreType.DMA((FPA + 1,)),
        ],
        name="prolong",
        compiler_params=KERNEL,
    )(in_vmem(arrived), in_vmem(restriction), in_hbm(pattern))


def fetch_row(slot_ref, lines, row, held):
    for lane in range(LANES):
        slot = slot_ref[row, lane]
        held[lane : lane + 1, :] = lines[pl.ds(slot, 1), :]


def edges_kernel(s, slot_ref, in_ref, coef_ref, lines, top_ref, bottom_ref, *held):
    lines_from_tiles(s, in_ref, lines)
    places = []
    for at in range(s.depth):
        places += [(at, top_ref, at), (s.rows - s.depth + at, bottom_ref, at)]
    for (row, _, _), buffer in zip(places, held):
        fetch_row(slot_ref, lines, row, buffer)
    for (row, target, at), buffer in zip(places, held):
        target[at, 0 : s.comps, :] = buffer[...].T[0 : s.comps]
        target[at, s.comps :, :] = coef_ref[row]


def edges(s, received, slots, coefs):
    edge = vmem_result(s.depth, s.comps + COEFS, LANES)
    return pl.pallas_call(
        functools.partial(edges_kernel, s),
        in_specs=[pl.BlockSpec(memory_space=pltpu.SMEM)] + [vmem_spec()] * 2,
        out_specs=[vmem_spec()] * 3,
        out_shape=[vmem_result(s.agg, LANES), edge, edge],
        scratch_shapes=[pltpu.VMEM((LANES, LANES), jnp.float32)] * (2 * s.depth),
        name="edges",
        compiler_params=KERNEL,
    )(slots, in_vmem(received), coefs)


def collect_kernel(s, slot_ref, lines, top_ref, bottom_ref, out_ref, even, odd):
    for at in range(s.depth):
        out_ref[at] = top_ref[at, 0 : s.comps]
        out_ref[s.rows - s.depth + at] = bottom_ref[at, 0 : s.comps]

    def place(row, held):
        out_ref[row] = held[...].T[0 : s.comps]

    fetch_row(slot_ref, lines, s.depth, even)
    last = s.rows - s.depth - 1

    def two(k, carry):
        row = s.depth + 2 * k
        fetch_row(slot_ref, lines, row + 1, odd)
        place(row, even)
        fetch_row(slot_ref, lines, jnp.minimum(row + 2, last), even)
        place(row + 1, odd)
        return carry

    lax.fori_loop(0, (s.rows - 2 * s.depth) // 2, two, 0)


def collect(s, slots, lines, top, bottom):
    return pl.pallas_call(
        functools.partial(collect_kernel, s),
        in_specs=[pl.BlockSpec(memory_space=pltpu.SMEM)] + [vmem_spec()] * 3,
        out_specs=vmem_spec(),
        out_shape=vmem_result(s.rows, s.comps, LANES),
        scratch_shapes=[pltpu.VMEM((LANES, LANES), jnp.float32)] * 2,
        name="collect",
        compiler_params=KERNEL,
    )(slots, lines, top, bottom)


PACK = 32
EDGE = LANES // PACK


def pack_lines(line_of, count, left_ref, right_ref, span, start=None):
    for pack in range(left_ref.shape[0]):
        left, right = (None, None) if start is None else (start[0][pack], start[1][pack])
        for member in range(min(PACK, count - pack * PACK)):
            line = line_of(pack * PACK + member)
            if line is None:
                continue
            by = (member + 1) * EDGE
            head, tail = turn(line, by - EDGE), turn(line, by)
            if left is None:
                left, right = head, tail
            else:
                here = lax.broadcasted_iota(jnp.int32, line.shape, 1) // EDGE == member
                left = jnp.where(here, head, left)
                right = jnp.where(here, tail, right)
        left_ref[pack, span, :] = left
        right_ref[pack, span, :] = right


def pack_kernel(s, body_ref, left_coef_ref, right_coef_ref, before_ref, after_ref, left_ref, right_ref):
    def line_of(at, own_ref, span):
        if at < s.depth:
            return before_ref[at, span, :]
        if at < s.depth + s.rows:
            return None if own_ref is None else own_ref[at - s.depth]
        return after_ref[at - s.depth - s.rows, span, :]

    loads, coefs = slice(0, s.comps), slice(s.comps, s.comps + COEFS)
    pack_lines(lambda at: line_of(at, body_ref, loads), s.wide, left_ref, right_ref, loads)
    start = (left_coef_ref, right_coef_ref)
    pack_lines(lambda at: line_of(at, None, coefs), s.wide, left_ref, right_ref, coefs, start)


def pack_edges(s, body, packs, before, after):
    shape = vmem_result(-(-s.wide // PACK), s.comps + COEFS, LANES)
    return pl.pallas_call(
        functools.partial(pack_kernel, s),
        in_specs=[vmem_spec()] * 5,
        out_specs=[vmem_spec()] * 2,
        out_shape=[shape, shape],
        name="pack_edges",
        compiler_params=KERNEL,
    )(body, *packs, in_vmem(before), in_vmem(after))


COEFS = 48


def prepare_kernel(s, inv_ref, off_ref, pat_ref, body_ref, left_ref, right_ref, flat):
    rows = s.rows
    flat[0 : 9 * rows, :] = inv_ref[...]
    for direction in range(4):
        mask = pat_ref[direction * rows : (direction + 1) * rows, :].astype(jnp.float32)
        for entry in range(9):
            at = direction * 9 + entry
            flat[(9 + at) * rows : (10 + at) * rows, :] = off_ref[at * rows : (at + 1) * rows, :] * mask
    flat[45 * rows : COEFS * rows, :] = jnp.zeros(((COEFS - 45) * rows, LANES), jnp.float32)

    def one(row, carry):
        for low in range(0, COEFS, 8):
            body_ref[row, low : low + 8, :] = flat[pl.ds(low * rows + row, 8, stride=rows), :]
        return carry

    lax.fori_loop(0, rows, one, 0)

    def line_of(at):
        return body_ref[at - s.depth] if s.depth <= at < s.depth + rows else None

    pack_lines(line_of, s.wide, left_ref, right_ref, slice(0, COEFS))


def prepare(s, inverse, blocks, pattern):
    return pl.pallas_call(
        functools.partial(prepare_kernel, s),
        in_specs=[vmem_spec()] * 3,
        out_specs=[vmem_spec()] * 3,
        out_shape=[vmem_result(s.rows, COEFS, LANES)] + [vmem_result(-(-s.wide // PACK), COEFS, LANES)] * 2,
        scratch_shapes=[pltpu.VMEM((COEFS * s.rows, LANES), jnp.float32)],
        name="prepare",
        compiler_params=KERNEL,
    )(inverse.reshape(-1, LANES), blocks.reshape(-1, LANES), pattern.reshape(-1, LANES))


class Jacobi:
    def __init__(self, s, rhs_ref, coef_ref):
        self.q, self.rhs, self.coef = s.q, rhs_ref, coef_ref
        self.halves = range(0, s.q, 8)

    def span(self, comp, low):
        return slice(comp * self.q + low, comp * self.q + low + 8)

    def read(self, ref, at):
        return [[ref[at, self.span(comp, low), :] for low in self.halves] for comp in range(3)]

    def write(self, ref, at, fresh):
        for comp in range(3):
            for half, low in enumerate(self.halves):
                ref[at, self.span(comp, low), :] = fresh[comp][half]

    def factor(self, at, index):
        return self.coef[at, index : index + 1, :]

    def invert(self, at, total):
        fresh = []
        for comp in range(3):
            value = [None] * len(self.halves)
            for source in range(3):
                factor = self.factor(at, comp * 3 + source)
                for half in range(len(self.halves)):
                    term = factor * total[source][half]
                    value[half] = term if source == 0 else value[half] + term
            fresh.append(value)
        return fresh

    def first(self, at):
        return self.invert(at, self.read(self.rhs, at))

    def next(self, old, at):
        here = self.read(old, at)
        pieces = [
            self.read(old, at - 1),
            self.read(old, at + 1),
            [[turn(x, 1) for x in each] for each in here],
            [[turn(x, -1) for x in each] for each in here],
        ]
        total = self.read(self.rhs, at)
        for comp in range(3):
            for direction in range(4):
                for source in range(3):
                    factor = self.factor(at, 9 + (direction * 3 + comp) * 3 + source)
                    for half in range(len(self.halves)):
                        total[comp][half] = total[comp][half] - factor * pieces[direction][source][half]
        return self.invert(at, total)

    def run(self, s, even, odd):
        def first(k, carry):
            for at in (2 * k, 2 * k + 1):
                self.write(even, at, self.first(at))
            return carry

        lax.fori_loop(0, s.wide // 2, first, 0)
        old, new = even, odd
        for inner in range(1, s.depth):
            def middle(k, carry, old=old, new=new, inner=inner):
                for step in range(2):
                    at = inner + 2 * k + step
                    self.write(new, at, self.next(old, at))
                return carry

            lax.fori_loop(0, (s.wide - 2 * inner) // 2, middle, 0)
            old, new = new, old
        return old


HALF = LANES // 2


def inside_of(axis):
    here = lax.axis_index(axis)
    return [jnp.where(x, 1.0, 0.0) for x in (here > 0, here < lax.axis_size(axis) - 1)]


def inner_kernel(
    s, rhs_ref, own_ref, before_ref, after_ref,
    sol_ref, rhs_strip_ref, coef_strip_ref, wide, coef_ref, even, odd,
):
    inside = inside_of("row")
    lane = lax.broadcasted_iota(jnp.int32, (COEFS, LANES), 1)
    for held, own, strip, part in (
        (wide, rhs_ref, rhs_strip_ref, slice(0, s.comps)),
        (coef_ref, own_ref, coef_strip_ref, slice(s.comps, s.comps + COEFS)),
    ):
        for at in range(s.wide):
            row = at - s.depth
            if row < 0:
                line, side = before_ref[at, part, :], inside[0]
            elif row < s.rows:
                line, side = own[row], None
            else:
                line, side = after_ref[row - s.rows, part, :], inside[1]
            if held is coef_ref and side is not None:
                line = line * side
            held[at] = line
            strip[at] = jnp.where(lane < LANES // 4, line, turn(line, HALF))

    jacobi = Jacobi(s, wide, coef_ref)
    old = jacobi.run(s, even, odd)

    def last(k, carry):
        for row in (2 * k, 2 * k + 1):
            jacobi.write(sol_ref, row, jacobi.next(old, row + s.depth))
        return carry

    lax.fori_loop(0, s.rows // 2, last, 0)


def inner(s, rhs, coefs, before, after):
    strip = (s.wide, s.comps, LANES)
    coef_strip = (s.wide, COEFS, LANES)
    state = pltpu.VMEM(strip, jnp.float32)
    return pl.pallas_call(
        functools.partial(inner_kernel, s),
        in_specs=[vmem_spec()] * 4,
        out_specs=[vmem_spec()] * 3,
        out_shape=[vmem_result(s.rows, s.comps, LANES), vmem_result(*strip), vmem_result(*coef_strip)],
        scratch_shapes=[state, pltpu.VMEM(coef_strip, jnp.float32), state, state],
        name="inner",
        compiler_params=KERNEL,
    )(rhs, coefs, in_vmem(before), in_vmem(after))


def outer_kernel(
    s, slot_ref, inner_ref, rhs_strip_ref, coef_strip_ref, past_ref, ahead_ref,
    sol_hbm, out_ref, wide, coef_ref, even, odd, sol_ref, lines, ahead_lines, behind_lines, sem,
):
    lane = lax.broadcasted_iota(jnp.int32, (COEFS, LANES), 1)
    left, right = lane >= LANES - s.depth, (lane >= HALF) & (lane < HALF + s.depth)
    rows = inside_of("row")
    columns = inside_of("col")
    for held, own, part in (
        (wide, rhs_strip_ref, slice(0, s.comps)),
        (coef_ref, coef_strip_ref, slice(s.comps, s.comps + COEFS)),
    ):
        for pack in range(past_ref.shape[0]):
            past, ahead = past_ref[pack, part, :], ahead_ref[pack, part, :]
            if held is coef_ref:
                past, ahead = past * columns[1], ahead * columns[0]
            for member in range(min(PACK, s.wide - pack * PACK)):
                at = pack * PACK + member
                far, near = turn(past, HALF - member * EDGE), turn(ahead, -(member + 1) * EDGE)
                if held is coef_ref and not s.depth <= at < s.depth + s.rows:
                    side = rows[0] if at < s.depth else rows[1]
                    far, near = far * side, near * side
                held[at] = jnp.where(right, far, jnp.where(left, near, own[at]))

    jacobi = Jacobi(s, wide, coef_ref)
    old = jacobi.run(s, even, odd)
    place = lax.broadcasted_iota(jnp.int32, (8, LANES), 1)

    def finish(row, held):
        fresh = jacobi.next(old, row + s.depth)
        main = jacobi.read(inner_ref, row)
        for comp in range(3):
            for half in range(len(fresh[comp])):
                strip = fresh[comp][half]
                value = jnp.where(place < s.depth, strip, main[comp][half])
                fresh[comp][half] = jnp.where(place >= LANES - s.depth, turn(strip, HALF), value)
        jacobi.write(sol_ref, row, fresh)
        held[:, 0 : s.comps] = jnp.concatenate([x for each in fresh for x in each], axis=0).T

    def send(row, held):
        for column in range(LANES):
            slot = slot_ref[row, column]
            lines[pl.ds(slot, 1), :] = held[column : column + 1, :]

    finish(0, ahead_lines)
    finish(1, behind_lines)

    def two(k, carry):
        row = 2 * k
        send(row, ahead_lines)
        send(row + 1, behind_lines)
        finish(row + 2, ahead_lines)
        finish(row + 3, behind_lines)
        return carry

    lax.fori_loop(0, s.rows // 2 - 1, two, 0)
    copy = pltpu.make_async_copy(sol_ref, sol_hbm, sem)
    copy.start()
    send(s.rows - 2, ahead_lines)
    send(s.rows - 1, behind_lines)
    tiles_from_lines(s, lines, out_ref)
    copy.wait()


def outer(s, slots, main, rhs_strip, coef_strip, past, ahead):
    state = pltpu.VMEM((s.wide, s.comps, LANES), jnp.float32)
    return pl.pallas_call(
        functools.partial(outer_kernel, s),
        in_specs=[pl.BlockSpec(memory_space=pltpu.SMEM)] + [vmem_spec()] * 5,
        out_specs=[pl.BlockSpec(memory_space=pltpu.HBM), vmem_spec()],
        out_shape=[
            pltpu.HBM((s.rows, s.comps, LANES), jnp.float32),
            jax.ShapeDtypeStruct((s.devices * s.per_peer, LANES), jnp.float32),
        ],
        scratch_shapes=[
            state,
            pltpu.VMEM((s.wide, COEFS, LANES), jnp.float32),
            state,
            state,
            pltpu.VMEM((s.rows, s.comps, LANES), jnp.float32),
            pltpu.VMEM((s.agg, LANES), jnp.float32),
            pltpu.VMEM((LANES, LANES), jnp.float32),
            pltpu.VMEM((LANES, LANES), jnp.float32),
            pltpu.SemaphoreType.DMA,
        ],
        name="outer",
        compiler_params=KERNEL,
    )(slots, main, rhs_strip, coef_strip, in_vmem(past), in_vmem(ahead))


def ring(axis):
    count = lax.axis_size(axis)
    up = [(i, (i + 1) % count) for i in range(count)]
    return up, [(j, i) for i, j in up]


def exchange(s, outgoing):
    blocks = outgoing.reshape(s.devices, s.per_peer, LANES)
    moved = lax.all_to_all(blocks, AXES, split_axis=0, concat_axis=0, tiled=True)
    return moved.reshape(s.devices * s.per_peer, LANES)


def body(
    fine_residual,
    restriction,
    restriction_pattern,
    cell_aggregate,
    block_inverse,
    off_blocks,
    operator_pattern,
):
    s = Sizes(
        fine_residual.shape[2],
        fine_residual.shape[0],
        cell_aggregate.shape[0],
        cell_aggregate.shape[1],
        lax.axis_size("row"),
        lax.axis_size("col"),
    )
    residual = fine_residual.transpose(1, 0, 2)
    pattern = restriction_pattern.reshape(1, -1)

    outgoing = restrict(s, residual, restriction, pattern)
    received = exchange(s, outgoing)
    owner = cell_aggregate // s.agg
    local = cell_aggregate % s.agg
    slots = local // s.devices * s.devices + owner
    coefs, *packs = prepare(s, block_inverse, off_blocks, operator_pattern)

    up, down = ring("row")
    lines, top, bottom = edges(s, received, slots, coefs)
    before = lax.ppermute(bottom, "row", up)
    after = lax.ppermute(top, "row", down)
    rhs = collect(s, slots, lines, top, bottom)
    left, right = pack_edges(s, rhs, packs, before, after)
    up, down = ring("col")
    ahead = lax.ppermute(right, "col", up)
    past = lax.ppermute(left, "col", down)
    main, *strips = inner(s, rhs, coefs, before, after)
    solved, outgoing = outer(s, slots, main, *strips, past, ahead)
    correction = prolong(s, exchange(s, outgoing), restriction, pattern)
    coarse = solved.reshape(s.rows, 3, s.loads, LANES).transpose(2, 1, 0, 3)
    return coarse, correction.transpose(1, 0, 2)


def solution(mesh):
    in_specs = (
        P(None, None, AXES),
        P(None, None, AXES),
        P(AXES),
        P("row", "col"),
        P(None, None, "row", "col"),
        P(None, None, None, "row", "col"),
        P(None, "row", "col"),
    )
    out_specs = (P(None, None, "row", "col"), P(None, None, AXES))
    return jax.shard_map(body, mesh=mesh, in_specs=in_specs, out_specs=out_specs, check_vma=False)
```

```python
import functools
import math

import jax
import jax.numpy as jnp
from jax import lax
from jax.experimental import pallas as pl
from jax.experimental.pallas import tpu as pltpu
from jax.sharding import PartitionSpec as P

FPA = 8
ITERS = 4
LANES = 128
UNROLL = 4
AXES = ("row", "col")


def vmem_spec():
    return pl.BlockSpec(memory_space=pltpu.VMEM)


KERNEL = pltpu.CompilerParams(vmem_limit_bytes=30 * 1024 * 1024)


def in_vmem(x):
    return pltpu.with_memory_space_constraint(x, pltpu.VMEM)


def in_hbm(x):
    return pltpu.with_memory_space_constraint(x, pltpu.HBM)


def vmem_result(*shape):
    return pltpu.VMEM(shape, jnp.float32)


class Sizes:
    def __init__(self, fine, loads, rows, cols, rows_n, cols_n):
        self.devices = rows_n * cols_n
        self.rows_n, self.cols_n = rows_n, cols_n
        self.fine = fine
        self.agg = fine // FPA
        self.blocks = self.agg // LANES
        self.loads = loads
        self.rows, self.cols = rows, cols
        self.q = loads
        self.comps = 3 * self.q
        self.group = LANES // math.gcd(self.comps, LANES)
        self.groups = self.blocks // self.group
        self.tiles = self.group * self.comps // LANES
        self.low = LANES // self.devices
        self.per_peer = self.tiles * self.groups * self.low
        self.depth = ITERS - 1
        self.wide = rows + 2 * self.depth


def starts(s, grp, tile):
    for low in range(s.low):
        slot = (grp * s.tiles + tile) * s.low + low
        for first in range(0, s.devices, 8):
            yield low * s.devices + first, first * s.per_peer + slot


def pieces(s, grp):
    for member in range(s.group):
        done = 0
        while done < s.comps:
            at = member * s.comps + done
            size = min(s.comps - done, LANES - at % LANES)
            yield at // LANES, at % LANES, member, done, size
            done += size


def store_tiles(s, out_ref, rows_of):
    for grp in range(s.groups):
        rows = jnp.concatenate([rows_of(grp * s.group + member) for member in range(s.group)], axis=0)
        for tile in range(s.tiles):
            turned = rows[tile * LANES : (tile + 1) * LANES].T
            for lane, start in starts(s, grp, tile):
                out_ref[pl.ds(start, 8, stride=s.per_peer), :] = turned[lane : lane + 8]


def load_tiles(s, in_ref, take):
    for grp in range(s.groups):
        turned = []
        for tile in range(s.tiles):
            parts = [in_ref[pl.ds(start, 8, stride=s.per_peer), :] for _, start in starts(s, grp, tile)]
            turned.append(jnp.concatenate(parts, axis=0).T)
        rows = jnp.concatenate(turned, axis=0)
        for member in range(s.group):
            take(grp * s.group + member, rows[member * s.comps : (member + 1) * s.comps])


def turn(x, by):
    return pltpu.roll(x, by % LANES, 1) if by % LANES else x


def lines_from_tiles(s, in_ref, lines):
    where = lax.broadcasted_iota(jnp.int32, (8, LANES), 1)
    for grp in range(s.groups):
        runs = [dict(starts(s, grp, tile)) for tile in range(s.tiles)]
        for lane in runs[0]:
            held = [in_ref[pl.ds(run[lane], 8, stride=s.per_peer), :] for run in runs]
            made = {}
            for tile, low, member, done, size in pieces(s, grp):
                part = turn(held[tile], done - low)
                made[member] = jnp.where(where >= done, part, made[member]) if member in made else part
            for member, line in made.items():
                row = (grp * s.group + member) * LANES + lane
                lines[row : row + 8, :] = line


def tiles_from_lines(s, lines, out_ref):
    where = lax.broadcasted_iota(jnp.int32, (8, LANES), 1)
    for grp in range(s.groups):
        runs = [dict(starts(s, grp, tile)) for tile in range(s.tiles)]
        for lane in runs[0]:
            held = []
            for member in range(s.group):
                row = (grp * s.group + member) * LANES + lane
                held.append(lines[row : row + 8, :])
            made = {}
            for tile, low, member, done, size in pieces(s, grp):
                part = turn(held[member], low - done)
                made[tile] = jnp.where(where >= low, part, made[tile]) if tile in made else part
            for tile, value in made.items():
                out_ref[pl.ds(runs[tile][lane], 8, stride=s.per_peer), :] = value


def spread(row):
    return jnp.broadcast_to(row, (8, LANES))


def each_column(s, visit):
    def some(block, carry):
        for step in range(UNROLL):
            visit(pl.ds(pl.multiple_of((block * UNROLL + step) * LANES, LANES), LANES))
        return carry

    lax.fori_loop(0, s.blocks // UNROLL, some, 0)


def restrict_kernel(s, x_hbm, rest_hbm, pat_hbm, out_ref, x_ref, rest_ref, pat_ref, acc, sems):
    copies = []
    for part in range(FPA):
        at = pl.ds(part * s.agg, s.agg)
        group = (
            pltpu.make_async_copy(rest_hbm.at[:, :, at], rest_ref.at[part], sems.at[part, 0]),
            pltpu.make_async_copy(pat_hbm.at[:, at], pat_ref.at[part], sems.at[part, 1]),
            pltpu.make_async_copy(x_hbm.at[:, :, at], x_ref.at[part], sems.at[part, 2]),
        )
        for copy in group:
            copy.start()
        copies.append(group)

    for part in range(FPA):
        for copy in copies[part]:
            copy.wait()

        def column(at, part=part):
            mask = spread(pat_ref[part, 0:1, at]).astype(jnp.float32)
            for comp in range(3):
                factor = [spread(rest_ref[part, comp, k : k + 1, at]) * mask for k in range(3)]
                for low in range(0, s.q, 8):
                    loads = slice(low, low + 8)
                    total = factor[0] * x_ref[part, 0, loads, at]
                    for source in range(1, 3):
                        total = total + factor[source] * x_ref[part, source, loads, at]
                    acc[comp, loads, at] = total if part == 0 else acc[comp, loads, at] + total

        each_column(s, column)

    def rows_of(block):
        return jnp.concatenate([acc[comp, :, block * LANES : (block + 1) * LANES] for comp in range(3)], axis=0)

    store_tiles(s, out_ref, rows_of)


def restrict(s, residual, restriction, pattern):
    return pl.pallas_call(
        functools.partial(restrict_kernel, s),
        in_specs=[pl.BlockSpec(memory_space=pltpu.HBM)] * 3,
        out_specs=vmem_spec(),
        out_shape=vmem_result(s.devices * s.per_peer, LANES),
        scratch_shapes=[
            pltpu.VMEM((FPA, 3, s.q, s.agg), jnp.float32),
            pltpu.VMEM((FPA, 3, 3, s.agg), jnp.float32),
            pltpu.VMEM((FPA, 1, s.agg), jnp.int32),
            pltpu.VMEM((3, s.q, s.agg), jnp.float32),
            pltpu.SemaphoreType.DMA((FPA, 3)),
        ],
        name="restrict",
        compiler_params=KERNEL,
    )(*map(in_hbm, (residual, restriction, pattern)))


def prolong_kernel(s, in_ref, rest_ref, pat_hbm, out_hbm, agg, out_ref, pat_ref, sems):
    fetch = pltpu.make_async_copy(pat_hbm, pat_ref, sems.at[FPA])
    fetch.start()

    def take(block, rows):
        for comp in range(3):
            agg[comp, :, block * LANES : (block + 1) * LANES] = rows[comp * s.q : (comp + 1) * s.q]

    load_tiles(s, in_ref, take)
    fetch.wait()
    copies = []
    for part in range(FPA):
        def column(at, part=part):
            there = pl.ds(pl.multiple_of(at.start + part * s.agg, LANES), LANES)
            mask = spread(pat_ref[0:1, there]).astype(jnp.float32)
            for comp in range(3):
                factor = [spread(rest_ref[k, comp : comp + 1, there]) * mask for k in range(3)]
                for low in range(0, s.q, 8):
                    loads = slice(low, low + 8)
                    total = factor[0] * agg[0, loads, at]
                    for source in range(1, 3):
                        total = total + factor[source] * agg[source, loads, at]
                    out_ref[part, comp, loads, at] = total

        each_column(s, column)
        copy = pltpu.make_async_copy(
            out_ref.at[part], out_hbm.at[:, :, pl.ds(part * s.agg, s.agg)], sems.at[part]
        )
        copy.start()
        copies.append(copy)
    for copy in copies:
        copy.wait()


def prolong(s, arrived, restriction, pattern):
    return pl.pallas_call(
        functools.partial(prolong_kernel, s),
        in_specs=[vmem_spec()] * 2 + [pl.BlockSpec(memory_space=pltpu.HBM)],
        out_specs=pl.BlockSpec(memory_space=pltpu.HBM),
        out_shape=jax.ShapeDtypeStruct((3, s.loads, s.fine), jnp.float32),
        scratch_shapes=[
            pltpu.VMEM((3, s.q, s.agg), jnp.float32),
            pltpu.VMEM((FPA, 3, s.q, s.agg), jnp.float32),
            pltpu.VMEM((1, s.fine), jnp.int32),
            pltpu.SemaphoreType.DMA((FPA + 1,)),
        ],
        name="prolong",
        compiler_params=KERNEL,
    )(in_vmem(arrived), in_vmem(restriction), in_hbm(pattern))


def fetch_row(slot_ref, lines, row, held):
    for lane in range(LANES):
        slot = slot_ref[row, lane]
        held[lane : lane + 1, :] = lines[pl.ds(slot, 1), :]


def edges_kernel(s, slot_ref, in_ref, coef_ref, lines, top_ref, bottom_ref, *held):
    lines_from_tiles(s, in_ref, lines)
    places = []
    for at in range(s.depth):
        places += [(at, top_ref, at), (s.rows - s.depth + at, bottom_ref, at)]
    for (row, _, _), buffer in zip(places, held):
        fetch_row(slot_ref, lines, row, buffer)
    for (row, target, at), buffer in zip(places, held):
        target[at, 0 : s.comps, :] = buffer[...].T[0 : s.comps]
        target[at, s.comps :, :] = coef_ref[row]


def edges(s, received, slots, coefs):
    edge = vmem_result(s.depth, s.comps + COEFS, LANES)
    return pl.pallas_call(
        functools.partial(edges_kernel, s),
        in_specs=[pl.BlockSpec(memory_space=pltpu.SMEM)] + [vmem_spec()] * 2,
        out_specs=[vmem_spec()] * 3,
        out_shape=[vmem_result(s.agg, LANES), edge, edge],
        scratch_shapes=[pltpu.VMEM((LANES, LANES), jnp.float32)] * (2 * s.depth),
        name="edges",
        compiler_params=KERNEL,
    )(slots, in_vmem(received), coefs)


def collect_kernel(s, slot_ref, lines, top_ref, bottom_ref, out_ref, even, odd):
    for at in range(s.depth):
        out_ref[at] = top_ref[at, 0 : s.comps]
        out_ref[s.rows - s.depth + at] = bottom_ref[at, 0 : s.comps]

    def place(row, held):
        out_ref[row] = held[...].T[0 : s.comps]

    fetch_row(slot_ref, lines, s.depth, even)
    last = s.rows - s.depth - 1

    def two(k, carry):
        row = s.depth + 2 * k
        fetch_row(slot_ref, lines, row + 1, odd)
        place(row, even)
        fetch_row(slot_ref, lines, jnp.minimum(row + 2, last), even)
        place(row + 1, odd)
        return carry

    lax.fori_loop(0, (s.rows - 2 * s.depth) // 2, two, 0)


def collect(s, slots, lines, top, bottom):
    return pl.pallas_call(
        functools.partial(collect_kernel, s),
        in_specs=[pl.BlockSpec(memory_space=pltpu.SMEM)] + [vmem_spec()] * 3,
        out_specs=vmem_spec(),
        out_shape=vmem_result(s.rows, s.comps, LANES),
        scratch_shapes=[pltpu.VMEM((LANES, LANES), jnp.float32)] * 2,
        name="collect",
        compiler_params=KERNEL,
    )(slots, lines, top, bottom)


PACK = 32
EDGE = LANES // PACK


def pack_lines(line_of, count, left_ref, right_ref, span, start=None):
    for pack in range(left_ref.shape[0]):
        left, right = (None, None) if start is None else (start[0][pack], start[1][pack])
        for member in range(min(PACK, count - pack * PACK)):
            line = line_of(pack * PACK + member)
            if line is None:
                continue
            by = (member + 1) * EDGE
            head, tail = turn(line, by - EDGE), turn(line, by)
            if left is None:
                left, right = head, tail
            else:
                here = lax.broadcasted_iota(jnp.int32, line.shape, 1) // EDGE == member
                left = jnp.where(here, head, left)
                right = jnp.where(here, tail, right)
        left_ref[pack, span, :] = left
        right_ref[pack, span, :] = right


def pack_kernel(s, body_ref, left_coef_ref, right_coef_ref, before_ref, after_ref, left_ref, right_ref):
    def line_of(at, own_ref, span):
        if at < s.depth:
            return before_ref[at, span, :]
        if at < s.depth + s.rows:
            return None if own_ref is None else own_ref[at - s.depth]
        return after_ref[at - s.depth - s.rows, span, :]

    loads, coefs = slice(0, s.comps), slice(s.comps, s.comps + COEFS)
    pack_lines(lambda at: line_of(at, body_ref, loads), s.wide, left_ref, right_ref, loads)
    start = (left_coef_ref, right_coef_ref)
    pack_lines(lambda at: line_of(at, None, coefs), s.wide, left_ref, right_ref, coefs, start)


def pack_edges(s, body, packs, before, after):
    shape = vmem_result(-(-s.wide // PACK), s.comps + COEFS, LANES)
    return pl.pallas_call(
        functools.partial(pack_kernel, s),
        in_specs=[vmem_spec()] * 5,
        out_specs=[vmem_spec()] * 2,
        out_shape=[shape, shape],
        name="pack_edges",
        compiler_params=KERNEL,
    )(body, *packs, in_vmem(before), in_vmem(after))


COEFS = 48
HALF = LANES // 2
SHIFT = LANES // 4


def own_strip(line):
    lane = lax.broadcasted_iota(jnp.int32, line.shape, 1)
    return jnp.where(lane < SHIFT, line, turn(line, HALF))


def second(shape):
    lane = lax.broadcasted_iota(jnp.int32, shape, 1)
    return (lane + SHIFT // 2) // SHIFT % 2 == 1


def prepare_kernel(s, inv_ref, off_ref, pat_ref, body_ref, left_ref, right_ref, strip_ref, flat):
    rows = s.rows
    flat[0 : 9 * rows, :] = inv_ref[...]
    for direction in range(4):
        mask = pat_ref[direction * rows : (direction + 1) * rows, :].astype(jnp.float32)
        for entry in range(9):
            at = direction * 9 + entry
            flat[(9 + at) * rows : (10 + at) * rows, :] = off_ref[at * rows : (at + 1) * rows, :] * mask
    flat[45 * rows : COEFS * rows, :] = jnp.zeros(((COEFS - 45) * rows, LANES), jnp.float32)

    def one(row, carry):
        for low in range(0, COEFS, 8):
            line = flat[pl.ds(low * rows + row, 8, stride=rows), :]
            body_ref[row, low : low + 8, :] = line
            strip_ref[row, low : low + 8, :] = own_strip(line)
        return carry

    lax.fori_loop(0, rows, one, 0)

    def line_of(at):
        return body_ref[at - s.depth] if s.depth <= at < s.depth + rows else None

    pack_lines(line_of, s.wide, left_ref, right_ref, slice(0, COEFS))


def prepare(s, inverse, blocks, pattern):
    return pl.pallas_call(
        functools.partial(prepare_kernel, s),
        in_specs=[vmem_spec()] * 3,
        out_specs=[vmem_spec()] * 4,
        out_shape=[
            vmem_result(s.rows, COEFS, LANES),
            vmem_result(-(-s.wide // PACK), COEFS, LANES),
            vmem_result(-(-s.wide // PACK), COEFS, LANES),
            vmem_result(s.rows, COEFS, LANES),
        ],
        scratch_shapes=[pltpu.VMEM((COEFS * s.rows, LANES), jnp.float32)],
        name="prepare",
        compiler_params=KERNEL,
    )(inverse.reshape(-1, LANES), blocks.reshape(-1, LANES), pattern.reshape(-1, LANES))


class Jacobi:
    def __init__(self, loads, rhs_ref, coef_ref):
        self.q, self.rhs, self.coef = loads, rhs_ref, coef_ref
        self.halves = range(0, loads, 8)

    def span(self, comp, low):
        return slice(comp * self.q + low, comp * self.q + low + 8)

    def read(self, ref, at):
        return [[ref[at, self.span(comp, low), :] for low in self.halves] for comp in range(3)]

    def write(self, ref, at, fresh):
        for comp in range(3):
            for half, low in enumerate(self.halves):
                ref[at, self.span(comp, low), :] = fresh[comp][half]

    def factor(self, at, index):
        return self.coef[at, index : index + 1, :]

    def invert(self, at, total):
        fresh = []
        for comp in range(3):
            value = [None] * len(self.halves)
            for source in range(3):
                factor = self.factor(at, comp * 3 + source)
                for half in range(len(self.halves)):
                    term = factor * total[source][half]
                    value[half] = term if source == 0 else value[half] + term
            fresh.append(value)
        return fresh

    def first(self, at):
        return self.invert(at, self.read(self.rhs, at))

    def next(self, old, at):
        here = self.read(old, at)
        pieces = [
            self.read(old, at - 1),
            self.read(old, at + 1),
            [[turn(x, 1) for x in each] for each in here],
            [[turn(x, -1) for x in each] for each in here],
        ]
        total = self.read(self.rhs, at)
        for comp in range(3):
            for direction in range(4):
                for source in range(3):
                    factor = self.factor(at, 9 + (direction * 3 + comp) * 3 + source)
                    for half in range(len(self.halves)):
                        total[comp][half] = total[comp][half] - factor * pieces[direction][source][half]
        return self.invert(at, total)

    def run(self, s, even, odd):
        def first(k, carry):
            for at in (2 * k, 2 * k + 1):
                self.write(even, at, self.first(at))
            return carry

        lax.fori_loop(0, s.wide // 2, first, 0)
        old, new = even, odd
        for inner in range(1, s.depth):
            def middle(k, carry, old=old, new=new, inner=inner):
                for step in range(2):
                    at = inner + 2 * k + step
                    self.write(new, at, self.next(old, at))
                return carry

            lax.fori_loop(0, (s.wide - 2 * inner) // 2, middle, 0)
            old, new = new, old
        return old


def inside_of(axis):
    here = lax.axis_index(axis)
    return [jnp.where(x, 1.0, 0.0) for x in (here > 0, here < lax.axis_size(axis) - 1)]


def inner_kernel(s, rhs_ref, own_ref, before_ref, after_ref, wide, coef_ref, even, strip_ref, odd):
    inside = inside_of("row")
    loads, coefs = slice(0, s.comps), slice(s.comps, s.comps + COEFS)
    upper = second((8, LANES))
    for at in range(s.wide):
        row = at - s.depth
        if row < 0:
            line, factor = before_ref[at, loads, :], before_ref[at, coefs, :] * inside[0]
        elif row < s.rows:
            line, factor = rhs_ref[row], own_ref[row]
        else:
            line, factor = after_ref[row - s.rows, loads, :], after_ref[row - s.rows, coefs, :] * inside[1]
        wide[at] = line
        coef_ref[at] = factor
        for comp in range(3):
            low = comp * s.q
            first, other = own_strip(line[low : low + 8]), own_strip(line[low + 8 : low + 16])
            strip_ref[at, comp * 8 : comp * 8 + 8, :] = jnp.where(upper, turn(other, SHIFT), first)
    Jacobi(s.q, wide, coef_ref).run(s, even, odd)


def inner(s, rhs, coefs, before, after):
    tile = (s.wide, s.comps, LANES)
    return pl.pallas_call(
        functools.partial(inner_kernel, s),
        in_specs=[vmem_spec()] * 4,
        out_specs=[vmem_spec()] * 4,
        out_shape=[
            vmem_result(*tile),
            vmem_result(s.wide, COEFS, LANES),
            vmem_result(*tile),
            vmem_result(s.wide, 24, LANES),
        ],
        scratch_shapes=[pltpu.VMEM(tile, jnp.float32)],
        name="inner",
        compiler_params=KERNEL,
    )(rhs, coefs, in_vmem(before), in_vmem(after))


def outer_kernel(
    s, slot_ref, main_rhs_ref, main_coef_ref, main_ref, rhs_strip_ref, coef_strip_ref, past_ref, ahead_ref,
    sol_hbm, out_ref, wide, coef_ref, even, odd, sol_ref, lines, ahead_lines, behind_lines, sem,
):
    columns = inside_of("col")
    rows = inside_of("row")

    def sides(shape, by):
        lane = lax.broadcasted_iota(jnp.int32, shape, 1)
        right = (lane >= HALF + by) & (lane < HALF + by + s.depth)
        end = by if by else LANES
        return right, (lane >= end - s.depth) & (lane < end)

    upper = second((COEFS, LANES))
    factor_sides = sides((COEFS, LANES), 0)
    load_sides = [sides((8, LANES), 0), sides((8, LANES), SHIFT)]
    coefs = slice(s.comps, s.comps + COEFS)
    for at in range(s.wide):
        pack, member = divmod(at, PACK)
        row = at - s.depth
        far = turn(past_ref[pack, coefs, :], HALF - member * EDGE) * columns[1]
        near = turn(ahead_ref[pack, coefs, :], -(member + 1) * EDGE) * columns[0]
        if 0 <= row < s.rows:
            own = coef_strip_ref[row]
        else:
            own = own_strip(main_coef_ref[at])
            side = rows[0] if row < 0 else rows[1]
            far, near = far * side, near * side
        right, left = factor_sides
        factor = jnp.where(right, far, jnp.where(left, near, own))
        coef_ref[at] = jnp.where(upper, turn(factor, SHIFT), factor)
        for comp in range(3):
            value = rhs_strip_ref[at, comp * 8 : comp * 8 + 8, :]
            for half in range(2):
                part = slice(comp * s.q + half * 8, comp * s.q + half * 8 + 8)
                by = half * SHIFT
                right, left = load_sides[half]
                far = turn(past_ref[pack, part, :], HALF + by - member * EDGE)
                near = turn(ahead_ref[pack, part, :], by - (member + 1) * EDGE)
                value = jnp.where(right, far, jnp.where(left, near, value))
            wide[at, comp * 8 : comp * 8 + 8, :] = value

    strips = Jacobi(8, wide, coef_ref)
    old = strips.run(s, even, odd)
    main = Jacobi(s.q, main_rhs_ref, main_coef_ref)
    place = lax.broadcasted_iota(jnp.int32, (8, LANES), 1)

    def finish(row, held):
        fresh = main.next(main_ref, row + s.depth)
        ends = strips.next(old, row + s.depth)
        for comp in range(3):
            (strip,) = ends[comp]
            for half in range(2):
                by = half * SHIFT
                value = jnp.where(place < s.depth, turn(strip, -by), fresh[comp][half])
                fresh[comp][half] = jnp.where(place >= LANES - s.depth, turn(strip, HALF - by), value)
        main.write(sol_ref, row, fresh)
        held[:, 0 : s.comps] = jnp.concatenate([x for each in fresh for x in each], axis=0).T

    def send(row, held):
        for column in range(LANES):
            slot = slot_ref[row, column]
            lines[pl.ds(slot, 1), :] = held[column : column + 1, :]

    finish(0, ahead_lines)
    finish(1, behind_lines)

    def two(k, carry):
        row = 2 * k
        send(row, ahead_lines)
        send(row + 1, behind_lines)
        finish(row + 2, ahead_lines)
        finish(row + 3, behind_lines)
        return carry

    lax.fori_loop(0, s.rows // 2 - 1, two, 0)
    copy = pltpu.make_async_copy(sol_ref, sol_hbm, sem)
    copy.start()
    send(s.rows - 2, ahead_lines)
    send(s.rows - 1, behind_lines)
    tiles_from_lines(s, lines, out_ref)
    copy.wait()


def outer(s, slots, tile, coef_strip, past, ahead):
    state = pltpu.VMEM((s.wide, 24, LANES), jnp.float32)
    return pl.pallas_call(
        functools.partial(outer_kernel, s),
        in_specs=[pl.BlockSpec(memory_space=pltpu.SMEM)] + [vmem_spec()] * 7,
        out_specs=[pl.BlockSpec(memory_space=pltpu.HBM), vmem_spec()],
        out_shape=[
            pltpu.HBM((s.rows, s.comps, LANES), jnp.float32),
            jax.ShapeDtypeStruct((s.devices * s.per_peer, LANES), jnp.float32),
        ],
        scratch_shapes=[
            state,
            pltpu.VMEM((s.wide, COEFS, LANES), jnp.float32),
            state,
            state,
            pltpu.VMEM((s.rows, s.comps, LANES), jnp.float32),
            pltpu.VMEM((s.agg, LANES), jnp.float32),
            pltpu.VMEM((LANES, LANES), jnp.float32),
            pltpu.VMEM((LANES, LANES), jnp.float32),
            pltpu.SemaphoreType.DMA,
        ],
        name="outer",
        compiler_params=KERNEL,
    )(slots, *tile, coef_strip, in_vmem(past), in_vmem(ahead))


def ring(axis):
    count = lax.axis_size(axis)
    up = [(i, (i + 1) % count) for i in range(count)]
    return up, [(j, i) for i, j in up]


def exchange(s, outgoing):
    blocks = outgoing.reshape(s.devices, s.per_peer, LANES)
    moved = lax.all_to_all(blocks, AXES, split_axis=0, concat_axis=0, tiled=True)
    return moved.reshape(s.devices * s.per_peer, LANES)


def body(
    fine_residual,
    restriction,
    restriction_pattern,
    cell_aggregate,
    block_inverse,
    off_blocks,
    operator_pattern,
):
    s = Sizes(
        fine_residual.shape[2],
        fine_residual.shape[0],
        cell_aggregate.shape[0],
        cell_aggregate.shape[1],
        lax.axis_size("row"),
        lax.axis_size("col"),
    )
    residual = fine_residual.transpose(1, 0, 2)
    pattern = restriction_pattern.reshape(1, -1)

    outgoing = restrict(s, residual, restriction, pattern)
    received = exchange(s, outgoing)
    owner = cell_aggregate // s.agg
    local = cell_aggregate % s.agg
    slots = local // s.devices * s.devices + owner
    slots, block_inverse = lax.optimization_barrier((slots, block_inverse))
    coefs, *packs, coef_strip = prepare(s, block_inverse, off_blocks, operator_pattern)

    up, down = ring("row")
    lines, top, bottom = edges(s, received, slots, coefs)
    before = lax.ppermute(bottom, "row", up)
    after = lax.ppermute(top, "row", down)
    rhs = collect(s, slots, lines, top, bottom)
    left, right = pack_edges(s, rhs, packs, before, after)
    up, down = ring("col")
    ahead = lax.ppermute(right, "col", up)
    past = lax.ppermute(left, "col", down)
    tile = inner(s, rhs, coefs, before, after)
    solved, outgoing = outer(s, slots, tile, coef_strip, past, ahead)
    correction = prolong(s, exchange(s, outgoing), restriction, pattern)
    coarse = solved.reshape(s.rows, 3, s.loads, LANES).transpose(2, 1, 0, 3)
    return coarse, correction.transpose(1, 0, 2)


def solution(mesh):
    in_specs = (
        P(None, None, AXES),
        P(None, None, AXES),
        P(AXES),
        P("row", "col"),
        P(None, None, "row", "col"),
        P(None, None, None, "row", "col"),
        P(None, "row", "col"),
    )
    out_specs = (P(None, None, "row", "col"), P(None, None, AXES))
    return jax.shard_map(body, mesh=mesh, in_specs=in_specs, out_specs=out_specs, check_vma=False)
```

```python
import functools
import math

import jax
import jax.numpy as jnp
from jax import lax
from jax.experimental import pallas as pl
from jax.experimental.pallas import tpu as pltpu
from jax.sharding import PartitionSpec as P

FPA = 8
ITERS = 4
LANES = 128
UNROLL = 4
AXES = ("row", "col")


def vmem_spec():
    return pl.BlockSpec(memory_space=pltpu.VMEM)


KERNEL = pltpu.CompilerParams(vmem_limit_bytes=30 * 1024 * 1024)


def in_vmem(x):
    return pltpu.with_memory_space_constraint(x, pltpu.VMEM)


def in_hbm(x):
    return pltpu.with_memory_space_constraint(x, pltpu.HBM)


def vmem_result(*shape):
    return pltpu.VMEM(shape, jnp.float32)


class Sizes:
    def __init__(self, fine, loads, rows, cols, rows_n, cols_n):
        self.devices = rows_n * cols_n
        self.rows_n, self.cols_n = rows_n, cols_n
        self.fine = fine
        self.agg = fine // FPA
        self.blocks = self.agg // LANES
        self.loads = loads
        self.rows, self.cols = rows, cols
        self.q = loads
        self.comps = 3 * self.q
        self.group = LANES // math.gcd(self.comps, LANES)
        self.groups = self.blocks // self.group
        self.tiles = self.group * self.comps // LANES
        self.low = LANES // self.devices
        self.per_peer = self.tiles * self.groups * self.low
        self.depth = ITERS - 1
        self.wide = rows + 2 * self.depth


def starts(s, grp, tile):
    for low in range(s.low):
        slot = (grp * s.tiles + tile) * s.low + low
        for first in range(0, s.devices, 8):
            yield low * s.devices + first, first * s.per_peer + slot


def pieces(s, grp):
    for member in range(s.group):
        done = 0
        while done < s.comps:
            at = member * s.comps + done
            size = min(s.comps - done, LANES - at % LANES)
            yield at // LANES, at % LANES, member, done, size
            done += size


def store_tiles(s, out_ref, rows_of):
    for grp in range(s.groups):
        rows = jnp.concatenate([rows_of(grp * s.group + member) for member in range(s.group)], axis=0)
        for tile in range(s.tiles):
            turned = rows[tile * LANES : (tile + 1) * LANES].T
            for lane, start in starts(s, grp, tile):
                out_ref[pl.ds(start, 8, stride=s.per_peer), :] = turned[lane : lane + 8]


def load_tiles(s, in_ref, take):
    for grp in range(s.groups):
        turned = []
        for tile in range(s.tiles):
            parts = [in_ref[pl.ds(start, 8, stride=s.per_peer), :] for _, start in starts(s, grp, tile)]
            turned.append(jnp.concatenate(parts, axis=0).T)
        rows = jnp.concatenate(turned, axis=0)
        for member in range(s.group):
            take(grp * s.group + member, rows[member * s.comps : (member + 1) * s.comps])


def turn(x, by):
    return pltpu.roll(x, by % LANES, 1) if by % LANES else x


def lines_from_tiles(s, in_ref, lines):
    where = lax.broadcasted_iota(jnp.int32, (8, LANES), 1)
    for grp in range(s.groups):
        runs = [dict(starts(s, grp, tile)) for tile in range(s.tiles)]
        for lane in runs[0]:
            held = [in_ref[pl.ds(run[lane], 8, stride=s.per_peer), :] for run in runs]
            made = {}
            for tile, low, member, done, size in pieces(s, grp):
                part = turn(held[tile], done - low)
                made[member] = jnp.where(where >= done, part, made[member]) if member in made else part
            for member, line in made.items():
                row = (grp * s.group + member) * LANES + lane
                lines[row : row + 8, :] = line


def tiles_from_lines(s, lines, out_ref):
    where = lax.broadcasted_iota(jnp.int32, (8, LANES), 1)
    for grp in range(s.groups):
        runs = [dict(starts(s, grp, tile)) for tile in range(s.tiles)]
        for lane in runs[0]:
            held = []
            for member in range(s.group):
                row = (grp * s.group + member) * LANES + lane
                held.append(lines[row : row + 8, :])
            made = {}
            for tile, low, member, done, size in pieces(s, grp):
                part = turn(held[member], low - done)
                made[tile] = jnp.where(where >= low, part, made[tile]) if tile in made else part
            for tile, value in made.items():
                out_ref[pl.ds(runs[tile][lane], 8, stride=s.per_peer), :] = value


def spread(row):
    return jnp.broadcast_to(row, (8, LANES))


def each_column(s, visit):
    def some(block, carry):
        for step in range(UNROLL):
            visit(pl.ds(pl.multiple_of((block * UNROLL + step) * LANES, LANES), LANES))
        return carry

    lax.fori_loop(0, s.blocks // UNROLL, some, 0)


def restrict_kernel(s, x_hbm, rest_hbm, pat_hbm, out_ref, x_ref, rest_ref, pat_ref, acc, sems):
    copies = []
    for part in range(FPA):
        at = pl.ds(part * s.agg, s.agg)
        group = (
            pltpu.make_async_copy(rest_hbm.at[:, :, at], rest_ref.at[part], sems.at[part, 0]),
            pltpu.make_async_copy(pat_hbm.at[:, at], pat_ref.at[part], sems.at[part, 1]),
            pltpu.make_async_copy(x_hbm.at[:, :, at], x_ref.at[part], sems.at[part, 2]),
        )
        for copy in group:
            copy.start()
        copies.append(group)

    for part in range(FPA):
        for copy in copies[part]:
            copy.wait()

        def column(at, part=part):
            mask = spread(pat_ref[part, 0:1, at]).astype(jnp.float32)
            for comp in range(3):
                factor = [spread(rest_ref[part, comp, k : k + 1, at]) * mask for k in range(3)]
                for low in range(0, s.q, 8):
                    loads = slice(low, low + 8)
                    total = factor[0] * x_ref[part, 0, loads, at]
                    for source in range(1, 3):
                        total = total + factor[source] * x_ref[part, source, loads, at]
                    acc[comp, loads, at] = total if part == 0 else acc[comp, loads, at] + total

        each_column(s, column)

    def rows_of(block):
        return jnp.concatenate([acc[comp, :, block * LANES : (block + 1) * LANES] for comp in range(3)], axis=0)

    store_tiles(s, out_ref, rows_of)


def restrict(s, residual, restriction, pattern):
    return pl.pallas_call(
        functools.partial(restrict_kernel, s),
        in_specs=[pl.BlockSpec(memory_space=pltpu.HBM)] * 3,
        out_specs=vmem_spec(),
        out_shape=vmem_result(s.devices * s.per_peer, LANES),
        scratch_shapes=[
            pltpu.VMEM((FPA, 3, s.q, s.agg), jnp.float32),
            pltpu.VMEM((FPA, 3, 3, s.agg), jnp.float32),
            pltpu.VMEM((FPA, 1, s.agg), jnp.int32),
            pltpu.VMEM((3, s.q, s.agg), jnp.float32),
            pltpu.SemaphoreType.DMA((FPA, 3)),
        ],
        name="restrict",
        compiler_params=KERNEL,
    )(*map(in_hbm, (residual, restriction, pattern)))


def prolong_kernel(s, in_ref, rest_ref, pat_hbm, out_hbm, agg, out_ref, pat_ref, sems):
    fetch = pltpu.make_async_copy(pat_hbm, pat_ref, sems.at[FPA])
    fetch.start()

    def take(block, rows):
        for comp in range(3):
            agg[comp, :, block * LANES : (block + 1) * LANES] = rows[comp * s.q : (comp + 1) * s.q]

    load_tiles(s, in_ref, take)
    fetch.wait()
    copies = []
    for part in range(FPA):
        def column(at, part=part):
            there = pl.ds(pl.multiple_of(at.start + part * s.agg, LANES), LANES)
            mask = spread(pat_ref[0:1, there]).astype(jnp.float32)
            for comp in range(3):
                factor = [spread(rest_ref[k, comp : comp + 1, there]) * mask for k in range(3)]
                for low in range(0, s.q, 8):
                    loads = slice(low, low + 8)
                    total = factor[0] * agg[0, loads, at]
                    for source in range(1, 3):
                        total = total + factor[source] * agg[source, loads, at]
                    out_ref[part, comp, loads, at] = total

        each_column(s, column)
        copy = pltpu.make_async_copy(
            out_ref.at[part], out_hbm.at[:, :, pl.ds(part * s.agg, s.agg)], sems.at[part]
        )
        copy.start()
        copies.append(copy)
    for copy in copies:
        copy.wait()


def prolong(s, arrived, restriction, pattern):
    return pl.pallas_call(
        functools.partial(prolong_kernel, s),
        in_specs=[vmem_spec()] * 2 + [pl.BlockSpec(memory_space=pltpu.HBM)],
        out_specs=pl.BlockSpec(memory_space=pltpu.HBM),
        out_shape=jax.ShapeDtypeStruct((3, s.loads, s.fine), jnp.float32),
        scratch_shapes=[
            pltpu.VMEM((3, s.q, s.agg), jnp.float32),
            pltpu.VMEM((FPA, 3, s.q, s.agg), jnp.float32),
            pltpu.VMEM((1, s.fine), jnp.int32),
            pltpu.SemaphoreType.DMA((FPA + 1,)),
        ],
        name="prolong",
        compiler_params=KERNEL,
    )(in_vmem(arrived), in_vmem(restriction), in_hbm(pattern))


def fetch_row(slot_ref, lines, row, held):
    for lane in range(LANES):
        slot = slot_ref[row, lane]
        held[lane : lane + 1, :] = lines[pl.ds(slot, 1), :]


def edges_kernel(s, slot_ref, in_ref, coef_ref, lines, top_ref, bottom_ref, *held):
    lines_from_tiles(s, in_ref, lines)
    places = []
    for at in range(s.depth):
        places += [(at, top_ref, at), (s.rows - s.depth + at, bottom_ref, at)]
    for (row, _, _), buffer in zip(places, held):
        fetch_row(slot_ref, lines, row, buffer)
    for (row, target, at), buffer in zip(places, held):
        target[at, 0 : s.comps, :] = buffer[...].T[0 : s.comps]
        target[at, s.comps :, :] = coef_ref[row]


def edges(s, received, slots, coefs):
    edge = vmem_result(s.depth, s.comps + COEFS, LANES)
    return pl.pallas_call(
        functools.partial(edges_kernel, s),
        in_specs=[pl.BlockSpec(memory_space=pltpu.SMEM)] + [vmem_spec()] * 2,
        out_specs=[vmem_spec()] * 3,
        out_shape=[vmem_result(s.agg, LANES), edge, edge],
        scratch_shapes=[pltpu.VMEM((LANES, LANES), jnp.float32)] * (2 * s.depth),
        name="edges",
        compiler_params=KERNEL,
    )(slots, in_vmem(received), coefs)


def collect_kernel(s, slot_ref, lines, top_ref, bottom_ref, out_ref, even, odd):
    for at in range(s.depth):
        out_ref[at] = top_ref[at, 0 : s.comps]
        out_ref[s.rows - s.depth + at] = bottom_ref[at, 0 : s.comps]

    def place(row, held):
        out_ref[row] = held[...].T[0 : s.comps]

    fetch_row(slot_ref, lines, s.depth, even)
    last = s.rows - s.depth - 1

    def two(k, carry):
        row = s.depth + 2 * k
        fetch_row(slot_ref, lines, row + 1, odd)
        place(row, even)
        fetch_row(slot_ref, lines, jnp.minimum(row + 2, last), even)
        place(row + 1, odd)
        return carry

    lax.fori_loop(0, (s.rows - 2 * s.depth) // 2, two, 0)


def collect(s, slots, lines, top, bottom):
    return pl.pallas_call(
        functools.partial(collect_kernel, s),
        in_specs=[pl.BlockSpec(memory_space=pltpu.SMEM)] + [vmem_spec()] * 3,
        out_specs=vmem_spec(),
        out_shape=vmem_result(s.rows, s.comps, LANES),
        scratch_shapes=[pltpu.VMEM((LANES, LANES), jnp.float32)] * 2,
        name="collect",
        compiler_params=KERNEL,
    )(slots, lines, top, bottom)


PACK = 32
EDGE = LANES // PACK


def pack_lines(line_of, count, left_ref, right_ref, span, start=None):
    for pack in range(left_ref.shape[0]):
        left, right = (None, None) if start is None else (start[0][pack], start[1][pack])
        for member in range(min(PACK, count - pack * PACK)):
            line = line_of(pack * PACK + member)
            if line is None:
                continue
            by = (member + 1) * EDGE
            head, tail = turn(line, by - EDGE), turn(line, by)
            if left is None:
                left, right = head, tail
            else:
                here = lax.broadcasted_iota(jnp.int32, line.shape, 1) // EDGE == member
                left = jnp.where(here, head, left)
                right = jnp.where(here, tail, right)
        left_ref[pack, span, :] = left
        right_ref[pack, span, :] = right


def beyond(past, ahead, member, depth):
    if member:
        past = pltpu.roll(past, LANES - member * EDGE, 1)
    turn = (member + 1) * EDGE
    if turn < LANES:
        ahead = pltpu.roll(ahead, LANES - turn, 1)
    lane = lax.broadcasted_iota(jnp.int32, past.shape, 1)
    return jnp.where(lane < depth, past, jnp.where(lane >= LANES - depth, ahead, 0.0))


def pack_kernel(s, body_ref, left_coef_ref, right_coef_ref, before_ref, after_ref, left_ref, right_ref):
    def line_of(at, own_ref, span):
        if at < s.depth:
            return before_ref[at, span, :]
        if at < s.depth + s.rows:
            return None if own_ref is None else own_ref[at - s.depth]
        return after_ref[at - s.depth - s.rows, span, :]

    loads, coefs = slice(0, s.comps), slice(s.comps, s.comps + COEFS)
    pack_lines(lambda at: line_of(at, body_ref, loads), s.wide, left_ref, right_ref, loads)
    start = (left_coef_ref, right_coef_ref)
    pack_lines(lambda at: line_of(at, None, coefs), s.wide, left_ref, right_ref, coefs, start)


def pack_edges(s, body, packs, before, after):
    shape = vmem_result(-(-s.wide // PACK), s.comps + COEFS, LANES)
    return pl.pallas_call(
        functools.partial(pack_kernel, s),
        in_specs=[vmem_spec()] * 5,
        out_specs=[vmem_spec()] * 2,
        out_shape=[shape, shape],
        name="pack_edges",
        compiler_params=KERNEL,
    )(body, *packs, in_vmem(before), in_vmem(after))


COEFS = 48


def prepare_kernel(s, inv_ref, off_ref, pat_ref, body_ref, left_ref, right_ref, flat):
    rows = s.rows
    flat[0 : 9 * rows, :] = inv_ref[...]
    for direction in range(4):
        mask = pat_ref[direction * rows : (direction + 1) * rows, :].astype(jnp.float32)
        for entry in range(9):
            at = direction * 9 + entry
            flat[(9 + at) * rows : (10 + at) * rows, :] = off_ref[at * rows : (at + 1) * rows, :] * mask
    flat[45 * rows : COEFS * rows, :] = jnp.zeros(((COEFS - 45) * rows, LANES), jnp.float32)

    def one(row, carry):
        for low in range(0, COEFS, 8):
            body_ref[row, low : low + 8, :] = flat[pl.ds(low * rows + row, 8, stride=rows), :]
        return carry

    lax.fori_loop(0, rows, one, 0)

    def line_of(at):
        return body_ref[at - s.depth] if s.depth <= at < s.depth + rows else None

    pack_lines(line_of, s.wide, left_ref, right_ref, slice(0, COEFS))


def prepare(s, inverse, blocks, pattern):
    return pl.pallas_call(
        functools.partial(prepare_kernel, s),
        in_specs=[vmem_spec()] * 3,
        out_specs=[vmem_spec()] * 3,
        out_shape=[vmem_result(s.rows, COEFS, LANES)] + [vmem_result(-(-s.wide // PACK), COEFS, LANES)] * 2,
        scratch_shapes=[pltpu.VMEM((COEFS * s.rows, LANES), jnp.float32)],
        name="prepare",
        compiler_params=KERNEL,
    )(inverse.reshape(-1, LANES), blocks.reshape(-1, LANES), pattern.reshape(-1, LANES))


def inside_of(axis):
    here = lax.axis_index(axis)
    return [jnp.where(x, 1.0, 0.0) for x in (here > 0, here < lax.axis_size(axis) - 1)]


def sweeps_kernel(
    s, slot_ref, rhs_ref, own_ref, before_ref, after_ref, past_ref, ahead_ref,
    sol_hbm, out_ref, wide, coef_ref, even, odd, sol_ref, lines, ahead_lines, behind_lines, sem,
):
    q = s.q
    halves = range(0, q, 8)
    lane = lax.broadcasted_iota(jnp.int32, (COEFS, LANES), 1)
    rows, columns = inside_of("row"), inside_of("col")
    side = jnp.where(lane < LANES // 2, columns[1], columns[0])
    for held, inner_ref, part in (
        (wide, rhs_ref, slice(0, s.comps)),
        (coef_ref, own_ref, slice(s.comps, s.comps + COEFS)),
    ):
        for at in range(s.wide):
            if at < s.depth:
                line, inside = before_ref[at, part, :], rows[0]
            elif at < s.depth + s.rows:
                line, inside = inner_ref[at - s.depth], None
            else:
                line, inside = after_ref[at - s.depth - s.rows, part, :], rows[1]
            pack, member = divmod(at, PACK)
            other = beyond(past_ref[pack, part, :], ahead_ref[pack, part, :], member, s.depth)
            if held is coef_ref:
                other = other * side
                if inside is not None:
                    line, other = line * inside, other * inside
            held[at, :, 0:LANES] = line
            held[at, :, LANES : 2 * LANES] = other

    lane = lax.broadcasted_iota(jnp.int32, (8, LANES), 1)
    is_first = lane == 0
    is_last = lane == LANES - 1
    columns = (slice(0, LANES), slice(LANES, 2 * LANES))

    def span(comp, low):
        return slice(comp * q + low, comp * q + low + 8)

    def invert(at, total, column):
        fresh = []
        for comp in range(3):
            value = [None] * len(halves)
            for source in range(3):
                index = comp * 3 + source
                factor = coef_ref[at, index : index + 1, column]
                for half in range(len(halves)):
                    term = factor * total[source][half]
                    value[half] = term if source == 0 else value[half] + term
            fresh.append(value)
        return fresh

    def put(target, at, fresh, column):
        for comp in range(3):
            for half, low in enumerate(halves):
                target[at, span(comp, low), column] = fresh[comp][half]

    def first(at, carry):
        for column in columns:
            total = [[wide[at, span(comp, low), column] for low in halves] for comp in range(3)]
            put(even, at, invert(at, total, column), column)
        return carry

    lax.fori_loop(0, s.wide, first, 0)

    def turned(old, at):
        west = ([], [])
        east = ([], [])
        for comp in range(3):
            for side in west + east:
                side.append([])
            for low in halves:
                here = [old[at, span(comp, low), column] for column in columns]
                up = [pltpu.roll(x, 1, 1) for x in here]
                down = [pltpu.roll(x, LANES - 1, 1) for x in here]
                for v in range(2):
                    west[v][-1].append(jnp.where(is_first, up[1 - v], up[v]))
                    east[v][-1].append(jnp.where(is_last, down[1 - v], down[v]))
        return west, east

    def sweep(old, at, count):
        west, east = turned(old, at)
        result = []
        for v in range(count):
            column = columns[v]
            pieces = []
            for where in (at - 1, at + 1):
                pieces.append([[old[where, span(comp, low), column] for low in halves] for comp in range(3)])
            pieces += [west[v], east[v]]
            total = []
            for comp in range(3):
                value = [wide[at, span(comp, low), column] for low in halves]
                for direction in range(4):
                    for source in range(3):
                        index = 9 + (direction * 3 + comp) * 3 + source
                        factor = coef_ref[at, index : index + 1, column]
                        for half in range(len(halves)):
                            value[half] = value[half] - factor * pieces[direction][source][half]
                total.append(value)
            result.append(invert(at, total, column))
        return result

    old, new = even, odd
    for inner in range(1, s.depth):
        def middle(k, carry, old=old, new=new, inner=inner):
            for step in range(2):
                at = inner + 2 * k + step
                for column, fresh in zip(columns, sweep(old, at, 2)):
                    put(new, at, fresh, column)
            return carry

        lax.fori_loop(0, (s.wide - 2 * inner) // 2, middle, 0)
        old, new = new, old

    def finish(row, held):
        (fresh,) = sweep(old, row + s.depth, 1)
        put(sol_ref, row, fresh, columns[0])
        parts = [fresh[comp][half] for comp in range(3) for half in range(len(halves))]
        held[:, 0 : s.comps] = jnp.concatenate(parts, axis=0).T

    def send(row, held):
        for column in range(LANES):
            slot = slot_ref[row, column]
            lines[pl.ds(slot, 1), :] = held[column : column + 1, :]

    finish(0, ahead_lines)
    finish(1, behind_lines)

    def two(k, carry):
        row = 2 * k
        send(row, ahead_lines)
        send(row + 1, behind_lines)
        finish(row + 2, ahead_lines)
        finish(row + 3, behind_lines)
        return carry

    lax.fori_loop(0, s.rows // 2 - 1, two, 0)
    copy = pltpu.make_async_copy(sol_ref, sol_hbm, sem)
    copy.start()
    send(s.rows - 2, ahead_lines)
    send(s.rows - 1, behind_lines)
    tiles_from_lines(s, lines, out_ref)
    copy.wait()


def sweeps(s, slots, rhs, coefs, before, after, past, ahead):
    state = pltpu.VMEM((s.wide, s.comps, 2 * LANES), jnp.float32)
    return pl.pallas_call(
        functools.partial(sweeps_kernel, s),
        in_specs=[pl.BlockSpec(memory_space=pltpu.SMEM)] + [vmem_spec()] * 6,
        out_specs=[pl.BlockSpec(memory_space=pltpu.HBM), vmem_spec()],
        out_shape=[
            pltpu.HBM((s.rows, s.comps, LANES), jnp.float32),
            jax.ShapeDtypeStruct((s.devices * s.per_peer, LANES), jnp.float32),
        ],
        scratch_shapes=[
            state,
            pltpu.VMEM((s.wide, COEFS, 2 * LANES), jnp.float32),
            state,
            state,
            pltpu.VMEM((s.rows, s.comps, LANES), jnp.float32),
            pltpu.VMEM((s.agg, LANES), jnp.float32),
            pltpu.VMEM((LANES, LANES), jnp.float32),
            pltpu.VMEM((LANES, LANES), jnp.float32),
            pltpu.SemaphoreType.DMA,
        ],
        name="sweeps",
        compiler_params=KERNEL,
    )(slots, rhs, coefs, *map(in_vmem, (before, after, past, ahead)))


def ring(axis):
    count = lax.axis_size(axis)
    up = [(i, (i + 1) % count) for i in range(count)]
    return up, [(j, i) for i, j in up]


def exchange(s, outgoing):
    blocks = outgoing.reshape(s.devices, s.per_peer, LANES)
    moved = lax.all_to_all(blocks, AXES, split_axis=0, concat_axis=0, tiled=True)
    return moved.reshape(s.devices * s.per_peer, LANES)


def body(
    fine_residual,
    restriction,
    restriction_pattern,
    cell_aggregate,
    block_inverse,
    off_blocks,
    operator_pattern,
):
    s = Sizes(
        fine_residual.shape[2],
        fine_residual.shape[0],
        cell_aggregate.shape[0],
        cell_aggregate.shape[1],
        lax.axis_size("row"),
        lax.axis_size("col"),
    )
    residual = fine_residual.transpose(1, 0, 2)
    pattern = restriction_pattern.reshape(1, -1)

    outgoing = restrict(s, residual, restriction, pattern)
    received = exchange(s, outgoing)
    owner = cell_aggregate // s.agg
    local = cell_aggregate % s.agg
    slots = local // s.devices * s.devices + owner
    coefs, *packs = prepare(s, block_inverse, off_blocks, operator_pattern)

    up, down = ring("row")
    lines, top, bottom = edges(s, received, slots, coefs)
    before = lax.ppermute(bottom, "row", up)
    after = lax.ppermute(top, "row", down)
    rhs = collect(s, slots, lines, top, bottom)
    left, right = pack_edges(s, rhs, packs, before, after)
    up, down = ring("col")
    ahead = lax.ppermute(right, "col", up)
    past = lax.ppermute(left, "col", down)
    solved, outgoing = sweeps(s, slots, rhs, coefs, before, after, past, ahead)
    correction = prolong(s, exchange(s, outgoing), restriction, pattern)
    coarse = solved.reshape(s.rows, 3, s.loads, LANES).transpose(2, 1, 0, 3)
    return coarse, correction.transpose(1, 0, 2)


def solution(mesh):
    in_specs = (
        P(None, None, AXES),
        P(None, None, AXES),
        P(AXES),
        P("row", "col"),
        P(None, None, "row", "col"),
        P(None, None, None, "row", "col"),
        P(None, "row", "col"),
    )
    out_specs = (P(None, None, "row", "col"), P(None, None, AXES))
    return jax.shard_map(body, mesh=mesh, in_specs=in_specs, out_specs=out_specs, check_vma=False)
```

```python
import functools
import math

import jax
import jax.numpy as jnp
from jax import lax
from jax.experimental import pallas as pl
from jax.experimental.pallas import tpu as pltpu
from jax.sharding import PartitionSpec as P

FPA = 8
ITERS = 4
LANES = 128
UNROLL = 4
AXES = ("row", "col")


def vmem_spec():
    return pl.BlockSpec(memory_space=pltpu.VMEM)


KERNEL = pltpu.CompilerParams(vmem_limit_bytes=30 * 1024 * 1024)


def in_vmem(x):
    return pltpu.with_memory_space_constraint(x, pltpu.VMEM)


def in_hbm(x):
    return pltpu.with_memory_space_constraint(x, pltpu.HBM)


def vmem_result(*shape):
    return pltpu.VMEM(shape, jnp.float32)


class Sizes:
    def __init__(self, fine, loads, rows, cols, rows_n, cols_n):
        self.devices = rows_n * cols_n
        self.rows_n, self.cols_n = rows_n, cols_n
        self.fine = fine
        self.agg = fine // FPA
        self.blocks = self.agg // LANES
        self.loads = loads
        self.rows, self.cols = rows, cols
        self.q = loads
        self.comps = 3 * self.q
        self.group = LANES // math.gcd(self.comps, LANES)
        self.groups = self.blocks // self.group
        self.tiles = self.group * self.comps // LANES
        self.low = LANES // self.devices
        self.per_peer = self.tiles * self.groups * self.low
        self.depth = ITERS - 1
        self.wide = rows + 2 * self.depth


def starts(s, grp, tile):
    for low in range(s.low):
        slot = (grp * s.tiles + tile) * s.low + low
        for first in range(0, s.devices, 8):
            yield low * s.devices + first, first * s.per_peer + slot


def pieces(s, grp):
    for member in range(s.group):
        done = 0
        while done < s.comps:
            at = member * s.comps + done
            size = min(s.comps - done, LANES - at % LANES)
            yield at // LANES, at % LANES, member, done, size
            done += size


def store_tiles(s, out_ref, rows_of):
    for grp in range(s.groups):
        rows = jnp.concatenate([rows_of(grp * s.group + member) for member in range(s.group)], axis=0)
        for tile in range(s.tiles):
            turned = rows[tile * LANES : (tile + 1) * LANES].T
            for lane, start in starts(s, grp, tile):
                out_ref[pl.ds(start, 8, stride=s.per_peer), :] = turned[lane : lane + 8]


def load_tiles(s, in_ref, take):
    for grp in range(s.groups):
        turned = []
        for tile in range(s.tiles):
            parts = [in_ref[pl.ds(start, 8, stride=s.per_peer), :] for _, start in starts(s, grp, tile)]
            turned.append(jnp.concatenate(parts, axis=0).T)
        rows = jnp.concatenate(turned, axis=0)
        for member in range(s.group):
            take(grp * s.group + member, rows[member * s.comps : (member + 1) * s.comps])


def turn(x, by):
    return pltpu.roll(x, by % LANES, 1) if by % LANES else x


def lines_from_tiles(s, in_ref, lines):
    where = lax.broadcasted_iota(jnp.int32, (8, LANES), 1)
    for grp in range(s.groups):
        runs = [dict(starts(s, grp, tile)) for tile in range(s.tiles)]
        for lane in runs[0]:
            held = [in_ref[pl.ds(run[lane], 8, stride=s.per_peer), :] for run in runs]
            made = {}
            for tile, low, member, done, size in pieces(s, grp):
                part = turn(held[tile], done - low)
                made[member] = jnp.where(where >= done, part, made[member]) if member in made else part
            for member, line in made.items():
                row = (grp * s.group + member) * LANES + lane
                lines[row : row + 8, :] = line


def tiles_from_lines(s, lines, out_ref):
    where = lax.broadcasted_iota(jnp.int32, (8, LANES), 1)
    for grp in range(s.groups):
        runs = [dict(starts(s, grp, tile)) for tile in range(s.tiles)]
        for lane in runs[0]:
            held = []
            for member in range(s.group):
                row = (grp * s.group + member) * LANES + lane
                held.append(lines[row : row + 8, :])
            made = {}
            for tile, low, member, done, size in pieces(s, grp):
                part = turn(held[member], low - done)
                made[tile] = jnp.where(where >= low, part, made[tile]) if tile in made else part
            for tile, value in made.items():
                out_ref[pl.ds(runs[tile][lane], 8, stride=s.per_peer), :] = value


def spread(row):
    return jnp.broadcast_to(row, (8, LANES))


def each_column(s, visit):
    def some(block, carry):
        for step in range(UNROLL):
            visit(pl.ds(pl.multiple_of((block * UNROLL + step) * LANES, LANES), LANES))
        return carry

    lax.fori_loop(0, s.blocks // UNROLL, some, 0)


def restrict_kernel(s, x_hbm, rest_hbm, pat_hbm, out_ref, x_ref, rest_ref, pat_ref, acc, sems):
    copies = []
    for part in range(FPA):
        at = pl.ds(part * s.agg, s.agg)
        group = (
            pltpu.make_async_copy(rest_hbm.at[:, :, at], rest_ref.at[part], sems.at[part, 0]),
            pltpu.make_async_copy(pat_hbm.at[:, at], pat_ref.at[part], sems.at[part, 1]),
            pltpu.make_async_copy(x_hbm.at[:, :, at], x_ref.at[part], sems.at[part, 2]),
        )
        for copy in group:
            copy.start()
        copies.append(group)

    for part in range(FPA):
        for copy in copies[part]:
            copy.wait()

        def column(at, part=part):
            mask = spread(pat_ref[part, 0:1, at]).astype(jnp.float32)
            for comp in range(3):
                factor = [spread(rest_ref[part, comp, k : k + 1, at]) * mask for k in range(3)]
                for low in range(0, s.q, 8):
                    loads = slice(low, low + 8)
                    total = factor[0] * x_ref[part, 0, loads, at]
                    for source in range(1, 3):
                        total = total + factor[source] * x_ref[part, source, loads, at]
                    acc[comp, loads, at] = total if part == 0 else acc[comp, loads, at] + total

        each_column(s, column)

    def rows_of(block):
        return jnp.concatenate([acc[comp, :, block * LANES : (block + 1) * LANES] for comp in range(3)], axis=0)

    store_tiles(s, out_ref, rows_of)


def restrict(s, residual, restriction, pattern):
    return pl.pallas_call(
        functools.partial(restrict_kernel, s),
        in_specs=[pl.BlockSpec(memory_space=pltpu.HBM)] * 3,
        out_specs=vmem_spec(),
        out_shape=vmem_result(s.devices * s.per_peer, LANES),
        scratch_shapes=[
            pltpu.VMEM((FPA, 3, s.q, s.agg), jnp.float32),
            pltpu.VMEM((FPA, 3, 3, s.agg), jnp.float32),
            pltpu.VMEM((FPA, 1, s.agg), jnp.int32),
            pltpu.VMEM((3, s.q, s.agg), jnp.float32),
            pltpu.SemaphoreType.DMA((FPA, 3)),
        ],
        name="restrict",
        compiler_params=KERNEL,
    )(*map(in_hbm, (residual, restriction, pattern)))


def prolong_kernel(s, in_ref, rest_ref, pat_hbm, out_hbm, agg, out_ref, pat_ref, sems):
    fetch = pltpu.make_async_copy(pat_hbm, pat_ref, sems.at[FPA])
    fetch.start()

    def take(block, rows):
        for comp in range(3):
            agg[comp, :, block * LANES : (block + 1) * LANES] = rows[comp * s.q : (comp + 1) * s.q]

    load_tiles(s, in_ref, take)
    fetch.wait()
    copies = []
    for part in range(FPA):
        def column(at, part=part):
            there = pl.ds(pl.multiple_of(at.start + part * s.agg, LANES), LANES)
            mask = spread(pat_ref[0:1, there]).astype(jnp.float32)
            for comp in range(3):
                factor = [spread(rest_ref[k, comp : comp + 1, there]) * mask for k in range(3)]
                for low in range(0, s.q, 8):
                    loads = slice(low, low + 8)
                    total = factor[0] * agg[0, loads, at]
                    for source in range(1, 3):
                        total = total + factor[source] * agg[source, loads, at]
                    out_ref[part, comp, loads, at] = total

        each_column(s, column)
        copy = pltpu.make_async_copy(
            out_ref.at[part], out_hbm.at[:, :, pl.ds(part * s.agg, s.agg)], sems.at[part]
        )
        copy.start()
        copies.append(copy)
    for copy in copies:
        copy.wait()


def prolong(s, arrived, restriction, pattern):
    return pl.pallas_call(
        functools.partial(prolong_kernel, s),
        in_specs=[vmem_spec()] * 2 + [pl.BlockSpec(memory_space=pltpu.HBM)],
        out_specs=pl.BlockSpec(memory_space=pltpu.HBM),
        out_shape=jax.ShapeDtypeStruct((3, s.loads, s.fine), jnp.float32),
        scratch_shapes=[
            pltpu.VMEM((3, s.q, s.agg), jnp.float32),
            pltpu.VMEM((FPA, 3, s.q, s.agg), jnp.float32),
            pltpu.VMEM((1, s.fine), jnp.int32),
            pltpu.SemaphoreType.DMA((FPA + 1,)),
        ],
        name="prolong",
        compiler_params=KERNEL,
    )(in_vmem(arrived), in_vmem(restriction), in_hbm(pattern))


def fetch_row(slot_ref, lines, row, held):
    for lane in range(LANES):
        slot = slot_ref[row, lane]
        held[lane : lane + 1, :] = lines[pl.ds(slot, 1), :]


def edges_kernel(s, slot_vmem, in_ref, coef_ref, lines, top_ref, bottom_ref, slot_ref, sem, *held):
    fetch = pltpu.make_async_copy(slot_vmem, slot_ref, sem)
    fetch.start()
    lines_from_tiles(s, in_ref, lines)
    fetch.wait()
    places = []
    for at in range(s.depth):
        places += [(at, top_ref, at), (s.rows - s.depth + at, bottom_ref, at)]
    for (row, _, _), buffer in zip(places, held):
        fetch_row(slot_ref, lines, row, buffer)
    for (row, target, at), buffer in zip(places, held):
        target[at, 0 : s.comps, :] = buffer[...].T[0 : s.comps]
        target[at, s.comps :, :] = coef_ref[row]


def slot_scratch(s):
    return [pltpu.SMEM((s.rows, LANES), jnp.int32), pltpu.SemaphoreType.DMA]


def edges(s, received, slots, coefs):
    edge = vmem_result(s.depth, s.comps + COEFS, LANES)
    return pl.pallas_call(
        functools.partial(edges_kernel, s),
        in_specs=[vmem_spec()] * 3,
        out_specs=[vmem_spec()] * 3,
        out_shape=[vmem_result(s.agg, LANES), edge, edge],
        scratch_shapes=slot_scratch(s) + [pltpu.VMEM((LANES, LANES), jnp.float32)] * (2 * s.depth),
        name="edges",
        compiler_params=KERNEL,
    )(in_vmem(slots), in_vmem(received), coefs)


def collect_kernel(s, slot_ref, lines, top_ref, bottom_ref, out_ref, even, odd):
    for at in range(s.depth):
        out_ref[at] = top_ref[at, 0 : s.comps]
        out_ref[s.rows - s.depth + at] = bottom_ref[at, 0 : s.comps]

    def place(row, held):
        out_ref[row] = held[...].T[0 : s.comps]

    fetch_row(slot_ref, lines, s.depth, even)
    last = s.rows - s.depth - 1

    def two(k, carry):
        row = s.depth + 2 * k
        fetch_row(slot_ref, lines, row + 1, odd)
        place(row, even)
        fetch_row(slot_ref, lines, jnp.minimum(row + 2, last), even)
        place(row + 1, odd)
        return carry

    lax.fori_loop(0, (s.rows - 2 * s.depth) // 2, two, 0)


def collect(s, slots, lines, top, bottom):
    return pl.pallas_call(
        functools.partial(collect_kernel, s),
        in_specs=[pl.BlockSpec(memory_space=pltpu.SMEM)] + [vmem_spec()] * 3,
        out_specs=vmem_spec(),
        out_shape=vmem_result(s.rows, s.comps, LANES),
        scratch_shapes=[pltpu.VMEM((LANES, LANES), jnp.float32)] * 2,
        name="collect",
        compiler_params=KERNEL,
    )(slots, lines, top, bottom)


PACK = 32
EDGE = LANES // PACK


def pack_lines(line_of, count, left_ref, right_ref, span, start=None):
    for pack in range(left_ref.shape[0]):
        left, right = (None, None) if start is None else (start[0][pack], start[1][pack])
        for member in range(min(PACK, count - pack * PACK)):
            line = line_of(pack * PACK + member)
            if line is None:
                continue
            by = (member + 1) * EDGE
            head, tail = turn(line, by - EDGE), turn(line, by)
            if left is None:
                left, right = head, tail
            else:
                here = lax.broadcasted_iota(jnp.int32, line.shape, 1) // EDGE == member
                left = jnp.where(here, head, left)
                right = jnp.where(here, tail, right)
        left_ref[pack, span, :] = left
        right_ref[pack, span, :] = right


def beyond(past, ahead, member, depth):
    if member:
        past = pltpu.roll(past, LANES - member * EDGE, 1)
    turn = (member + 1) * EDGE
    if turn < LANES:
        ahead = pltpu.roll(ahead, LANES - turn, 1)
    lane = lax.broadcasted_iota(jnp.int32, past.shape, 1)
    return jnp.where(lane < depth, past, jnp.where(lane >= LANES - depth, ahead, 0.0))


def pack_kernel(s, body_ref, left_coef_ref, right_coef_ref, before_ref, after_ref, left_ref, right_ref):
    def line_of(at, own_ref, span):
        if at < s.depth:
            return before_ref[at, span, :]
        if at < s.depth + s.rows:
            return None if own_ref is None else own_ref[at - s.depth]
        return after_ref[at - s.depth - s.rows, span, :]

    loads, coefs = slice(0, s.comps), slice(s.comps, s.comps + COEFS)
    pack_lines(lambda at: line_of(at, body_ref, loads), s.wide, left_ref, right_ref, loads)
    start = (left_coef_ref, right_coef_ref)
    pack_lines(lambda at: line_of(at, None, coefs), s.wide, left_ref, right_ref, coefs, start)


def pack_edges(s, body, packs, before, after):
    shape = vmem_result(-(-s.wide // PACK), s.comps + COEFS, LANES)
    return pl.pallas_call(
        functools.partial(pack_kernel, s),
        in_specs=[vmem_spec()] * 5,
        out_specs=[vmem_spec()] * 2,
        out_shape=[shape, shape],
        name="pack_edges",
        compiler_params=KERNEL,
    )(body, *packs, in_vmem(before), in_vmem(after))


COEFS = 48


def prepare_kernel(s, inv_ref, off_ref, pat_ref, body_ref, left_ref, right_ref, flat):
    rows = s.rows
    flat[0 : 9 * rows, :] = inv_ref[...]
    for direction in range(4):
        mask = pat_ref[direction * rows : (direction + 1) * rows, :].astype(jnp.float32)
        for entry in range(9):
            at = direction * 9 + entry
            flat[(9 + at) * rows : (10 + at) * rows, :] = off_ref[at * rows : (at + 1) * rows, :] * mask
    flat[45 * rows : COEFS * rows, :] = jnp.zeros(((COEFS - 45) * rows, LANES), jnp.float32)

    def one(row, carry):
        for low in range(0, COEFS, 8):
            body_ref[row, low : low + 8, :] = flat[pl.ds(low * rows + row, 8, stride=rows), :]
        return carry

    lax.fori_loop(0, rows, one, 0)

    def line_of(at):
        return body_ref[at - s.depth] if s.depth <= at < s.depth + rows else None

    pack_lines(line_of, s.wide, left_ref, right_ref, slice(0, COEFS))


def prepare(s, inverse, blocks, pattern):
    return pl.pallas_call(
        functools.partial(prepare_kernel, s),
        in_specs=[vmem_spec()] * 3,
        out_specs=[vmem_spec()] * 3,
        out_shape=[vmem_result(s.rows, COEFS, LANES)] + [vmem_result(-(-s.wide // PACK), COEFS, LANES)] * 2,
        scratch_shapes=[pltpu.VMEM((COEFS * s.rows, LANES), jnp.float32)],
        name="prepare",
        compiler_params=KERNEL,
    )(inverse.reshape(-1, LANES), blocks.reshape(-1, LANES), pattern.reshape(-1, LANES))


def inside_of(axis):
    here = lax.axis_index(axis)
    return [jnp.where(x, 1.0, 0.0) for x in (here > 0, here < lax.axis_size(axis) - 1)]


def sweeps_kernel(
    s, slot_vmem, rhs_ref, own_ref, before_ref, after_ref, past_ref, ahead_ref,
    sol_hbm, out_ref, wide, coef_ref, even, odd, sol_ref, lines, ahead_lines, behind_lines, sem, slot_ref, slot_sem,
):
    q = s.q
    halves = range(0, q, 8)
    fetch = pltpu.make_async_copy(slot_vmem, slot_ref, slot_sem)
    fetch.start()
    lane = lax.broadcasted_iota(jnp.int32, (COEFS, LANES), 1)
    rows, columns = inside_of("row"), inside_of("col")
    side = jnp.where(lane < LANES // 2, columns[1], columns[0])
    for held, inner_ref, part in (
        (wide, rhs_ref, slice(0, s.comps)),
        (coef_ref, own_ref, slice(s.comps, s.comps + COEFS)),
    ):
        for at in range(s.wide):
            if at < s.depth:
                line, inside = before_ref[at, part, :], rows[0]
            elif at < s.depth + s.rows:
                line, inside = inner_ref[at - s.depth], None
            else:
                line, inside = after_ref[at - s.depth - s.rows, part, :], rows[1]
            pack, member = divmod(at, PACK)
            other = beyond(past_ref[pack, part, :], ahead_ref[pack, part, :], member, s.depth)
            if held is coef_ref:
                other = other * side
                if inside is not None:
                    line, other = line * inside, other * inside
            held[at, :, 0:LANES] = line
            held[at, :, LANES : 2 * LANES] = other

    lane = lax.broadcasted_iota(jnp.int32, (8, LANES), 1)
    is_first = lane == 0
    is_last = lane == LANES - 1
    columns = (slice(0, LANES), slice(LANES, 2 * LANES))

    def span(comp, low):
        return slice(comp * q + low, comp * q + low + 8)

    def invert(at, total, column):
        fresh = []
        for comp in range(3):
            value = [None] * len(halves)
            for source in range(3):
                index = comp * 3 + source
                factor = coef_ref[at, index : index + 1, column]
                for half in range(len(halves)):
                    term = factor * total[source][half]
                    value[half] = term if source == 0 else value[half] + term
            fresh.append(value)
        return fresh

    def put(target, at, fresh, column):
        for comp in range(3):
            for half, low in enumerate(halves):
                target[at, span(comp, low), column] = fresh[comp][half]

    def first(k, carry):
        for at in (2 * k, 2 * k + 1):
            for column in columns:
                total = [[wide[at, span(comp, low), column] for low in halves] for comp in range(3)]
                put(even, at, invert(at, total, column), column)
        return carry

    lax.fori_loop(0, s.wide // 2, first, 0)

    def turned(old, at):
        west = ([], [])
        east = ([], [])
        for comp in range(3):
            for side in west + east:
                side.append([])
            for low in halves:
                here = [old[at, span(comp, low), column] for column in columns]
                up = [pltpu.roll(x, 1, 1) for x in here]
                down = [pltpu.roll(x, LANES - 1, 1) for x in here]
                for v in range(2):
                    west[v][-1].append(jnp.where(is_first, up[1 - v], up[v]))
                    east[v][-1].append(jnp.where(is_last, down[1 - v], down[v]))
        return west, east

    def sweep(old, at, count):
        west, east = turned(old, at)
        result = []
        for v in range(count):
            column = columns[v]
            pieces = []
            for where in (at - 1, at + 1):
                pieces.append([[old[where, span(comp, low), column] for low in halves] for comp in range(3)])
            pieces += [west[v], east[v]]
            total = []
            for comp in range(3):
                value = [wide[at, span(comp, low), column] for low in halves]
                for direction in range(4):
                    for source in range(3):
                        index = 9 + (direction * 3 + comp) * 3 + source
                        factor = coef_ref[at, index : index + 1, column]
                        for half in range(len(halves)):
                            value[half] = value[half] - factor * pieces[direction][source][half]
                total.append(value)
            result.append(invert(at, total, column))
        return result

    old, new = even, odd
    for inner in range(1, s.depth):
        def middle(k, carry, old=old, new=new, inner=inner):
            for step in range(2):
                at = inner + 2 * k + step
                for column, fresh in zip(columns, sweep(old, at, 2)):
                    put(new, at, fresh, column)
            return carry

        lax.fori_loop(0, (s.wide - 2 * inner) // 2, middle, 0)
        old, new = new, old

    def finish(row, held):
        (fresh,) = sweep(old, row + s.depth, 1)
        put(sol_ref, row, fresh, columns[0])
        parts = [fresh[comp][half] for comp in range(3) for half in range(len(halves))]
        held[:, 0 : s.comps] = jnp.concatenate(parts, axis=0).T

    def send(row, held):
        for column in range(LANES):
            slot = slot_ref[row, column]
            lines[pl.ds(slot, 1), :] = held[column : column + 1, :]

    finish(0, ahead_lines)
    finish(1, behind_lines)
    fetch.wait()

    def two(k, carry):
        row = 2 * k
        send(row, ahead_lines)
        send(row + 1, behind_lines)
        finish(row + 2, ahead_lines)
        finish(row + 3, behind_lines)
        return carry

    lax.fori_loop(0, s.rows // 2 - 1, two, 0)
    copy = pltpu.make_async_copy(sol_ref, sol_hbm, sem)
    copy.start()
    send(s.rows - 2, ahead_lines)
    send(s.rows - 1, behind_lines)
    tiles_from_lines(s, lines, out_ref)
    copy.wait()


def sweeps(s, slots, rhs, coefs, before, after, past, ahead):
    state = pltpu.VMEM((s.wide, s.comps, 2 * LANES), jnp.float32)
    return pl.pallas_call(
        functools.partial(sweeps_kernel, s),
        in_specs=[vmem_spec()] * 7,
        out_specs=[pl.BlockSpec(memory_space=pltpu.HBM), vmem_spec()],
        out_shape=[
            pltpu.HBM((s.rows, s.comps, LANES), jnp.float32),
            jax.ShapeDtypeStruct((s.devices * s.per_peer, LANES), jnp.float32),
        ],
        scratch_shapes=[
            state,
            pltpu.VMEM((s.wide, COEFS, 2 * LANES), jnp.float32),
            state,
            state,
            pltpu.VMEM((s.rows, s.comps, LANES), jnp.float32),
            pltpu.VMEM((s.agg, LANES), jnp.float32),
            pltpu.VMEM((LANES, LANES), jnp.float32),
            pltpu.VMEM((LANES, LANES), jnp.float32),
            pltpu.SemaphoreType.DMA,
            *slot_scratch(s),
        ],
        name="sweeps",
        compiler_params=KERNEL,
    )(in_vmem(slots), rhs, coefs, *map(in_vmem, (before, after, past, ahead)))


def ring(axis):
    count = lax.axis_size(axis)
    up = [(i, (i + 1) % count) for i in range(count)]
    return up, [(j, i) for i, j in up]


def exchange(s, outgoing):
    blocks = outgoing.reshape(s.devices, s.per_peer, LANES)
    moved = lax.all_to_all(blocks, AXES, split_axis=0, concat_axis=0, tiled=True)
    return moved.reshape(s.devices * s.per_peer, LANES)


def body(
    fine_residual,
    restriction,
    restriction_pattern,
    cell_aggregate,
    block_inverse,
    off_blocks,
    operator_pattern,
):
    s = Sizes(
        fine_residual.shape[2],
        fine_residual.shape[0],
        cell_aggregate.shape[0],
        cell_aggregate.shape[1],
        lax.axis_size("row"),
        lax.axis_size("col"),
    )
    residual = fine_residual.transpose(1, 0, 2)
    pattern = restriction_pattern.reshape(1, -1)

    outgoing = restrict(s, residual, restriction, pattern)
    received = exchange(s, outgoing)
    owner = cell_aggregate // s.agg
    local = cell_aggregate % s.agg
    slots = local // s.devices * s.devices + owner
    coefs, *packs = prepare(s, block_inverse, off_blocks, operator_pattern)

    up, down = ring("row")
    lines, top, bottom = edges(s, received, slots, coefs)
    before = lax.ppermute(bottom, "row", up)
    after = lax.ppermute(top, "row", down)
    rhs = collect(s, slots, lines, top, bottom)
    left, right = pack_edges(s, rhs, packs, before, after)
    up, down = ring("col")
    ahead = lax.ppermute(right, "col", up)
    past = lax.ppermute(left, "col", down)
    solved, outgoing = sweeps(s, slots, rhs, coefs, before, after, past, ahead)
    correction = prolong(s, exchange(s, outgoing), restriction, pattern)
    coarse = solved.reshape(s.rows, 3, s.loads, LANES).transpose(2, 1, 0, 3)
    return coarse, correction.transpose(1, 0, 2)


def solution(mesh):
    in_specs = (
        P(None, None, AXES),
        P(None, None, AXES),
        P(AXES),
        P("row", "col"),
        P(None, None, "row", "col"),
        P(None, None, None, "row", "col"),
        P(None, "row", "col"),
    )
    out_specs = (P(None, None, "row", "col"), P(None, None, AXES))
    return jax.shard_map(body, mesh=mesh, in_specs=in_specs, out_specs=out_specs, check_vma=False)
```
